32 devices in a mesh: gx: 2 (over core), gy: 4 (over y, x), gz: 4 (over z).
Axes of the slice: x: 2, y: 2, z: 4, core: 2. Of those that a mesh axis runs over, the one named last changes fastest.
Arguments:
- displacement_start: float32 [3, 8, 64, 512], P(None, 'gx', 'gy', 'gz'), may hold values from -4 to 4
- external_force: float32 [3, 8, 64, 512], P(None, 'gx', 'gy', 'gz'), may hold values from -6 to 6
- damage_old: float32 [8, 64, 512], P('gx', 'gy', 'gz'), may hold values from 0 to 0.9
- history_old: float32 [8, 64, 512], P('gx', 'gy', 'gz'), may hold values from 0.02 to 2
- crack_labels: int32 [8, 64, 512], P('gx', 'gy', 'gz'), may hold values 0 or 1
- fixed_flags: int32 [8, 64, 512], P('gx', 'gy', 'gz'), may hold values 0 or 1
Outputs:
- displacement: float32 [3, 8, 64, 512], P(None, 'gx', 'gy', 'gz')
- damage: float32 [8, 64, 512], P('gx', 'gy', 'gz')
- history: float32 [8, 64, 512], P('gx', 'gy', 'gz')
The draws below stay inside these ranges and needn't reach their ends.
All inputs are finite; a program needn't handle non-finite values. No bound on the sum of `crack_labels` or of `fixed_flags` on one device may be relied on, other than what follows from the above.
Results may differ from the reference program's by a relative error of at most 0.0001.
Values sent between devices are 32-bit elements; how exact they have to be, the bound alone decides.
A program may use at most 64 MiB of HBM per device.

```python
import math
import jax
import jax.numpy as jnp
import numpy as np
from jax import lax

DISP_ITERS = 4
DMG_ITERS = 2
NX = 8
NY = 64
NZ = 512


def plant(array, key, least, top_value):
    shape = array.shape
    place = [jax.random.randint(jax.random.fold_in(key, axis), (), 0, shape[axis]) for axis in range(len(shape))]
    array = array.at[tuple(place)].set(least)
    longest = shape.index(max(shape))
    place[longest] = (place[longest] + 1) % shape[longest]
    return array.at[tuple(place)].set(top_value)


def block_scale(rng, dims, split, smallest, high):
    factor_of, own = 1.0, jax.random.fold_in(rng, 6)
    for axis_at, parts in split:
        steps = jnp.exp(jax.random.uniform(jax.random.fold_in(own, axis_at), (parts,), jnp.float32, smallest / len(split), high / len(split)))
        factor_of = factor_of * jnp.repeat(steps, dims[axis_at] // parts).reshape([-1 if axis == axis_at else 1 for axis in range(len(dims))])
    return factor_of


def noise(rng, dims, deviation, bound, shards=(), kind=jnp.bfloat16):
    level = block_scale(rng, dims, shards, -0.22, 0.18) if shards else 1.0
    array = jax.random.normal(rng, dims, jnp.float32) * deviation * level
    return jnp.minimum(jnp.maximum(array, -bound), bound).astype(kind)


def setup_inputs(seed: int = 0) -> dict:
    key_of = jax.random.split(jax.random.key(seed), 7)
    displacement_start = noise(key_of[0], (3, NX, NY, NZ), 0.5, 4.0, ((1, 2), (2, 4), (3, 4)), jnp.float32)
    external_force = noise(key_of[1], (3, NX, NY, NZ), 1.0, 6.0, ((1, 2), (2, 4), (3, 4)), jnp.float32)
    damage_old = jnp.clip(0.9 * jax.random.uniform(key_of[2], (NX, NY, NZ), jnp.float32) ** block_scale(key_of[2], (NX, NY, NZ), ((0, 2), (1, 4), (2, 4)), -0.2, 0.2), 0.0, 0.9)
    history_old = jnp.clip(jnp.exp(math.log(2.0) - 4.6051702 * jax.random.uniform(key_of[3], (NX, NY, NZ), jnp.float32) ** block_scale(key_of[3], (NX, NY, NZ), ((0, 2), (1, 4), (2, 4)), -0.2, 0.2)), 0.02, 2.0)
    crack_labels = plant((jax.random.randint(key_of[4], (NX, NY, NZ), 0, 32) < 1).astype(jnp.int32), jax.random.fold_in(key_of[4], 1), 0, 1)
    fixed_flags = plant((jax.random.randint(key_of[5], (NX, NY, NZ), 0, 16) < 1).astype(jnp.int32), jax.random.fold_in(key_of[5], 1), 0, 1)
    return dict(displacement_start=displacement_start, external_force=external_force, damage_old=damage_old, history_old=history_old, crack_labels=crack_labels, fixed_flags=fixed_flags)


LAME_LAMBDA = 0.5769230769230769
LAME_MU = 0.38461538461538464
BULK_MODULUS = LAME_LAMBDA + 2.0 * LAME_MU / 3.0
RESIDUAL_STIFFNESS = 0.001
TOUGHNESS = 1.0
LENGTH_SCALE = 2.0
CRACK_HISTORY = 40.0

def corner_offsets(corner):
    return (corner >> 2 & 1, corner >> 1 & 1, corner & 1)

def shape_gradients(sample):
    gradient = np.zeros((3, 8))
    for corner in range(8):
        offsets = corner_offsets(corner)
        values = [sample[k] if offsets[k] else 1.0 - sample[k] for k in range(3)]
        slopes = [1.0 if offsets[k] else -1.0 for k in range(3)]
        gradient[0, corner] = slopes[0] * values[1] * values[2]
        gradient[1, corner] = values[0] * slopes[1] * values[2]
        gradient[2, corner] = values[0] * values[1] * slopes[2]
    return gradient

def strain_matrix(gradient):
    strain = np.zeros((6, 24))
    for corner in range(8):
        column = 3 * corner
        strain[0, column] = gradient[0, corner]
        strain[1, column + 1] = gradient[1, corner]
        strain[2, column + 2] = gradient[2, corner]
        strain[3, column] = gradient[1, corner]
        strain[3, column + 1] = gradient[0, corner]
        strain[4, column + 1] = gradient[2, corner]
        strain[4, column + 2] = gradient[1, corner]
        strain[5, column] = gradient[2, corner]
        strain[5, column + 2] = gradient[0, corner]
    return strain

def element_tables():
    moduli = np.zeros((6, 6))
    moduli[:3, :3] = LAME_LAMBDA
    for k in range(3):
        moduli[k, k] += 2.0 * LAME_MU
        moduli[k + 3, k + 3] = LAME_MU
    points = [0.5 - 0.5 / np.sqrt(3.0), 0.5 + 0.5 / np.sqrt(3.0)]
    stiff_table = np.zeros((24, 24))
    laplace_table = np.zeros((8, 8))
    for sample_index in range(8):
        sample = tuple((points[k] for k in corner_offsets(sample_index)))
        gradient = shape_gradients(sample)
        strain = strain_matrix(gradient)
        stiff_table += 0.125 * strain.T @ moduli @ strain
        laplace_table += 0.125 * gradient.T @ gradient
    centre_table = strain_matrix(shape_gradients((0.5, 0.5, 0.5)))
    return (stiff_table.astype(np.float32), laplace_table.astype(np.float32), centre_table.astype(np.float32))

def corner_views(padded, element_shape):
    corner_list = []
    for corner in range(8):
        offx, offy, offz = corner_offsets(corner)
        corner_list.append(padded[..., offx:offx + element_shape[0], offy:offy + element_shape[1], offz:offz + element_shape[2]])
    return corner_list

def assemble_nodes(pieces):
    running = None
    for corner in range(8):
        offx, offy, offz = corner_offsets(corner)
        leading = [(0, 0)] * (pieces[corner].ndim - 3)
        placed = jnp.pad(pieces[corner], leading + [(offx, 1 - offx), (offy, 1 - offy), (offz, 1 - offz)])
        running = placed if running is None else running + placed
    return running

def valid_line(count):
    index = jnp.arange(count + 1, dtype=jnp.int32)
    return ((index >= 1) & (index <= count - 1)).astype(jnp.float32)

def strain_energy(strain):
    trace = strain[0] + strain[1] + strain[2]
    deviator = strain[:3] - trace[None] / 3.0
    shear = strain[3:]
    tensile = jnp.maximum(trace, 0.0)
    return 0.5 * BULK_MODULUS * tensile * tensile + LAME_MU * (lax.optimization_barrier(jnp.sum(deviator * deviator, axis=0)) + 0.5 * lax.optimization_barrier(jnp.sum(shear * shear, axis=0)))

def conjugate(solution, residual, apply_fn, inverse, count):
    precond = inverse * residual
    norm_now = jnp.sum(residual * precond)
    direction = precond
    for step in range(count):
        applied = apply_fn(direction)
        step_length = norm_now / jnp.sum(direction * applied)
        solution = solution + step_length * direction
        residual = residual - step_length * applied
        if step + 1 < count:
            precond = inverse * residual
            norm_next = jnp.sum(residual * precond)
            direction = precond + norm_next / norm_now * direction
            norm_now = norm_next
    return solution

def reference(displacement_start, external_force, damage_old, history_old, crack_labels, fixed_flags):
    tables = element_tables()
    stiff_table = jnp.asarray(tables[0], jnp.float32)
    laplace_table = jnp.asarray(tables[1], jnp.float32)
    centre_table = jnp.asarray(tables[2], jnp.float32)
    highest = lax.Precision.HIGHEST
    free_mask = 1.0 - fixed_flags.astype(jnp.float32)
    start_disp = displacement_start * free_mask[None]
    element_valid = valid_line(NX)[:, None, None] * valid_line(NY)[None, :, None] * valid_line(NZ)[None, None, :]
    element_shape = element_valid.shape
    damage_mean = sum(corner_views(jnp.pad(damage_old, 1), element_shape)) / 8.0
    stiffness = ((1.0 - damage_mean) ** 2 + RESIDUAL_STIFFNESS) * element_valid

    def elastic(nodal_field):
        padded = jnp.pad(nodal_field, ((0, 0), (1, 1), (1, 1), (1, 1)))
        corner_list = corner_views(padded, element_shape)
        pieces = []
        for target in range(8):
            running = None
            for source in range(8):
                block = stiff_table[3 * target:3 * target + 3, 3 * source:3 * source + 3]
                term = jnp.einsum('ij,jxyz->ixyz', block, corner_list[source], precision=highest)
                running = term if running is None else running + term
            pieces.append(stiffness[None] * running)
        return assemble_nodes(pieces)[:, 1:-1, 1:-1, 1:-1]

    def laplacian(nodal_field):
        corner_list = corner_views(jnp.pad(nodal_field, 1), element_shape)
        pieces = []
        for target in range(8):
            running = None
            for source in range(8):
                term = laplace_table[target, source] * corner_list[source]
                running = term if running is None else running + term
            pieces.append(element_valid * running)
        return assemble_nodes(pieces)[1:-1, 1:-1, 1:-1]
    disp_views = corner_views(jnp.pad(start_disp, ((0, 0), (1, 1), (1, 1), (1, 1))), element_shape)
    strain = None
    for source in range(8):
        term = jnp.einsum('ij,jxyz->ixyz', centre_table[:, 3 * source:3 * source + 3], disp_views[source], precision=highest)
        strain = term if strain is None else strain + term
    energy = strain_energy(strain) * element_valid
    nodal_energy = assemble_nodes([energy] * 8)[1:-1, 1:-1, 1:-1] / 8.0
    history = jnp.maximum(jnp.maximum(history_old, nodal_energy), CRACK_HISTORY * crack_labels.astype(jnp.float32))
    stiff_diag = jnp.diagonal(stiff_table)
    diag_pieces = [stiffness[None] * stiff_diag[3 * target:3 * target + 3][:, None, None, None] for target in range(8)]
    elastic_diag = assemble_nodes(diag_pieces)[:, 1:-1, 1:-1, 1:-1]
    inverse_elastic = 1.0 / (free_mask[None] * elastic_diag + (1.0 - free_mask[None]))

    def constrained(nodal_field):
        return free_mask[None] * elastic(free_mask[None] * nodal_field) + (1.0 - free_mask[None]) * nodal_field
    residual = free_mask[None] * (external_force - elastic(start_disp))
    displacement = conjugate(start_disp, residual, constrained, inverse_elastic, DISP_ITERS)
    reaction = TOUGHNESS / LENGTH_SCALE + 2.0 * history
    laplace_diag = assemble_nodes([element_valid * laplace_table[target, target] for target in range(8)])[1:-1, 1:-1, 1:-1]
    inverse_damage = 1.0 / (TOUGHNESS * LENGTH_SCALE * laplace_diag + reaction)

    def damage_operator(nodal_field):
        return TOUGHNESS * LENGTH_SCALE * laplacian(nodal_field) + reaction * nodal_field
    damage_residual = 2.0 * history - damage_operator(damage_old)
    damage = conjugate(damage_old, damage_residual, damage_operator, inverse_damage, DMG_ITERS)
    return (displacement, damage, history)
```

```python
import functools
import jax
import jax.numpy as jnp
import numpy as np
from jax import lax
from jax.experimental import pallas as pl
from jax.experimental.pallas import tpu as pltpu
from jax.sharding import PartitionSpec as P

DISP_ITERS = 4
DMG_ITERS = 2


LAME_LAMBDA = 0.5769230769230769
LAME_MU = 0.38461538461538464
BULK_MODULUS = LAME_LAMBDA + 2.0 * LAME_MU / 3.0
RESIDUAL_STIFFNESS = 0.001
TOUGHNESS = 1.0
LENGTH_SCALE = 2.0
CRACK_HISTORY = 40.0


def padded_2(cells, sides, width):
    for axis, dim in sides:
        count = lax.axis_size(axis)
        ends = count - 1
        head = lax.slice_in_dim(cells, 0, width, axis=dim)
        tail = lax.slice_in_dim(cells, cells.shape[dim] - width, cells.shape[dim], axis=dim)
        cells = jnp.concatenate(
            [
                lax.ppermute(tail, axis, [(i, (i + 1) % count) for i in range(ends)]),
                cells,
                lax.ppermute(head, axis, [((i + 1) % count, i) for i in range(ends)]),
            ],
            axis=dim,
        )
    return cells


def corner_offsets(corner):
    return (corner >> 2 & 1, corner >> 1 & 1, corner & 1)


def shape_gradients(sample):
    gradient = np.zeros((3, 8))
    for corner in range(8):
        offsets = corner_offsets(corner)
        values = [sample[k] if offsets[k] else 1.0 - sample[k] for k in range(3)]
        slopes = [1.0 if offsets[k] else -1.0 for k in range(3)]
        gradient[0, corner] = slopes[0] * values[1] * values[2]
        gradient[1, corner] = values[0] * slopes[1] * values[2]
        gradient[2, corner] = values[0] * values[1] * slopes[2]
    return gradient


def strain_matrix(gradient):
    strain = np.zeros((6, 24))
    for corner in range(8):
        column = 3 * corner
        strain[0, column] = gradient[0, corner]
        strain[1, column + 1] = gradient[1, corner]
        strain[2, column + 2] = gradient[2, corner]
        strain[3, column] = gradient[1, corner]
        strain[3, column + 1] = gradient[0, corner]
        strain[4, column + 1] = gradient[2, corner]
        strain[4, column + 2] = gradient[1, corner]
        strain[5, column] = gradient[2, corner]
        strain[5, column + 2] = gradient[0, corner]
    return strain


def element_tables():
    moduli = np.zeros((6, 6))
    moduli[:3, :3] = LAME_LAMBDA
    for k in range(3):
        moduli[k, k] += 2.0 * LAME_MU
        moduli[k + 3, k + 3] = LAME_MU
    points = [0.5 - 0.5 / np.sqrt(3.0), 0.5 + 0.5 / np.sqrt(3.0)]
    stiff_table = np.zeros((24, 24))
    laplace_table = np.zeros((8, 8))
    for sample_index in range(8):
        sample = tuple((points[k] for k in corner_offsets(sample_index)))
        gradient = shape_gradients(sample)
        strain = strain_matrix(gradient)
        stiff_table += 0.125 * strain.T @ moduli @ strain
        laplace_table += 0.125 * gradient.T @ gradient
    centre_table = strain_matrix(shape_gradients((0.5, 0.5, 0.5)))
    return (
        stiff_table.astype(np.float32),
        laplace_table.astype(np.float32),
        centre_table.astype(np.float32),
    )


def corner_views(padded, element_shape):
    corner_list = []
    for corner in range(8):
        offx, offy, offz = corner_offsets(corner)
        corner_list.append(
            padded[
                ...,
                offx : offx + element_shape[0],
                offy : offy + element_shape[1],
                offz : offz + element_shape[2],
            ]
        )
    return corner_list


def assemble_nodes(pieces):
    running = None
    for corner in range(8):
        offx, offy, offz = corner_offsets(corner)
        leading = [(0, 0)] * (pieces[corner].ndim - 3)
        placed = jnp.pad(
            pieces[corner], leading + [(offx, 1 - offx), (offy, 1 - offy), (offz, 1 - offz)]
        )
        running = placed if running is None else running + placed
    return running


def line_valid(position, devices, count):
    index = position * count + jnp.arange(count + 1, dtype=jnp.int32) - 1
    return ((index >= 0) & (index <= devices * count - 2)).astype(jnp.float32)


def strain_energy(strain):
    trace = strain[0] + strain[1] + strain[2]
    deviator = strain[:3] - trace[None] / 3.0
    shear = strain[3:]
    tensile = jnp.maximum(trace, 0.0)
    return 0.5 * BULK_MODULUS * tensile * tensile + LAME_MU * (
        jnp.sum(deviator * deviator, axis=0) + 0.5 * jnp.sum(shear * shear, axis=0)
    )


def forces_to_nodes(forces, stiffness):
    pieces = [stiffness[None] * forces[3 * target : 3 * target + 3] for target in range(8)]
    return assemble_nodes(pieces)


def element_apply(padded, stiffness, stiff_table):
    element_shape = stiffness.shape
    flat = jnp.stack(corner_views(padded, element_shape)).reshape(24, -1)
    forces = jnp.dot(stiff_table, flat, precision=lax.Precision.HIGHEST).reshape(
        (24,) + element_shape
    )
    return forces_to_nodes(forces, stiffness)


def laplace_apply(padded, element_valid, laplace_table):
    element_shape = element_valid.shape
    flat = jnp.stack(corner_views(padded, element_shape)).reshape(8, -1)
    forces = jnp.dot(laplace_table, flat, precision=lax.Precision.HIGHEST).reshape(
        (8,) + element_shape
    )
    return assemble_nodes([element_valid * forces[target] for target in range(8)])


def single_pair(pair):
    return tuple(lax.psum(pair, ("gx", "gy", "gz")))


def conjugate(solutions, residuals, inverses, counts, apply_fn):
    solutions = list(solutions)
    residuals = list(residuals)
    number = len(solutions)
    steps = max(counts)

    def pair_totals(pairs):
        return [single_pair(pairs[0])]

    precs = [inverses[0] * residuals[0]]
    applied = apply_fn(precs, list(range(number)))
    pairs = pair_totals([(jnp.sum(residuals[0] * precs[0]), jnp.sum(precs[0] * applied[0]))])
    norms = [pair[0] for pair in pairs]
    lengths = [pair[0] / pair[1] for pair in pairs]
    directions = list(precs)
    alongs = list(applied)
    for step in range(steps):
        active = [i for i in range(number) if step < counts[i]]
        for i in active:
            solutions[i] = solutions[i] + lengths[i] * directions[i]
            residuals[i] = residuals[i] - lengths[i] * alongs[i]
        later = [i for i in active if step + 1 < counts[i]]
        if later:
            i = later[0]
            precs[i] = inverses[i] * residuals[i]
            images = apply_fn([precs[i] for i in later], later)
            pairs = pair_totals(
                [
                    (jnp.sum(residuals[i] * precs[i]), jnp.sum(precs[i] * images[k]))
                    for k, i in enumerate(later)
                ]
            )
            for k, i in enumerate(later):
                norm_next, curve_sum = pairs[k]
                ratio = norm_next / norms[i]
                lengths[i] = norm_next / (curve_sum - ratio * norm_next / lengths[i])
                directions[i] = precs[i] + ratio * directions[i]
                alongs[i] = images[k] + ratio * alongs[i]
                norms[i] = norm_next
    return solutions


def body_any_mesh(displacement_start, external_force, damage_old, history_old, crack_labels, fixed_flags):
    tables = element_tables()
    stiff_table = jnp.asarray(tables[0], jnp.float32)
    laplace_table = jnp.asarray(tables[1], jnp.float32)
    centre_table = jnp.asarray(tables[2], jnp.float32)
    highest = lax.Precision.HIGHEST
    size_x, size_y, size_z = damage_old.shape
    free_mask = 1.0 - fixed_flags.astype(jnp.float32)
    start_disp = displacement_start * free_mask[None]
    element_valid = (
        line_valid(lax.axis_index("gx"), lax.axis_size("gx"), size_x)[:, None, None]
        * line_valid(lax.axis_index("gy"), lax.axis_size("gy"), size_y)[None, :, None]
        * line_valid(lax.axis_index("gz"), lax.axis_size("gz"), size_z)[None, None, :]
    )
    element_shape = element_valid.shape
    start_pad = padded_2(
        jnp.concatenate([start_disp, damage_old[None]], axis=0),
        (("gx", 1), ("gy", 2), ("gz", 3)),
        1,
    )
    corner_list = corner_views(start_pad, element_shape)
    damage_mean = sum((view[3] for view in corner_list)) / 8.0
    stiffness = ((1.0 - damage_mean) ** 2 + RESIDUAL_STIFFNESS) * element_valid
    flat = jnp.stack([view[:3] for view in corner_list]).reshape(24, -1)
    combined = jnp.dot(
        jnp.concatenate([stiff_table, centre_table], axis=0), flat, precision=highest
    )
    forces = combined[:24].reshape((24,) + element_shape)
    strain = combined[24:].reshape((6,) + element_shape)
    start_image = forces_to_nodes(forces, stiffness)[:, 1:-1, 1:-1, 1:-1]
    energy = strain_energy(strain) * element_valid
    nodal_energy = assemble_nodes([energy] * 8)[1:-1, 1:-1, 1:-1] / 8.0
    history = jnp.maximum(
        jnp.maximum(history_old, nodal_energy), CRACK_HISTORY * crack_labels.astype(jnp.float32)
    )
    stiff_diag = jnp.diagonal(stiff_table)
    diag_pieces = [
        stiffness[None] * stiff_diag[3 * target : 3 * target + 3][:, None, None, None]
        for target in range(8)
    ]
    elastic_diag = assemble_nodes(diag_pieces)[:, 1:-1, 1:-1, 1:-1]
    inverse_elastic = 1.0 / (free_mask[None] * elastic_diag + (1.0 - free_mask[None]))

    def constrained(nodal_field):
        masked = free_mask[None] * nodal_field
        padded = padded_2(masked, (("gx", 1), ("gy", 2), ("gz", 3)), 1)
        nodes = element_apply(padded, stiffness, stiff_table)[:, 1:-1, 1:-1, 1:-1]
        return free_mask[None] * nodes + (1.0 - free_mask[None]) * nodal_field

    reaction = TOUGHNESS / LENGTH_SCALE + 2.0 * history
    laplace_diag = assemble_nodes(
        [element_valid * laplace_table[target, target] for target in range(8)]
    )[1:-1, 1:-1, 1:-1]
    inverse_damage = 1.0 / (TOUGHNESS * LENGTH_SCALE * laplace_diag + reaction)
    residual = free_mask[None] * (external_force - start_image)
    start_lap = laplace_apply(start_pad[3], element_valid, laplace_table)[1:-1, 1:-1, 1:-1]
    damage_residual = 2.0 * history - (TOUGHNESS * LENGTH_SCALE * start_lap + reaction * damage_old)

    def damage_operator(nodal_field):
        padded = padded_2(nodal_field, (("gx", 0), ("gy", 1), ("gz", 2)), 1)
        lap_nodes = laplace_apply(padded, element_valid, laplace_table)[1:-1, 1:-1, 1:-1]
        return TOUGHNESS * LENGTH_SCALE * lap_nodes + reaction * nodal_field

    def single_elastic(fields, active):
        return [constrained(fields[0])]

    def single_damage(fields, active):
        return [damage_operator(fields[0])]

    displacement = conjugate(
        [start_disp], [residual], [inverse_elastic], [DISP_ITERS], single_elastic
    )[0]
    damage = conjugate(
        [damage_old], [damage_residual], [inverse_damage], [DMG_ITERS], single_damage
    )[0]
    return (displacement, damage, history)


SPECTRUM = 3.2
TILE = 8
GHOST = 4
DEEP = (0, 1, 2, 6)
TURNED = (0, 3)
MESH = pl.DeviceIdType.MESH


def walsh_tables():
    stiff, laplace, _ = element_tables()
    signs = np.array(
        [
            [np.prod([1.0 if c >> k & 1 else (-1.0 if m >> k & 1 else 1.0) for k in range(3)]) for c in range(8)]
            for m in range(8)
        ]
    )
    wide = np.kron(signs, np.eye(3))
    stiff_modes = wide @ stiff.astype(np.float64) @ wide.T / 64.0
    return stiff_modes, float(stiff[0, 0]), float(laplace[0, 0])


def kernel(
    sizes,
    disp_in,
    force_in,
    damage_in,
    history_in,
    labels_in,
    flags_in,
    out_disp,
    out_damage,
    out_history,
    disp_ref,
    force_ref,
    damage_ref,
    history_ref,
    labels_ref,
    flags_ref,
    own,
    part,
    down_send,
    up_send,
    from_up,
    from_down,
    part_up,
    part_down,
    zsend,
    zrecv,
    zpart,
    gz_wide,
    gz_rows,
    modes,
    basis,
    images,
    resid,
    stiff,
    inverse,
    hist,
    react,
    dinverse,
    dbasis,
    dresid,
    sums,
    in_sem,
    ysend_sem,
    yrecv_sem,
    zsend_sem,
    zrecv_sem,
    csend_sem,
    crecv_sem,
    xsend_sem,
    xrecv_sem,
    asend_sem,
    arecv_sem,
    hop_sem,
):
    ngy, ngz, lx, ly, lz = sizes
    nx = 2 * lx
    fields = 8
    npeer = ngy * ngz
    pairs = fields * lx // 2
    packs = fields * lx // 16
    extras = len(DEEP) * lx // TILE
    wide, rows = ly + 2 * TILE, ly + TILE
    GZ = nx
    f32 = jnp.float32
    stiff_modes, stiff_diag, laplace_diag = walsh_tables()
    gx, gy, gz = lax.axis_index("gx"), lax.axis_index("gy"), lax.axis_index("gz")
    me = gy * ngz + gz
    partner = (1 - gx, gy, gz)

    def there(dy, dz):
        y, z = gy + dy, gz + dz
        return (y >= 0) & (y < ngy) & (z >= 0) & (z < ngz)

    near = [(dy, dz) for dy in (-1, 0, 1) for dz in (-1, 0, 1) if dy or dz]
    number_near = sum(there(dy, dz).astype(jnp.int32) for dy, dz in near)

    barrier = pltpu.get_barrier_semaphore()

    def greet(semaphore):
        for dy, dz in near:

            @pl.when(there(dy, dz))
            def _():
                pl.semaphore_signal(
                    semaphore, inc=1, device_id=(gx, gy + dy, gz + dz), device_id_type=MESH
                )

    greet(barrier)
    pl.semaphore_signal(barrier, inc=1, device_id=partner, device_id_type=MESH)

    loads = [
        pltpu.make_async_copy(source, target, in_sem.at[i])
        for i, (source, target) in enumerate(
            [
                (flags_in, flags_ref),
                (disp_in, disp_ref),
                (force_in, force_ref),
                (damage_in, damage_ref),
                (history_in, history_ref),
                (labels_in, labels_ref),
            ]
        )
    ]
    for load in loads:
        load.start()

    for dz, side in ((1, 0), (-1, 1)):
        for dy, low, high in ((0, 0, ly), (1, ly, ly + TILE), (-1, ly + TILE, wide)):

            @pl.when(jnp.logical_not(there(dy, dz)))
            def _():
                zrecv[side, :, low:high] = jnp.zeros((packs, high - low, 128), f32)

    @pl.when(jnp.logical_not(there(1, 0)))
    def _():
        from_up[...] = jnp.zeros(from_up.shape, f32)

    @pl.when(jnp.logical_not(there(-1, 0)))
    def _():
        from_down[...] = jnp.zeros(from_down.shape, f32)

    for load in loads:
        load.wait()

    sign = (1 - 2 * gx).astype(f32)

    def place(q):
        return q + gx * (lx - 1 - 2 * q)

    values = []
    for q in range(lx):
        p = place(q)
        flag = flags_ref[p].astype(f32)
        free = 1.0 - flag
        top = jnp.maximum(history_ref[p], CRACK_HISTORY * labels_ref[p].astype(f32))
        here = [
            free * disp_ref[0, p] * sign,
            free * disp_ref[1, p],
            free * disp_ref[2, p],
            force_ref[0, p] * sign,
            force_ref[1, p],
            force_ref[2, p],
            damage_ref[p],
            top * (free - flag),
        ]
        for f in range(fields):
            own[f, q] = here[f]
        values.append(here)

    sub = lax.broadcasted_iota(jnp.int32, (TILE, 128), 0)

    def spin(a, shift, axis):
        shift = shift % a.shape[axis]
        return pltpu.roll(a, shift, axis) if shift else a

    def spot(f, q):
        return 8 * (f % 4 // 2) + 2 * q + f % 2

    group = lax.broadcasted_iota(jnp.int32, (ly, 128), 1) // 8
    for j in range(packs):
        low = jnp.zeros((ly, 128), f32)
        high = jnp.zeros((ly, 128), f32)
        for f in range(4 * j, 4 * j + 4):
            for q in range(lx):
                k = spot(f, q)
                turned = spin(values[q][f], 8 * k + 8, 1)
                low = jnp.where(group == (k + 1) % 16, turned, low)
                high = jnp.where(group == k, turned, high)
        zsend[0, j] = low
        zsend[1, j] = high
    for j in range(pairs):
        fa, qa = divmod(2 * j, lx)
        fb, qb = divmod(2 * j + 1, lx)
        a, b = values[qa][fa], values[qb][fb]
        down_send[j] = jnp.where(sub < GHOST, a[0:TILE], spin(b[0:TILE], GHOST, 0))
        up_send[j] = jnp.where(sub < GHOST, spin(b[ly - TILE : ly], GHOST, 0), a[ly - TILE : ly])
    for e in range(extras):
        tile = jnp.zeros((TILE, 128), f32)
        for s in range(TILE):
            k, q = divmod(TILE * e + s, lx)
            tile = jnp.where(sub == s, spin(values[q][DEEP[k]][0:TILE], s - GHOST, 0), tile)
        down_send[pairs + e] = tile

    pl.semaphore_wait(barrier, number_near + 1)

    def remote(src, dst, send, recv, k, device):
        return pltpu.make_async_remote_copy(
            src_ref=src, dst_ref=dst, send_sem=send.at[k], recv_sem=recv.at[k],
            device_id=device, device_id_type=MESH,
        )

    def xcopy(src, dst, k):
        return remote(src, dst, xsend_sem, xrecv_sem, k, partner)

    corner_rows = {-1: (0, ly), 1: (ly - TILE, ly + TILE)}

    def halo(dy, dz):
        device = (gx, gy + dy, gz + dz)
        if dz == 0:
            if dy < 0:
                return remote(down_send, from_up, ysend_sem, yrecv_sem, 0, device)
            return remote(up_send, from_down, ysend_sem, yrecv_sem, 1, device)
        side = 0 if dz < 0 else 1
        if dy == 0:
            return remote(
                zsend.at[side], zrecv.at[side, :, 0:ly], zsend_sem, zrecv_sem, side, device
            )
        source, target = corner_rows[dy]
        return remote(
            zsend.at[side, :, source : source + TILE],
            zrecv.at[side, :, target : target + TILE],
            csend_sem, crecv_sem, 2 * side + (dy > 0), device,
        )

    order = [(0, -1), (0, 1), (-1, -1), (1, -1), (-1, 1), (1, 1), (-1, 0), (1, 0)]
    halos = {way: halo(*way) for way in order}
    x_own = xcopy(own, part, 0)
    x_own.start()
    for way in order:
        pl.when(there(*way))(halos[way].start)
    for dy, dz in order[:6]:
        pl.when(there(-dy, -dz))(halos[dy, dz].wait_recv)
    x_z = xcopy(zrecv, zpart, 1)
    x_z.start()
    pl.when(there(1, 0))(halos[-1, 0].wait_recv)
    x_up = xcopy(from_up, part_up, 2)
    x_up.start()
    pl.when(there(-1, 0))(halos[1, 0].wait_recv)
    x_down = xcopy(from_down, part_down, 3)
    x_down.start()

    lane_w = lax.broadcasted_iota(jnp.int32, (wide, 128), 1)
    odd = lane_w // 8 % 2

    def merge(a):
        return jnp.concatenate(
            [a[0:ly], jnp.where(sub < GHOST, a[ly : ly + TILE], a[ly + TILE : wide])], axis=0
        )

    def both_sides(source, f):
        low, high = source[0, f // 4], source[1, f // 4]
        return jnp.where(odd == f % 2, high, low)

    halves = [spin(both_sides(zrecv, f), -8 * spot(f, 0), 1) for f in range(fields)]
    for exchange in (x_own, x_z, x_up, x_down):
        exchange.wait_recv()
    greet(hop_sem)
    for f in range(fields):
        far = both_sides(zpart, f)
        far = -far if f in TURNED else far
        whole = halves[f]
        for q in range(lx):
            at = nx - 1 - q
            whole = jnp.where(lane_w // 16 == at, spin(far, 8 * (2 * at - spot(f, q)), 1), whole)
        if f in DEEP:
            gz_wide[DEEP.index(f)] = whole
        if f not in (0, 1, 2):
            gz_rows[f - 3] = merge(whole)

    def pieces(f, q):
        mine = q < lx
        at = q if mine else nx - 1 - q
        j, half = divmod(f * lx + at, 2)
        above, below = (from_up, from_down) if mine else (part_up, part_down)
        main = own[f, at] if mine else part[f, at]
        return main, above, below, j, half, at, (not mine) and f in TURNED

    def load_wide(f, q):
        main, above, below, j, half, at, turn = pieces(f, q)
        a, b = above[j], below[j]
        if half:
            a, b = spin(a, GHOST, 0), spin(b, GHOST, 0)
        e, s = divmod(DEEP.index(f) * lx + at, TILE)
        a = jnp.where(sub == GHOST, spin(above[pairs + e], GHOST - s, 0), a)
        out = jnp.concatenate([main, a, b], axis=0)
        return -out if turn else out

    def load_rows(f, q):
        main, above, below, j, half, at, turn = pieces(f, q)
        a, b = above[j], below[j]
        ghost = spin(jnp.where(sub < GHOST, b, a), GHOST, 0) if half else jnp.where(sub < GHOST, a, b)
        out = jnp.concatenate([main, ghost], axis=0)
        return -out if turn else out

    row = lax.broadcasted_iota(jnp.int32, (rows, 128), 0)
    lane = lax.broadcasted_iota(jnp.int32, (rows, 128), 1)
    inside = lane % 16
    ypos = gy * ly + jnp.where(row < ly + GHOST, row, row - rows)
    zpos = gz * lz + lane
    zghost = gz * lz + jnp.where(inside < 8, inside - 8, inside + (lz - 8))

    def element_at(pos, count):
        return jnp.where((pos >= 0) & (pos <= count - 2), 1.0, 0.0)

    yvalid = element_at(ypos, ngy * ly)
    valid = yvalid * element_at(zpos, ngz * lz)
    gvalid = jnp.where(lane < 16 * (nx - 1), yvalid * element_at(zghost, ngz * lz), 0.0)

    def y_up(a):
        return pltpu.roll(a, a.shape[0] - 1, 0)

    def y_dn(a):
        return pltpu.roll(a, 1, 0)

    def lanes(a):
        return lane_w if a.shape[0] == wide else lane

    def z_up(a, ghost, p):
        return jnp.where(lanes(a) == 127, spin(ghost, 119 - 16 * p, 1), pltpu.roll(a, 127, 1))

    def z_up_take(acc, a, p):
        return jnp.where(lanes(a) == 16 * p + 7, spin(a, 16 * p + 7, 1), acc)

    def z_dn(a, ghost, p):
        return jnp.where(lanes(a) == 0, spin(ghost, 121 - 16 * p, 1), pltpu.roll(a, 1, 1))

    def z_dn_take(acc, a, p):
        return jnp.where(lanes(a) == 16 * p + 8, spin(a, 16 * p + 9, 1), acc)

    def plane_up(a):
        return pltpu.roll(a, 112, 1)

    def plane_dn(a):
        return pltpu.roll(a, 16, 1)

    blank = jnp.zeros((rows, 128), f32)
    zero = jnp.zeros((TILE, 128), f32)

    def half_back(ss, yd, zd, yz):
        s = (ss - yd) + y_dn(ss + yd)
        d = (zd - yz) + y_dn(zd + yz)
        return s - d, s + d

    def damage_sum(q):
        a = load_wide(6, q)
        s = a + z_up(a, gz_wide[3], q)
        return merge(s + y_up(s)), a

    def rigidity(low, high, mask):
        rest = 1.0 - (low + high) * 0.125
        return (rest * rest + RESIDUAL_STIFFNESS) * mask

    low, a = damage_sum(0)
    taken = z_up_take(pltpu.roll(gz_wide[3], 127, 1), a, 0)
    for q in range(nx - 1):
        high, a = damage_sum(q + 1)
        stiff[q] = rigidity(low, high, valid)
        taken = z_up_take(taken, a, q + 1)
        low = high
    taken = gz_wide[3] + taken
    taken = merge(taken + y_up(taken))
    stiff[GZ] = rigidity(taken, plane_up(taken), gvalid)
    stiff[nx - 1] = blank

    def gather_back(ref, planes, emit):
        ghost = ref[GZ]
        below = blank
        taken = pltpu.roll(ghost, 1, 1)
        for q in range(planes):
            a = ref[q]
            s = a + z_dn(a, ghost, q)
            here = s + y_dn(s)
            emit(q, below + here)
            below = here
            taken = z_dn_take(taken, a, q)
        s = ghost + taken
        s = s + y_dn(s)
        emit(GZ, s + plane_dn(s))

    def inv_emit(q, total):
        free = (gz_rows[4] if q == GZ else load_rows(7, q)) > 0.0
        inverse[q] = jnp.where(free, 1.0 / jnp.where(free, stiff_diag * total, 1.0), 0.0)

    gather_back(stiff, nx, inv_emit)

    def forward(u, near_u, keep):
        zs, zd = u + near_u, near_u - u
        a, b = keep(y_up(zs)), keep(y_up(zd))
        zs, zd = keep(zs), keep(zd)
        return zs + a, a - zs, zd + b, b - zd

    def same(a):
        return a

    def pass_one(load, planes, keep, height, with_ghost):
        for c in range(3):
            ghost = load(c, GZ)
            taken = pltpu.roll(ghost, 127, 1)
            for q in range(planes):
                u = load(c, q)
                out = forward(u, z_up(u, ghost, q), keep)
                for m in range(4):
                    modes[4 * c + m, q, 0:height] = out[m][0:height]
                if with_ghost:
                    taken = z_up_take(taken, u, q)
            if with_ghost:
                out = forward(ghost, taken, keep)
                for m in range(4):
                    modes[4 * c + m, GZ] = out[m]

    def sm(mode_a, comp_a, mode_b, comp_b):
        return float(stiff_modes[3 * mode_a + comp_a, 3 * mode_b + comp_b])

    k_lame = sm(4, 0, 2, 1)
    k_two = sm(4, 0, 4, 0) - k_lame
    k_shear = sm(2, 0, 2, 0)
    k_twist = sm(3, 0, 5, 1)
    k_bend = sm(3, 1, 3, 1)
    k_cross = sm(3, 1, 5, 0)
    k_last = sm(7, 0, 7, 0)

    def element(low, high, g, energy_at):
        S = [low[m] + high[m] if m % 4 else None for m in range(12)]
        D = [high[m] - low[m] for m in range(12)]
        xX, xXY, xXZ, xXYZ = D[0:4]
        yX, yXY, yXZ, yXYZ = D[4:8]
        zX, zXY, zXZ, zXYZ = D[8:12]
        _, xY, xZ, xYZ = S[0:4]
        _, yY, yZ, yYZ = S[4:8]
        _, zY, zZ, zYZ = S[8:12]
        div = xX + yY + zZ
        sxy, sxz, syz = xY + yX, xZ + zX, yZ + zY
        if energy_at is not None:
            trace = 0.25 * div
            tens = jnp.maximum(trace, 0.0)
            third = trace / 3.0
            ex, ey, ez = 0.25 * xX - third, 0.25 * yY - third, 0.25 * zZ - third
            dev = ex * ex + ey * ey + ez * ez
            she = (sxy * sxy + sxz * sxz + syz * syz) * 0.0625
            energy = 0.5 * BULK_MODULUS * tens * tens + LAME_MU * (dev + 0.5 * she)
            hist[energy_at] = jnp.where(g > 0.0, energy, 0.0)
        gl, g2, gs = k_lame * g, k_two * g, k_shear * g
        gt, gb, gc, g3 = k_twist * g, k_bend * g, k_cross * g, k_last * g
        pressure = gl * div
        fxX, fyY, fzZ = pressure + g2 * xX, pressure + g2 * yY, pressure + g2 * zZ
        txy, txz, tyz = gs * sxy, gs * sxz, gs * syz
        tw = xYZ + yXZ + zXY
        fxYZ, fyXZ, fzXY = gt * (xYZ + tw), gt * (yXZ + tw), gt * (zXY + tw)
        fyYZ, fxXZ = gb * yYZ + gc * xXZ, gb * xXZ + gc * yYZ
        fzYZ, fxXY = gb * zYZ + gc * xXY, gb * xXY + gc * zYZ
        fyXY, fzXZ = gb * yXY + gc * zXZ, gb * zXZ + gc * yXY
        FD = [
            fxX, fxXY, fxXZ, g3 * xXYZ,
            txy, fyXY, fyXZ, g3 * yXYZ,
            txz, fzXY, fzXZ, g3 * zXYZ,
        ]
        FS = [
            None, txy, txz, fxYZ,
            None, fyY, tyz, fyYZ,
            None, tyz, fzZ, fzYZ,
        ]
        lows = [(-FD[m]) if FS[m] is None else FS[m] - FD[m] for m in range(12)]
        highs = [FD[m] if FS[m] is None else FS[m] + FD[m] for m in range(12)]
        return lows, highs

    def element_pass(layers, energies, to_end):
        def step(chunk, carry):
            r = pl.ds(pl.multiple_of(chunk * TILE, TILE), TILE)
            low = [modes[m, 0, r, :] for m in range(12)]
            held = None
            for p in range(layers):
                high = [modes[m, p + 1, r, :] for m in range(12)]
                lows, highs = element(
                    low, high, stiff[p, r, :], (p, r, slice(None)) if p < energies else None
                )
                for m in range(12):
                    modes[m, p, r, :] = lows[m] + held[m] if p else lows[m]
                held, low = highs, high
            if to_end:
                for m in range(12):
                    modes[m, layers, r, :] = held[m]
            low = [modes[m, GZ, r, :] for m in range(12)]
            lows, highs = element(
                low, [plane_up(a) for a in low], stiff[GZ, r, :],
                (GZ, r, slice(None)) if energies else None,
            )
            for m in range(12):
                modes[m, GZ, r, :] = lows[m] + plane_dn(highs[m])
            return carry

        lax.fori_loop(0, rows // TILE, step, 0, unroll=True)

    def each_node(planes, emit, carry):
        ghosts = [half_back(*(modes[4 * c + m, GZ] for m in range(4))) for c in range(3)]
        taken = [pltpu.roll(g[1], 1, 1) for g in ghosts]
        for q in range(planes):
            got = []
            for c in range(3):
                near_w, far_w = half_back(*(modes[4 * c + m, q] for m in range(4)))
                got.append(near_w + z_dn(far_w, ghosts[c][1], q))
                taken[c] = z_dn_take(taken[c], far_w, q)
            carry = emit(q, got, carry)
        emit(GZ, [ghosts[c][0] + taken[c] for c in range(3)], carry)
        return carry

    def fold(a):
        total = a[0:TILE]
        for i in range(TILE, ly, TILE):
            total = total + a[i : i + TILE]
        return total

    nd, ng = DISP_ITERS, DMG_ITERS
    gram, vector = {}, {}

    def load_start(c, q):
        return gz_wide[c] if q == GZ else load_wide(c, q)

    pass_one(load_start, nx, merge, rows, True)
    element_pass(nx - 1, lx + ng, True)

    def start_emit(q, got, dot):
        inv = inverse[q]
        for c in range(3):
            force = gz_rows[c] if q == GZ else load_rows(3 + c, q)
            r = force - got[c]
            v = inv * r
            basis[c, q] = v
            if q < lx:
                resid[c, q] = r[0:ly]
                dot = dot + fold((v * r)[0:ly])
        return dot

    vector[0] = each_node(nx, start_emit, zero)

    def hist_emit(q, total):
        top = gz_rows[4] if q == GZ else load_rows(7, q)
        react[q] = jnp.maximum(jnp.abs(top), 0.125 * total)

    gather_back(hist, lx + ng, hist_emit)

    for k in range(nd - 1):
        planes = lx + nd - 1 - k
        pass_one(lambda c, q, k=k: basis[3 * k + c, q], planes + 1, same, rows, True)
        element_pass(planes, 0, False)

        def apply_emit(q, got, carry, k=k):
            carry = list(carry)
            inv = inverse[q] * (2.0 / SPECTRUM)
            for c in range(3):
                w = got[c]
                here = basis[3 * k + c, q]
                v = inv * w - here
                if k:
                    v = 2.0 * v - basis[3 * (k - 1) + c, q]
                basis[3 * (k + 1) + c, q] = v
                if q < lx:
                    wi, vi = w[0:ly], v[0:ly]
                    if k + 2 < nd:
                        images[3 * k + c, q] = wi
                    carry[0] = carry[0] + fold(here[0:ly] * wi)
                    carry[1] = carry[1] + fold(vi * resid[c, q])
                    carry[2] = carry[2] + fold(vi * wi)
                    for j in range(k):
                        carry[3 + j] = carry[3 + j] + fold(vi * images[3 * j + c, q])
            return tuple(carry)

        got = each_node(planes, apply_emit, (zero,) * (3 + k))
        gram[k, k], vector[k + 1], gram[k + 1, k] = got[:3]
        for j in range(k):
            gram[k + 1, j] = got[3 + j]

    def last_energy():
        pass_one(lambda c, q: basis[3 * (nd - 1) + c, q], lx + 1, same, ly, False)
        total, middle = zero, zero
        for chunk in range(ly // TILE):
            r = slice(TILE * chunk, TILE * chunk + TILE)
            low = [modes[m, 0, r, :] for m in range(12)]
            for p in range(lx):
                high = [modes[m, p + 1, r, :] for m in range(12)]
                S = [low[m] + high[m] if m % 4 else None for m in range(12)]
                D = [high[m] - low[m] for m in range(12)]
                xX, xXY, xXZ, xXYZ = D[0:4]
                yX, yXY, yXZ, yXYZ = D[4:8]
                zX, zXY, zXZ, zXYZ = D[8:12]
                _, xY, xZ, xYZ = S[0:4]
                _, yY, yZ, yYZ = S[4:8]
                _, zY, zZ, zYZ = S[8:12]
                div = xX + yY + zZ
                sxy, sxz, syz = xY + yX, xZ + zX, yZ + zY
                tw = xYZ + yXZ + zXY
                sum_two = xX * xX + yY * yY + zZ * zZ
                sum_shear = sxy * sxy + sxz * sxz + syz * syz
                sum_twist = xYZ * xYZ + yXZ * yXZ + zXY * zXY + tw * tw
                sum_bend = (yYZ * yYZ + xXZ * xXZ) + (zYZ * zYZ + xXY * xXY) + (yXY * yXY + zXZ * zXZ)
                sum_cross = yYZ * xXZ + zYZ * xXY + yXY * zXZ
                sum_last = xXYZ * xXYZ + yXYZ * yXYZ + zXYZ * zXYZ
                energy = (
                    (k_lame * (div * div) + k_two * sum_two)
                    + (k_shear * sum_shear + k_twist * sum_twist)
                    + (k_bend * sum_bend + (2.0 * k_cross) * sum_cross)
                    + k_last * sum_last
                ) * stiff[p, r, :]
                if p + 1 < lx:
                    total = total + energy
                else:
                    middle = middle + energy
                low = high
        return total + 0.5 * middle

    gram[nd - 1, nd - 1] = last_energy()

    cy = yvalid + element_at(ypos - 1, ngy * ly)
    cz = element_at(zpos, ngz * lz) + element_at(zpos - 1, ngz * lz)
    czg = element_at(zghost, ngz * lz) + element_at(zghost - 1, ngz * lz)
    cxg = jnp.where((lane < 16) | (lane >= 16 * (nx - 1)), 1.0, 2.0)
    node = jnp.where(cy * cz > 0.0, 1.0, 0.0)
    gnode = jnp.where(cy * czg > 0.0, 1.0, 0.0)
    diag_scale = laplace_diag * TOUGHNESS * LENGTH_SCALE
    lap_scale = TOUGHNESS * LENGTH_SCALE / 36.0

    def lines(d, after, before, count_z):
        s, n = after + before, count_z * d
        mass, slope = 2.0 * n + s, n - s
        s, n = y_up(mass) + y_dn(mass), cy * mass
        both = 2.0 * n + s
        mixed = (n - s) + (2.0 * (cy * slope) + (y_up(slope) + y_dn(slope)))
        return 2.0 * mixed + both, mixed - both

    def laplace_pass(load, planes, emit, carry, with_ghost):
        ghost = load(GZ)
        after = pltpu.roll(ghost, 127, 1)
        before = pltpu.roll(ghost, 1, 1)
        reach = planes + 1 if planes < nx else nx
        ahead = []
        for q in range(reach):
            d = load(q)
            ahead.append(lines(d, z_up(d, ghost, q), z_dn(d, ghost, q), cz))
            if with_ghost:
                after = z_up_take(after, d, q)
                before = z_dn_take(before, d, q)
            p = q - 1
            if p >= 0:
                total = ahead[p][0] if p == 0 else 2.0 * ahead[p][0] + ahead[p - 1][1]
                carry = emit(p, lap_scale * (total + ahead[q][1]), carry)
        if with_ghost:
            inner, outer = lines(ghost, after, before, czg)
            total = cxg * inner + jnp.where(lane >= 16, plane_dn(outer), 0.0)
            total = total + jnp.where(lane < 16 * (nx - 1), plane_up(outer), 0.0)
            emit(GZ, lap_scale * total, carry)
        return carry

    def reaction_of(q):
        return TOUGHNESS / LENGTH_SCALE + 2.0 * react[q]

    def old_damage(q):
        return gz_rows[3] if q == GZ else load_rows(6, q)

    def dstart(q, lap, dot):
        reaction = reaction_of(q)
        if q == GZ:
            count, mask = cxg * cy * czg, gnode
        else:
            count, mask = (cy * cz if q == 0 else 2.0 * cy * cz), node
        inv = mask / (diag_scale * count + reaction)
        dinverse[q] = inv
        r = 2.0 * react[q] - (lap + reaction * old_damage(q))
        v = inv * r
        dbasis[0, q] = v
        if q < lx:
            dresid[q] = r[0:ly]
            dot = dot + fold((v * r)[0:ly])
        return dot

    dvector, dgram = {}, {}
    dvector[0] = laplace_pass(old_damage, lx + ng, dstart, zero, True)
    dimages = {}
    for k in range(ng):
        more = k + 1 < ng

        def dstep(q, lap, carry, k=k, more=more):
            carry = list(carry)
            here = dbasis[k, q]
            w = lap + reaction_of(q) * here
            if q < lx:
                carry[0] = carry[0] + fold((here * w)[0:ly])
            if more:
                v = dinverse[q] * w - here
                if k:
                    v = 2.0 * v - dbasis[k - 1, q]
                dbasis[k + 1, q] = v
                if q < lx:
                    carry[1] = carry[1] + fold(v[0:ly] * dresid[q])
                    carry[2] = carry[2] + fold((v * w)[0:ly])
            return tuple(carry)

        got = laplace_pass(
            lambda q, k=k: dbasis[k, q], lx + ng - 1 - k, dstep, (zero,) * (3 if more else 1), more
        )
        dgram[k, k] = got[0]
        if more:
            dvector[k + 1], dgram[k + 1, k] = got[1:]

    parts = [vector[i] for i in range(nd)] + [dvector[i] for i in range(ng)]
    parts += [gram[i, j] for i in range(nd) for j in range(i + 1)]
    parts += [dgram[i, j] for i in range(ng) for j in range(i + 1)]
    at = lax.broadcasted_iota(jnp.int32, (1, 128), 1)
    packed = jnp.zeros((1, 128), f32)
    for i, piece in enumerate(parts):
        line = jnp.sum(piece, axis=0, keepdims=True)
        packed = jnp.where(at == i, jnp.sum(line, axis=1, keepdims=True), packed)
    mine = gx * npeer + me
    sums[mine] = packed
    pl.semaphore_wait(hop_sem, number_near)

    def peer_copy(side, o, slot):
        q = lax.rem(me + o, npeer)
        k = side * npeer + o
        return remote(
            sums.at[mine], sums.at[slot], asend_sem, arecv_sem, k,
            (gx if side == 0 else 1 - gx, q // ngz, lax.rem(q, ngz)),
        )

    peers = [(side, o) for o in range(npeer) for side in (0, 1) if side or o]
    sends = [peer_copy(side, o, mine) for side, o in peers]
    for s in sends:
        s.start()
    for q in range(lx):
        out_history[place(q)] = react[q, 0:ly]
    for side, o in peers:
        from_x = gx if side == 0 else 1 - gx
        peer_copy(side, o, from_x * npeer + lax.rem(me + npeer - o, npeer)).wait_recv()
    layer = [sums[i] for i in range(2 * npeer)]
    while len(layer) > 1:
        layer = [a + b for a, b in zip(layer[::2], layer[1::2])] + layer[len(layer) & ~1 :]
    whole = layer[0]

    scalars = [
        jnp.sum(jnp.where(at == i, whole, 0.0), axis=1, keepdims=True) for i in range(len(parts))
    ]

    def solve(rhs, lower):
        n = len(rhs)
        A = [[lower[max(i, j)][min(i, j)] for j in range(n)] for i in range(n)]
        b = list(rhs)
        for i in range(n):
            pivot = 1.0 / A[i][i]
            for r in range(i + 1, n):
                ratio = A[r][i] * pivot
                for c in range(i + 1, n):
                    A[r][c] = A[r][c] - ratio * A[i][c]
                b[r] = b[r] - ratio * b[i]
        out = [None] * n
        for i in reversed(range(n)):
            s = b[i]
            for j in range(i + 1, n):
                s = s - A[i][j] * out[j]
            out[i] = s / A[i][i]
        return out

    def triangle(flat, n):
        return [[flat[k * (k + 1) // 2 + j] for j in range(k + 1)] for k in range(n)]

    rest = scalars[nd + ng :]
    cut = nd * (nd + 1) // 2
    weights = solve(scalars[:nd], triangle(rest[:cut], nd))
    dweights = solve(scalars[nd : nd + ng], triangle(rest[cut:], ng))
    for q in range(lx):
        p = place(q)
        for c in range(3):
            x = own[c, q]
            for k in range(nd):
                x = x + weights[k] * basis[3 * k + c, q, 0:ly]
            out_disp[c, p] = sign * x if c == 0 else x
        d = own[6, q]
        for k in range(ng):
            d = d + dweights[k] * dbasis[k, q, 0:ly]
        out_damage[p] = d

    for way in order:
        pl.when(there(*way))(halos[way].wait_send)
    for exchange in (x_own, x_z, x_up, x_down):
        exchange.wait_send()
    for s in sends:
        s.wait_send()


def hand_on(*refs):
    for source, target in zip(refs[:3], refs[3:]):
        target[...] = source[...]


def body_fused(sizes, *arrays):
    ngy, ngz, lx, ly, lz = sizes
    nx, rows, wide, fields = 2 * lx, ly + TILE, ly + 2 * TILE, 8
    packs, pairs, extras = fields * lx // 16, fields * lx // 2, len(DEEP) * lx // TILE
    npeer = ngy * ngz
    f32 = jnp.float32
    planes = (nx + 1, rows, lz)
    vmem = pl.BlockSpec(memory_space=pltpu.VMEM)
    hbm = pl.BlockSpec(memory_space=pltpu.HBM)
    dma = pltpu.SemaphoreType.DMA

    def room(*shape):
        return pltpu.VMEM(shape, f32)

    results = pl.pallas_call(
        functools.partial(kernel, sizes),
        out_shape=(
            jax.ShapeDtypeStruct((3, lx, ly, lz), f32),
            jax.ShapeDtypeStruct((lx, ly, lz), f32),
            jax.ShapeDtypeStruct((lx, ly, lz), f32),
        ),
        in_specs=[hbm] * 6,
        out_specs=(vmem,) * 3,
        scratch_shapes=[
            room(3, lx, ly, lz),
            room(3, lx, ly, lz),
            room(lx, ly, lz),
            room(lx, ly, lz),
            pltpu.VMEM((lx, ly, lz), jnp.int32),
            pltpu.VMEM((lx, ly, lz), jnp.int32),
            room(fields, lx, ly, lz),
            room(fields, lx, ly, lz),
            room(pairs + extras, TILE, 128),
            room(pairs, TILE, 128),
            room(pairs + extras, TILE, 128),
            room(pairs, TILE, 128),
            room(pairs + extras, TILE, 128),
            room(pairs, TILE, 128),
            room(2, packs, ly, 128),
            room(2, packs, wide, 128),
            room(2, packs, wide, 128),
            room(4, wide, 128),
            room(5, rows, 128),
            room(12, *planes),
            room(3 * DISP_ITERS, *planes),
            room(3 * (DISP_ITERS - 2), lx, ly, lz),
            room(3, lx, ly, lz),
            room(*planes),
            room(*planes),
            room(*planes),
            room(*planes),
            room(*planes),
            room(DMG_ITERS, *planes),
            room(lx, ly, lz),
            room(2 * npeer, 1, 128),
            dma((6,)),
            dma((2,)),
            dma((2,)),
            dma((2,)),
            dma((2,)),
            dma((4,)),
            dma((4,)),
            dma((4,)),
            dma((4,)),
            dma((2 * npeer,)),
            dma((2 * npeer,)),
            pltpu.SemaphoreType.REGULAR,
        ],
        compiler_params=pltpu.CompilerParams(
            collective_id=0, has_side_effects=True, vmem_limit_bytes=VMEM_LIMIT
        ),
    )(*arrays)
    return pl.pallas_call(
        hand_on,
        out_shape=tuple(jax.ShapeDtypeStruct(r.shape, f32) for r in results),
        in_specs=[vmem] * 3,
        out_specs=(vmem,) * 3,
    )(*results)


VMEM_LIMIT = 60 * 1024 * 1024


def solution(mesh):
    shape = dict(mesh.shape)

    def body(*arrays):
        lx, ly, lz = arrays[2].shape
        fits = shape["gx"] == 2 and shape["gy"] * shape["gz"] > 1
        fits = fits and max(shape["gy"], shape["gz"]) <= 4
        fits = fits and lx == 4 and ly % 8 == 0 and lz == 128
        if fits:
            return body_fused((shape["gy"], shape["gz"], lx, ly, lz), *arrays)
        return body_any_mesh(*arrays)

    return jax.shard_map(
        body,
        mesh=mesh,
        in_specs=(
            P(None, "gx", "gy", "gz"),
            P(None, "gx", "gy", "gz"),
            P("gx", "gy", "gz"),
            P("gx", "gy", "gz"),
            P("gx", "gy", "gz"),
            P("gx", "gy", "gz"),
        ),
        out_specs=(P(None, "gx", "gy", "gz"), P("gx", "gy", "gz"), P("gx", "gy", "gz")),
        check_vma=False,
    )
```

```python
import functools
import jax
import jax.numpy as jnp
import numpy as np
from jax import lax
from jax.experimental import pallas as pl
from jax.experimental.pallas import tpu as pltpu
from jax.sharding import PartitionSpec as P

DISP_ITERS = 4
DMG_ITERS = 2


LAME_LAMBDA = 0.5769230769230769
LAME_MU = 0.38461538461538464
BULK_MODULUS = LAME_LAMBDA + 2.0 * LAME_MU / 3.0
RESIDUAL_STIFFNESS = 0.001
TOUGHNESS = 1.0
LENGTH_SCALE = 2.0
CRACK_HISTORY = 40.0


def padded_2(cells, sides, width):
    for axis, dim in sides:
        count = lax.axis_size(axis)
        ends = count - 1
        head = lax.slice_in_dim(cells, 0, width, axis=dim)
        tail = lax.slice_in_dim(cells, cells.shape[dim] - width, cells.shape[dim], axis=dim)
        cells = jnp.concatenate(
            [
                lax.ppermute(tail, axis, [(i, (i + 1) % count) for i in range(ends)]),
                cells,
                lax.ppermute(head, axis, [((i + 1) % count, i) for i in range(ends)]),
            ],
            axis=dim,
        )
    return cells


def corner_offsets(corner):
    return (corner >> 2 & 1, corner >> 1 & 1, corner & 1)


def shape_gradients(sample):
    gradient = np.zeros((3, 8))
    for corner in range(8):
        offsets = corner_offsets(corner)
        values = [sample[k] if offsets[k] else 1.0 - sample[k] for k in range(3)]
        slopes = [1.0 if offsets[k] else -1.0 for k in range(3)]
        gradient[0, corner] = slopes[0] * values[1] * values[2]
        gradient[1, corner] = values[0] * slopes[1] * values[2]
        gradient[2, corner] = values[0] * values[1] * slopes[2]
    return gradient


def strain_matrix(gradient):
    strain = np.zeros((6, 24))
    for corner in range(8):
        column = 3 * corner
        strain[0, column] = gradient[0, corner]
        strain[1, column + 1] = gradient[1, corner]
        strain[2, column + 2] = gradient[2, corner]
        strain[3, column] = gradient[1, corner]
        strain[3, column + 1] = gradient[0, corner]
        strain[4, column + 1] = gradient[2, corner]
        strain[4, column + 2] = gradient[1, corner]
        strain[5, column] = gradient[2, corner]
        strain[5, column + 2] = gradient[0, corner]
    return strain


def element_tables():
    moduli = np.zeros((6, 6))
    moduli[:3, :3] = LAME_LAMBDA
    for k in range(3):
        moduli[k, k] += 2.0 * LAME_MU
        moduli[k + 3, k + 3] = LAME_MU
    points = [0.5 - 0.5 / np.sqrt(3.0), 0.5 + 0.5 / np.sqrt(3.0)]
    stiff_table = np.zeros((24, 24))
    laplace_table = np.zeros((8, 8))
    for sample_index in range(8):
        sample = tuple((points[k] for k in corner_offsets(sample_index)))
        gradient = shape_gradients(sample)
        strain = strain_matrix(gradient)
        stiff_table += 0.125 * strain.T @ moduli @ strain
        laplace_table += 0.125 * gradient.T @ gradient
    centre_table = strain_matrix(shape_gradients((0.5, 0.5, 0.5)))
    return (
        stiff_table.astype(np.float32),
        laplace_table.astype(np.float32),
        centre_table.astype(np.float32),
    )


def corner_views(padded, element_shape):
    corner_list = []
    for corner in range(8):
        offx, offy, offz = corner_offsets(corner)
        corner_list.append(
            padded[
                ...,
                offx : offx + element_shape[0],
                offy : offy + element_shape[1],
                offz : offz + element_shape[2],
            ]
        )
    return corner_list


def assemble_nodes(pieces):
    running = None
    for corner in range(8):
        offx, offy, offz = corner_offsets(corner)
        leading = [(0, 0)] * (pieces[corner].ndim - 3)
        placed = jnp.pad(
            pieces[corner], leading + [(offx, 1 - offx), (offy, 1 - offy), (offz, 1 - offz)]
        )
        running = placed if running is None else running + placed
    return running


def line_valid(position, devices, count):
    index = position * count + jnp.arange(count + 1, dtype=jnp.int32) - 1
    return ((index >= 0) & (index <= devices * count - 2)).astype(jnp.float32)


def strain_energy(strain):
    trace = strain[0] + strain[1] + strain[2]
    deviator = strain[:3] - trace[None] / 3.0
    shear = strain[3:]
    tensile = jnp.maximum(trace, 0.0)
    return 0.5 * BULK_MODULUS * tensile * tensile + LAME_MU * (
        jnp.sum(deviator * deviator, axis=0) + 0.5 * jnp.sum(shear * shear, axis=0)
    )


def forces_to_nodes(forces, stiffness):
    pieces = [stiffness[None] * forces[3 * target : 3 * target + 3] for target in range(8)]
    return assemble_nodes(pieces)


def element_apply(padded, stiffness, stiff_table):
    element_shape = stiffness.shape
    flat = jnp.stack(corner_views(padded, element_shape)).reshape(24, -1)
    forces = jnp.dot(stiff_table, flat, precision=lax.Precision.HIGHEST).reshape(
        (24,) + element_shape
    )
    return forces_to_nodes(forces, stiffness)


def laplace_apply(padded, element_valid, laplace_table):
    element_shape = element_valid.shape
    flat = jnp.stack(corner_views(padded, element_shape)).reshape(8, -1)
    forces = jnp.dot(laplace_table, flat, precision=lax.Precision.HIGHEST).reshape(
        (8,) + element_shape
    )
    return assemble_nodes([element_valid * forces[target] for target in range(8)])


def single_pair(pair):
    return tuple(lax.psum(pair, ("gx", "gy", "gz")))


def conjugate(solutions, residuals, inverses, counts, apply_fn):
    solutions = list(solutions)
    residuals = list(residuals)
    number = len(solutions)
    steps = max(counts)

    def pair_totals(pairs):
        return [single_pair(pairs[0])]

    precs = [inverses[0] * residuals[0]]
    applied = apply_fn(precs, list(range(number)))
    pairs = pair_totals([(jnp.sum(residuals[0] * precs[0]), jnp.sum(precs[0] * applied[0]))])
    norms = [pair[0] for pair in pairs]
    lengths = [pair[0] / pair[1] for pair in pairs]
    directions = list(precs)
    alongs = list(applied)
    for step in range(steps):
        active = [i for i in range(number) if step < counts[i]]
        for i in active:
            solutions[i] = solutions[i] + lengths[i] * directions[i]
            residuals[i] = residuals[i] - lengths[i] * alongs[i]
        later = [i for i in active if step + 1 < counts[i]]
        if later:
            i = later[0]
            precs[i] = inverses[i] * residuals[i]
            images = apply_fn([precs[i] for i in later], later)
            pairs = pair_totals(
                [
                    (jnp.sum(residuals[i] * precs[i]), jnp.sum(precs[i] * images[k]))
                    for k, i in enumerate(later)
                ]
            )
            for k, i in enumerate(later):
                norm_next, curve_sum = pairs[k]
                ratio = norm_next / norms[i]
                lengths[i] = norm_next / (curve_sum - ratio * norm_next / lengths[i])
                directions[i] = precs[i] + ratio * directions[i]
                alongs[i] = images[k] + ratio * alongs[i]
                norms[i] = norm_next
    return solutions


def body_any_mesh(displacement_start, external_force, damage_old, history_old, crack_labels, fixed_flags):
    tables = element_tables()
    stiff_table = jnp.asarray(tables[0], jnp.float32)
    laplace_table = jnp.asarray(tables[1], jnp.float32)
    centre_table = jnp.asarray(tables[2], jnp.float32)
    highest = lax.Precision.HIGHEST
    size_x, size_y, size_z = damage_old.shape
    free_mask = 1.0 - fixed_flags.astype(jnp.float32)
    start_disp = displacement_start * free_mask[None]
    element_valid = (
        line_valid(lax.axis_index("gx"), lax.axis_size("gx"), size_x)[:, None, None]
        * line_valid(lax.axis_index("gy"), lax.axis_size("gy"), size_y)[None, :, None]
        * line_valid(lax.axis_index("gz"), lax.axis_size("gz"), size_z)[None, None, :]
    )
    element_shape = element_valid.shape
    start_pad = padded_2(
        jnp.concatenate([start_disp, damage_old[None]], axis=0),
        (("gx", 1), ("gy", 2), ("gz", 3)),
        1,
    )
    corner_list = corner_views(start_pad, element_shape)
    damage_mean = sum((view[3] for view in corner_list)) / 8.0
    stiffness = ((1.0 - damage_mean) ** 2 + RESIDUAL_STIFFNESS) * element_valid
    flat = jnp.stack([view[:3] for view in corner_list]).reshape(24, -1)
    combined = jnp.dot(
        jnp.concatenate([stiff_table, centre_table], axis=0), flat, precision=highest
    )
    forces = combined[:24].reshape((24,) + element_shape)
    strain = combined[24:].reshape((6,) + element_shape)
    start_image = forces_to_nodes(forces, stiffness)[:, 1:-1, 1:-1, 1:-1]
    energy = strain_energy(strain) * element_valid
    nodal_energy = assemble_nodes([energy] * 8)[1:-1, 1:-1, 1:-1] / 8.0
    history = jnp.maximum(
        jnp.maximum(history_old, nodal_energy), CRACK_HISTORY * crack_labels.astype(jnp.float32)
    )
    stiff_diag = jnp.diagonal(stiff_table)
    diag_pieces = [
        stiffness[None] * stiff_diag[3 * target : 3 * target + 3][:, None, None, None]
        for target in range(8)
    ]
    elastic_diag = assemble_nodes(diag_pieces)[:, 1:-1, 1:-1, 1:-1]
    inverse_elastic = 1.0 / (free_mask[None] * elastic_diag + (1.0 - free_mask[None]))

    def constrained(nodal_field):
        masked = free_mask[None] * nodal_field
        padded = padded_2(masked, (("gx", 1), ("gy", 2), ("gz", 3)), 1)
        nodes = element_apply(padded, stiffness, stiff_table)[:, 1:-1, 1:-1, 1:-1]
        return free_mask[None] * nodes + (1.0 - free_mask[None]) * nodal_field

    reaction = TOUGHNESS / LENGTH_SCALE + 2.0 * history
    laplace_diag = assemble_nodes(
        [element_valid * laplace_table[target, target] for target in range(8)]
    )[1:-1, 1:-1, 1:-1]
    inverse_damage = 1.0 / (TOUGHNESS * LENGTH_SCALE * laplace_diag + reaction)
    residual = free_mask[None] * (external_force - start_image)
    start_lap = laplace_apply(start_pad[3], element_valid, laplace_table)[1:-1, 1:-1, 1:-1]
    damage_residual = 2.0 * history - (TOUGHNESS * LENGTH_SCALE * start_lap + reaction * damage_old)

    def damage_operator(nodal_field):
        padded = padded_2(nodal_field, (("gx", 0), ("gy", 1), ("gz", 2)), 1)
        lap_nodes = laplace_apply(padded, element_valid, laplace_table)[1:-1, 1:-1, 1:-1]
        return TOUGHNESS * LENGTH_SCALE * lap_nodes + reaction * nodal_field

    def single_elastic(fields, active):
        return [constrained(fields[0])]

    def single_damage(fields, active):
        return [damage_operator(fields[0])]

    displacement = conjugate(
        [start_disp], [residual], [inverse_elastic], [DISP_ITERS], single_elastic
    )[0]
    damage = conjugate(
        [damage_old], [damage_residual], [inverse_damage], [DMG_ITERS], single_damage
    )[0]
    return (displacement, damage, history)


SPECTRUM = 3.2
TILE = 8
GHOST = 4
DEEP = (0, 1, 2, 6)
TURNED = (0, 3)
MESH = pl.DeviceIdType.MESH


def walsh_tables():
    stiff, laplace, _ = element_tables()
    signs = np.array(
        [
            [np.prod([1.0 if c >> k & 1 else (-1.0 if m >> k & 1 else 1.0) for k in range(3)]) for c in range(8)]
            for m in range(8)
        ]
    )
    wide = np.kron(signs, np.eye(3))
    stiff_modes = wide @ stiff.astype(np.float64) @ wide.T / 64.0
    return stiff_modes, float(stiff[0, 0]), float(laplace[0, 0])


def kernel(
    sizes,
    disp_in,
    force_in,
    damage_in,
    history_in,
    labels_in,
    flags_in,
    out_disp,
    out_damage,
    out_history,
    disp_ref,
    force_ref,
    damage_ref,
    history_ref,
    labels_ref,
    flags_ref,
    own,
    part,
    down_send,
    up_send,
    from_up,
    from_down,
    part_up,
    part_down,
    zsend,
    zrecv,
    zpart,
    gz_wide,
    gz_rows,
    modes,
    basis,
    images,
    resid,
    stiff,
    inverse,
    hist,
    react,
    dinverse,
    dbasis,
    dresid,
    sums,
    in_sem,
    ysend_sem,
    yrecv_sem,
    zsend_sem,
    zrecv_sem,
    csend_sem,
    crecv_sem,
    xsend_sem,
    xrecv_sem,
    asend_sem,
    arecv_sem,
    hop_sem,
):
    ngy, ngz, lx, ly, lz = sizes
    nx = 2 * lx
    fields = 8
    npeer = ngy * ngz
    pairs = fields * lx // 2
    packs = fields * lx // 16
    extras = len(DEEP) * lx // TILE
    wide, rows = ly + 2 * TILE, ly + TILE
    GZ = nx
    f32 = jnp.float32
    stiff_modes, stiff_diag, laplace_diag = walsh_tables()
    gx, gy, gz = lax.axis_index("gx"), lax.axis_index("gy"), lax.axis_index("gz")
    me = gy * ngz + gz
    partner = (1 - gx, gy, gz)

    def there(dy, dz):
        y, z = gy + dy, gz + dz
        return (y >= 0) & (y < ngy) & (z >= 0) & (z < ngz)

    near = [(dy, dz) for dy in (-1, 0, 1) for dz in (-1, 0, 1) if dy or dz]
    number_near = sum(there(dy, dz).astype(jnp.int32) for dy, dz in near)

    barrier = pltpu.get_barrier_semaphore()

    def greet(semaphore):
        for dy, dz in near:

            @pl.when(there(dy, dz))
            def _():
                pl.semaphore_signal(
                    semaphore, inc=1, device_id=(gx, gy + dy, gz + dz), device_id_type=MESH
                )

    greet(barrier)
    pl.semaphore_signal(barrier, inc=1, device_id=partner, device_id_type=MESH)

    loads = [
        pltpu.make_async_copy(source, target, in_sem.at[i])
        for i, (source, target) in enumerate(
            [
                (flags_in, flags_ref),
                (disp_in, disp_ref),
                (force_in, force_ref),
                (damage_in, damage_ref),
                (history_in, history_ref),
                (labels_in, labels_ref),
            ]
        )
    ]
    for load in loads:
        load.start()

    for dz, side in ((1, 0), (-1, 1)):
        for dy, low, high in ((0, 0, ly), (1, ly, ly + TILE), (-1, ly + TILE, wide)):

            @pl.when(jnp.logical_not(there(dy, dz)))
            def _():
                zrecv[side, :, low:high] = jnp.zeros((packs, high - low, 128), f32)

    @pl.when(jnp.logical_not(there(1, 0)))
    def _():
        from_up[...] = jnp.zeros(from_up.shape, f32)

    @pl.when(jnp.logical_not(there(-1, 0)))
    def _():
        from_down[...] = jnp.zeros(from_down.shape, f32)

    for load in loads:
        load.wait()

    sign = (1 - 2 * gx).astype(f32)

    def place(q):
        return q + gx * (lx - 1 - 2 * q)

    values = []
    for q in range(lx):
        p = place(q)
        flag = flags_ref[p].astype(f32)
        free = 1.0 - flag
        top = jnp.maximum(history_ref[p], CRACK_HISTORY * labels_ref[p].astype(f32))
        here = [
            free * disp_ref[0, p] * sign,
            free * disp_ref[1, p],
            free * disp_ref[2, p],
            force_ref[0, p] * sign,
            force_ref[1, p],
            force_ref[2, p],
            damage_ref[p],
            top * (free - flag),
        ]
        for f in range(fields):
            own[f, q] = here[f]
        values.append(here)

    sub = lax.broadcasted_iota(jnp.int32, (TILE, 128), 0)

    def spin(a, shift, axis):
        shift = shift % a.shape[axis]
        return pltpu.roll(a, shift, axis) if shift else a

    def spot(f, q):
        return 8 * (f % 4 // 2) + 2 * q + f % 2

    group = lax.broadcasted_iota(jnp.int32, (ly, 128), 1) // 8
    for j in range(packs):
        low = jnp.zeros((ly, 128), f32)
        high = jnp.zeros((ly, 128), f32)
        for f in range(4 * j, 4 * j + 4):
            for q in range(lx):
                k = spot(f, q)
                turned = spin(values[q][f], 8 * k + 8, 1)
                low = jnp.where(group == (k + 1) % 16, turned, low)
                high = jnp.where(group == k, turned, high)
        zsend[0, j] = low
        zsend[1, j] = high
    for j in range(pairs):
        fa, qa = divmod(2 * j, lx)
        fb, qb = divmod(2 * j + 1, lx)
        a, b = values[qa][fa], values[qb][fb]
        down_send[j] = jnp.where(sub < GHOST, a[0:TILE], spin(b[0:TILE], GHOST, 0))
        up_send[j] = jnp.where(sub < GHOST, spin(b[ly - TILE : ly], GHOST, 0), a[ly - TILE : ly])
    for e in range(extras):
        tile = jnp.zeros((TILE, 128), f32)
        for s in range(TILE):
            k, q = divmod(TILE * e + s, lx)
            tile = jnp.where(sub == s, spin(values[q][DEEP[k]][0:TILE], s - GHOST, 0), tile)
        down_send[pairs + e] = tile

    pl.semaphore_wait(barrier, number_near + 1)

    def remote(src, dst, send, recv, k, device):
        return pltpu.make_async_remote_copy(
            src_ref=src, dst_ref=dst, send_sem=send.at[k], recv_sem=recv.at[k],
            device_id=device, device_id_type=MESH,
        )

    def xcopy(src, dst, k):
        return remote(src, dst, xsend_sem, xrecv_sem, k, partner)

    corner_rows = {-1: (0, ly), 1: (ly - TILE, ly + TILE)}

    def halo(dy, dz):
        device = (gx, gy + dy, gz + dz)
        if dz == 0:
            if dy < 0:
                return remote(down_send, from_up, ysend_sem, yrecv_sem, 0, device)
            return remote(up_send, from_down, ysend_sem, yrecv_sem, 1, device)
        side = 0 if dz < 0 else 1
        if dy == 0:
            return remote(
                zsend.at[side], zrecv.at[side, :, 0:ly], zsend_sem, zrecv_sem, side, device
            )
        source, target = corner_rows[dy]
        return remote(
            zsend.at[side, :, source : source + TILE],
            zrecv.at[side, :, target : target + TILE],
            csend_sem, crecv_sem, 2 * side + (dy > 0), device,
        )

    order = [(0, -1), (0, 1), (-1, -1), (1, -1), (-1, 1), (1, 1), (-1, 0), (1, 0)]
    halos = {way: halo(*way) for way in order}
    x_own = xcopy(own, part, 0)
    x_own.start()
    for way in order:
        pl.when(there(*way))(halos[way].start)
    for dy, dz in order[:6]:
        pl.when(there(-dy, -dz))(halos[dy, dz].wait_recv)
    x_z = xcopy(zrecv, zpart, 1)
    x_z.start()
    pl.when(there(1, 0))(halos[-1, 0].wait_recv)
    x_up = xcopy(from_up, part_up, 2)
    x_up.start()
    pl.when(there(-1, 0))(halos[1, 0].wait_recv)
    x_down = xcopy(from_down, part_down, 3)
    x_down.start()

    lane_w = lax.broadcasted_iota(jnp.int32, (wide, 128), 1)
    odd = lane_w // 8 % 2

    def merge(a):
        return jnp.concatenate(
            [a[0:ly], jnp.where(sub < GHOST, a[ly : ly + TILE], a[ly + TILE : wide])], axis=0
        )

    def both_sides(source, f):
        low, high = source[0, f // 4], source[1, f // 4]
        return jnp.where(odd == f % 2, high, low)

    halves = [spin(both_sides(zrecv, f), -8 * spot(f, 0), 1) for f in range(fields)]
    for exchange in (x_own, x_z, x_up, x_down):
        exchange.wait_recv()
    greet(hop_sem)
    for f in range(fields):
        far = both_sides(zpart, f)
        far = -far if f in TURNED else far
        whole = halves[f]
        for q in range(lx):
            at = nx - 1 - q
            whole = jnp.where(lane_w // 16 == at, spin(far, 8 * (2 * at - spot(f, q)), 1), whole)
        if f in DEEP:
            gz_wide[DEEP.index(f)] = whole
        if f not in (0, 1, 2):
            gz_rows[f - 3] = merge(whole)

    def pieces(f, q):
        mine = q < lx
        at = q if mine else nx - 1 - q
        j, half = divmod(f * lx + at, 2)
        above, below = (from_up, from_down) if mine else (part_up, part_down)
        main = own[f, at] if mine else part[f, at]
        return main, above, below, j, half, at, (not mine) and f in TURNED

    def load_wide(f, q):
        main, above, below, j, half, at, turn = pieces(f, q)
        a, b = above[j], below[j]
        if half:
            a, b = spin(a, GHOST, 0), spin(b, GHOST, 0)
        e, s = divmod(DEEP.index(f) * lx + at, TILE)
        a = jnp.where(sub == GHOST, spin(above[pairs + e], GHOST - s, 0), a)
        out = jnp.concatenate([main, a, b], axis=0)
        return -out if turn else out

    def load_rows(f, q):
        main, above, below, j, half, at, turn = pieces(f, q)
        a, b = above[j], below[j]
        ghost = spin(jnp.where(sub < GHOST, b, a), GHOST, 0) if half else jnp.where(sub < GHOST, a, b)
        out = jnp.concatenate([main, ghost], axis=0)
        return -out if turn else out

    row = lax.broadcasted_iota(jnp.int32, (rows, 128), 0)
    lane = lax.broadcasted_iota(jnp.int32, (rows, 128), 1)
    inside = lane % 16
    ypos = gy * ly + jnp.where(row < ly + GHOST, row, row - rows)
    zpos = gz * lz + lane
    zghost = gz * lz + jnp.where(inside < 8, inside - 8, inside + (lz - 8))

    def element_at(pos, count):
        return jnp.where((pos >= 0) & (pos <= count - 2), 1.0, 0.0)

    yvalid = element_at(ypos, ngy * ly)
    valid = yvalid * element_at(zpos, ngz * lz)
    gvalid = jnp.where(lane < 16 * (nx - 1), yvalid * element_at(zghost, ngz * lz), 0.0)

    def y_up(a):
        return pltpu.roll(a, a.shape[0] - 1, 0)

    def y_dn(a):
        return pltpu.roll(a, 1, 0)

    def lanes(a):
        return lane_w if a.shape[0] == wide else lane

    def z_up(a, ghost, p):
        return jnp.where(lanes(a) == 127, spin(ghost, 119 - 16 * p, 1), pltpu.roll(a, 127, 1))

    def z_up_take(acc, a, p):
        return jnp.where(lanes(a) == 16 * p + 7, spin(a, 16 * p + 7, 1), acc)

    def z_dn(a, ghost, p):
        return jnp.where(lanes(a) == 0, spin(ghost, 121 - 16 * p, 1), pltpu.roll(a, 1, 1))

    def z_dn_take(acc, a, p):
        return jnp.where(lanes(a) == 16 * p + 8, spin(a, 16 * p + 9, 1), acc)

    def plane_up(a):
        return pltpu.roll(a, 112, 1)

    def plane_dn(a):
        return pltpu.roll(a, 16, 1)

    blank = jnp.zeros((rows, 128), f32)
    zero = jnp.zeros((TILE, 128), f32)

    def half_back(ss, yd, zd, yz):
        s = (ss - yd) + y_dn(ss + yd)
        d = (zd - yz) + y_dn(zd + yz)
        return s - d, s + d

    def damage_sum(q):
        a = load_wide(6, q)
        s = a + z_up(a, gz_wide[3], q)
        return merge(s + y_up(s)), a

    def rigidity(low, high, mask):
        rest = 1.0 - (low + high) * 0.125
        return (rest * rest + RESIDUAL_STIFFNESS) * mask

    low, a = damage_sum(0)
    taken = z_up_take(pltpu.roll(gz_wide[3], 127, 1), a, 0)
    for q in range(nx - 1):
        high, a = damage_sum(q + 1)
        stiff[q] = rigidity(low, high, valid)
        taken = z_up_take(taken, a, q + 1)
        low = high
    taken = gz_wide[3] + taken
    taken = merge(taken + y_up(taken))
    stiff[GZ] = rigidity(taken, plane_up(taken), gvalid)
    stiff[nx - 1] = blank

    def gather_back(ref, planes, emit):
        ghost = ref[GZ]
        below = blank
        taken = pltpu.roll(ghost, 1, 1)
        for q in range(planes):
            a = ref[q]
            s = a + z_dn(a, ghost, q)
            here = s + y_dn(s)
            emit(q, below + here)
            below = here
            taken = z_dn_take(taken, a, q)
        s = ghost + taken
        s = s + y_dn(s)
        emit(GZ, s + plane_dn(s))

    def inv_emit(q, total):
        free = (gz_rows[4] if q == GZ else load_rows(7, q)) > 0.0
        inverse[q] = jnp.where(free, 1.0 / jnp.where(free, stiff_diag * total, 1.0), 0.0)

    gather_back(stiff, nx, inv_emit)

    def forward(u, near_u, keep):
        zs, zd = u + near_u, near_u - u
        a, b = keep(y_up(zs)), keep(y_up(zd))
        zs, zd = keep(zs), keep(zd)
        return zs + a, a - zs, zd + b, b - zd

    def same(a):
        return a

    def pass_one(load, planes, keep, height, with_ghost):
        for c in range(3):
            ghost = load(c, GZ)
            taken = pltpu.roll(ghost, 127, 1)
            for q in range(planes):
                u = load(c, q)
                out = forward(u, z_up(u, ghost, q), keep)
                for m in range(4):
                    modes[4 * c + m, q, 0:height] = out[m][0:height]
                if with_ghost:
                    taken = z_up_take(taken, u, q)
            if with_ghost:
                out = forward(ghost, taken, keep)
                for m in range(4):
                    modes[4 * c + m, GZ] = out[m]

    def sm(mode_a, comp_a, mode_b, comp_b):
        return float(stiff_modes[3 * mode_a + comp_a, 3 * mode_b + comp_b])

    k_lame = sm(4, 0, 2, 1)
    k_two = sm(4, 0, 4, 0) - k_lame
    k_shear = sm(2, 0, 2, 0)
    k_twist = sm(3, 0, 5, 1)
    k_bend = sm(3, 1, 3, 1)
    k_cross = sm(3, 1, 5, 0)
    k_last = sm(7, 0, 7, 0)

    def element(low, high, g, energy_at):
        S = [low[m] + high[m] if m % 4 else None for m in range(12)]
        D = [high[m] - low[m] for m in range(12)]
        xX, xXY, xXZ, xXYZ = D[0:4]
        yX, yXY, yXZ, yXYZ = D[4:8]
        zX, zXY, zXZ, zXYZ = D[8:12]
        _, xY, xZ, xYZ = S[0:4]
        _, yY, yZ, yYZ = S[4:8]
        _, zY, zZ, zYZ = S[8:12]
        div = xX + yY + zZ
        sxy, sxz, syz = xY + yX, xZ + zX, yZ + zY
        if energy_at is not None:
            trace = 0.25 * div
            tens = jnp.maximum(trace, 0.0)
            third = trace / 3.0
            ex, ey, ez = 0.25 * xX - third, 0.25 * yY - third, 0.25 * zZ - third
            dev = ex * ex + ey * ey + ez * ez
            she = (sxy * sxy + sxz * sxz + syz * syz) * 0.0625
            energy = 0.5 * BULK_MODULUS * tens * tens + LAME_MU * (dev + 0.5 * she)
            hist[energy_at] = jnp.where(g > 0.0, energy, 0.0)
        gl, g2, gs = k_lame * g, k_two * g, k_shear * g
        gt, gb, gc, g3 = k_twist * g, k_bend * g, k_cross * g, k_last * g
        pressure = gl * div
        fxX, fyY, fzZ = pressure + g2 * xX, pressure + g2 * yY, pressure + g2 * zZ
        txy, txz, tyz = gs * sxy, gs * sxz, gs * syz
        tw = xYZ + yXZ + zXY
        fxYZ, fyXZ, fzXY = gt * (xYZ + tw), gt * (yXZ + tw), gt * (zXY + tw)
        fyYZ, fxXZ = gb * yYZ + gc * xXZ, gb * xXZ + gc * yYZ
        fzYZ, fxXY = gb * zYZ + gc * xXY, gb * xXY + gc * zYZ
        fyXY, fzXZ = gb * yXY + gc * zXZ, gb * zXZ + gc * yXY
        FD = [
            fxX, fxXY, fxXZ, g3 * xXYZ,
            txy, fyXY, fyXZ, g3 * yXYZ,
            txz, fzXY, fzXZ, g3 * zXYZ,
        ]
        FS = [
            None, txy, txz, fxYZ,
            None, fyY, tyz, fyYZ,
            None, tyz, fzZ, fzYZ,
        ]
        lows = [(-FD[m]) if FS[m] is None else FS[m] - FD[m] for m in range(12)]
        highs = [FD[m] if FS[m] is None else FS[m] + FD[m] for m in range(12)]
        return lows, highs

    def element_pass(layers, energies, to_end):
        def step(chunk, carry):
            r = pl.ds(pl.multiple_of(chunk * TILE, TILE), TILE)
            low = [modes[m, 0, r, :] for m in range(12)]
            held = None
            for p in range(layers):
                high = [modes[m, p + 1, r, :] for m in range(12)]
                lows, highs = element(
                    low, high, stiff[p, r, :], (p, r, slice(None)) if p < energies else None
                )
                for m in range(12):
                    modes[m, p, r, :] = lows[m] + held[m] if p else lows[m]
                held, low = highs, high
            if to_end:
                for m in range(12):
                    modes[m, layers, r, :] = held[m]
            low = [modes[m, GZ, r, :] for m in range(12)]
            lows, highs = element(
                low, [plane_up(a) for a in low], stiff[GZ, r, :],
                (GZ, r, slice(None)) if energies else None,
            )
            for m in range(12):
                modes[m, GZ, r, :] = lows[m] + plane_dn(highs[m])
            return carry

        lax.fori_loop(0, rows // TILE, step, 0, unroll=True)

    def each_node(planes, emit, carry):
        ghosts = [half_back(*(modes[4 * c + m, GZ] for m in range(4))) for c in range(3)]
        taken = [pltpu.roll(g[1], 1, 1) for g in ghosts]
        for q in range(planes):
            got = []
            for c in range(3):
                near_w, far_w = half_back(*(modes[4 * c + m, q] for m in range(4)))
                got.append(near_w + z_dn(far_w, ghosts[c][1], q))
                taken[c] = z_dn_take(taken[c], far_w, q)
            carry = emit(q, got, carry)
        emit(GZ, [ghosts[c][0] + taken[c] for c in range(3)], carry)
        return carry

    def fold(a):
        total = a[0:TILE]
        for i in range(TILE, ly, TILE):
            total = total + a[i : i + TILE]
        return total

    nd, ng = DISP_ITERS, DMG_ITERS
    gram, vector = {}, {}

    def load_start(c, q):
        return gz_wide[c] if q == GZ else load_wide(c, q)

    pass_one(load_start, nx, merge, rows, True)
    element_pass(nx - 1, lx + ng, True)

    def start_emit(q, got, dot):
        inv = inverse[q]
        for c in range(3):
            force = gz_rows[c] if q == GZ else load_rows(3 + c, q)
            r = force - got[c]
            v = inv * r
            basis[c, q] = v
            if q < lx:
                resid[c, q] = r[0:ly]
                dot = dot + fold((v * r)[0:ly])
        return dot

    vector[0] = each_node(nx, start_emit, zero)

    def hist_emit(q, total):
        top = gz_rows[4] if q == GZ else load_rows(7, q)
        react[q] = jnp.maximum(jnp.abs(top), 0.125 * total)

    gather_back(hist, lx + ng, hist_emit)

    for k in range(nd - 1):
        planes = lx + nd - 1 - k
        pass_one(lambda c, q, k=k: basis[3 * k + c, q], planes + 1, same, rows, True)
        element_pass(planes, 0, False)

        def apply_emit(q, got, carry, k=k):
            carry = list(carry)
            inv = inverse[q] * (2.0 / SPECTRUM)
            for c in range(3):
                w = got[c]
                here = basis[3 * k + c, q]
                v = inv * w - here
                if k:
                    v = 2.0 * v - basis[3 * (k - 1) + c, q]
                basis[3 * (k + 1) + c, q] = v
                if q < lx:
                    wi, vi = w[0:ly], v[0:ly]
                    if k + 2 < nd:
                        images[3 * k + c, q] = wi
                    carry[0] = carry[0] + fold(here[0:ly] * wi)
                    carry[1] = carry[1] + fold(vi * resid[c, q])
                    carry[2] = carry[2] + fold(vi * wi)
                    for j in range(k):
                        carry[3 + j] = carry[3 + j] + fold(vi * images[3 * j + c, q])
            return tuple(carry)

        got = each_node(planes, apply_emit, (zero,) * (3 + k))
        gram[k, k], vector[k + 1], gram[k + 1, k] = got[:3]
        for j in range(k):
            gram[k + 1, j] = got[3 + j]

    def last_energy():
        pass_one(lambda c, q: basis[3 * (nd - 1) + c, q], lx + 1, same, ly, False)
        total, middle = zero, zero
        for chunk in range(ly // TILE):
            r = slice(TILE * chunk, TILE * chunk + TILE)
            low = [modes[m, 0, r, :] for m in range(12)]
            for p in range(lx):
                high = [modes[m, p + 1, r, :] for m in range(12)]
                S = [low[m] + high[m] if m % 4 else None for m in range(12)]
                D = [high[m] - low[m] for m in range(12)]
                xX, xXY, xXZ, xXYZ = D[0:4]
                yX, yXY, yXZ, yXYZ = D[4:8]
                zX, zXY, zXZ, zXYZ = D[8:12]
                _, xY, xZ, xYZ = S[0:4]
                _, yY, yZ, yYZ = S[4:8]
                _, zY, zZ, zYZ = S[8:12]
                div = xX + yY + zZ
                sxy, sxz, syz = xY + yX, xZ + zX, yZ + zY
                tw = xYZ + yXZ + zXY
                sum_two = xX * xX + yY * yY + zZ * zZ
                sum_shear = sxy * sxy + sxz * sxz + syz * syz
                sum_twist = xYZ * xYZ + yXZ * yXZ + zXY * zXY + tw * tw
                sum_bend = (yYZ * yYZ + xXZ * xXZ) + (zYZ * zYZ + xXY * xXY) + (yXY * yXY + zXZ * zXZ)
                sum_cross = yYZ * xXZ + zYZ * xXY + yXY * zXZ
                sum_last = xXYZ * xXYZ + yXYZ * yXYZ + zXYZ * zXYZ
                energy = (
                    (k_lame * (div * div) + k_two * sum_two)
                    + (k_shear * sum_shear + k_twist * sum_twist)
                    + (k_bend * sum_bend + (2.0 * k_cross) * sum_cross)
                    + k_last * sum_last
                ) * stiff[p, r, :]
                if p + 1 < lx:
                    total = total + energy
                else:
                    middle = middle + energy
                low = high
        return total + 0.5 * middle

    gram[nd - 1, nd - 1] = last_energy()

    cy = yvalid + element_at(ypos - 1, ngy * ly)
    cz = element_at(zpos, ngz * lz) + element_at(zpos - 1, ngz * lz)
    czg = element_at(zghost, ngz * lz) + element_at(zghost - 1, ngz * lz)
    cxg = jnp.where((lane < 16) | (lane >= 16 * (nx - 1)), 1.0, 2.0)
    node = jnp.where(cy * cz > 0.0, 1.0, 0.0)
    gnode = jnp.where(cy * czg > 0.0, 1.0, 0.0)
    diag_scale = laplace_diag * TOUGHNESS * LENGTH_SCALE
    lap_scale = TOUGHNESS * LENGTH_SCALE / 36.0

    def lines(d, after, before, count_z):
        s, n = after + before, count_z * d
        mass, slope = 2.0 * n + s, n - s
        s, n = y_up(mass) + y_dn(mass), cy * mass
        both = 2.0 * n + s
        mixed = (n - s) + (2.0 * (cy * slope) + (y_up(slope) + y_dn(slope)))
        return 2.0 * mixed + both, mixed - both

    def laplace_pass(load, planes, emit, carry, with_ghost):
        ghost = load(GZ)
        after = pltpu.roll(ghost, 127, 1)
        before = pltpu.roll(ghost, 1, 1)
        reach = planes + 1 if planes < nx else nx
        ahead = []
        for q in range(reach):
            d = load(q)
            ahead.append(lines(d, z_up(d, ghost, q), z_dn(d, ghost, q), cz))
            if with_ghost:
                after = z_up_take(after, d, q)
                before = z_dn_take(before, d, q)
            p = q - 1
            if p >= 0:
                total = ahead[p][0] if p == 0 else 2.0 * ahead[p][0] + ahead[p - 1][1]
                carry = emit(p, lap_scale * (total + ahead[q][1]), carry)
        if with_ghost:
            inner, outer = lines(ghost, after, before, czg)
            total = cxg * inner + jnp.where(lane >= 16, plane_dn(outer), 0.0)
            total = total + jnp.where(lane < 16 * (nx - 1), plane_up(outer), 0.0)
            emit(GZ, lap_scale * total, carry)
        return carry

    def reaction_of(q):
        return TOUGHNESS / LENGTH_SCALE + 2.0 * react[q]

    def old_damage(q):
        return gz_rows[3] if q == GZ else load_rows(6, q)

    def dstart(q, lap, dot):
        reaction = reaction_of(q)
        if q == GZ:
            count, mask = cxg * cy * czg, gnode
        else:
            count, mask = (cy * cz if q == 0 else 2.0 * cy * cz), node
        inv = mask / (diag_scale * count + reaction)
        dinverse[q] = inv
        r = 2.0 * react[q] - (lap + reaction * old_damage(q))
        v = inv * r
        dbasis[0, q] = v
        if q < lx:
            dresid[q] = r[0:ly]
            dot = dot + fold((v * r)[0:ly])
        return dot

    dvector, dgram = {}, {}
    dvector[0] = laplace_pass(old_damage, lx + ng, dstart, zero, True)
    dimages = {}
    for k in range(ng):
        more = k + 1 < ng

        def dstep(q, lap, carry, k=k, more=more):
            carry = list(carry)
            here = dbasis[k, q]
            w = lap + reaction_of(q) * here
            if q < lx:
                carry[0] = carry[0] + fold((here * w)[0:ly])
            if more:
                v = dinverse[q] * w - here
                if k:
                    v = 2.0 * v - dbasis[k - 1, q]
                dbasis[k + 1, q] = v
                if q < lx:
                    carry[1] = carry[1] + fold(v[0:ly] * dresid[q])
                    carry[2] = carry[2] + fold((v * w)[0:ly])
            return tuple(carry)

        got = laplace_pass(
            lambda q, k=k: dbasis[k, q], lx + ng - 1 - k, dstep, (zero,) * (3 if more else 1), more
        )
        dgram[k, k] = got[0]
        if more:
            dvector[k + 1], dgram[k + 1, k] = got[1:]

    parts = [vector[i] for i in range(nd)] + [dvector[i] for i in range(ng)]
    parts += [gram[i, j] for i in range(nd) for j in range(i + 1)]
    parts += [dgram[i, j] for i in range(ng) for j in range(i + 1)]
    at = lax.broadcasted_iota(jnp.int32, (1, 128), 1)
    packed = jnp.zeros((1, 128), f32)
    for i, piece in enumerate(parts):
        line = jnp.sum(piece, axis=0, keepdims=True)
        packed = jnp.where(at == i, jnp.sum(line, axis=1, keepdims=True), packed)
    mine = gx * npeer + me
    sums[mine] = packed
    pl.semaphore_wait(hop_sem, number_near)

    def peer_copy(side, o, slot):
        q = lax.rem(me + o, npeer)
        k = side * npeer + o
        return remote(
            sums.at[mine], sums.at[slot], asend_sem, arecv_sem, k,
            (gx if side == 0 else 1 - gx, q // ngz, lax.rem(q, ngz)),
        )

    peers = [(side, o) for o in range(npeer) for side in (0, 1) if side or o]
    sends = [peer_copy(side, o, mine) for side, o in peers]
    for s in sends:
        s.start()
    for q in range(lx):
        out_history[place(q)] = react[q, 0:ly]
    for side, o in peers:
        from_x = gx if side == 0 else 1 - gx
        peer_copy(side, o, from_x * npeer + lax.rem(me + npeer - o, npeer)).wait_recv()
    layer = [sums[i] for i in range(2 * npeer)]
    while len(layer) > 1:
        layer = [a + b for a, b in zip(layer[::2], layer[1::2])] + layer[len(layer) & ~1 :]
    whole = layer[0]

    scalars = [
        jnp.sum(jnp.where(at == i, whole, 0.0), axis=1, keepdims=True) for i in range(len(parts))
    ]

    def solve(rhs, lower):
        n = len(rhs)
        A = [[lower[max(i, j)][min(i, j)] for j in range(n)] for i in range(n)]
        b = list(rhs)
        for i in range(n):
            pivot = 1.0 / A[i][i]
            for r in range(i + 1, n):
                ratio = A[r][i] * pivot
                for c in range(i + 1, n):
                    A[r][c] = A[r][c] - ratio * A[i][c]
                b[r] = b[r] - ratio * b[i]
        out = [None] * n
        for i in reversed(range(n)):
            s = b[i]
            for j in range(i + 1, n):
                s = s - A[i][j] * out[j]
            out[i] = s / A[i][i]
        return out

    def triangle(flat, n):
        return [[flat[k * (k + 1) // 2 + j] for j in range(k + 1)] for k in range(n)]

    rest = scalars[nd + ng :]
    cut = nd * (nd + 1) // 2
    weights = solve(scalars[:nd], triangle(rest[:cut], nd))
    dweights = solve(scalars[nd : nd + ng], triangle(rest[cut:], ng))
    for q in range(lx):
        p = place(q)
        for c in range(3):
            x = own[c, q]
            for k in range(nd):
                x = x + weights[k] * basis[3 * k + c, q, 0:ly]
            out_disp[c, p] = sign * x if c == 0 else x
        d = own[6, q]
        for k in range(ng):
            d = d + dweights[k] * dbasis[k, q, 0:ly]
        out_damage[p] = d

    for way in order:
        pl.when(there(*way))(halos[way].wait_send)
    for exchange in (x_own, x_z, x_up, x_down):
        exchange.wait_send()
    for s in sends:
        s.wait_send()


def hand_on(*refs):
    sources, targets, sem = refs[:3], refs[3:6], refs[6]
    copies = [
        pltpu.make_async_copy(source, target, sem.at[i])
        for i, (source, target) in enumerate(zip(sources, targets))
    ]
    for copy in copies:
        copy.start()
    for copy in copies:
        copy.wait()


def body_fused(sizes, *arrays):
    ngy, ngz, lx, ly, lz = sizes
    nx, rows, wide, fields = 2 * lx, ly + TILE, ly + 2 * TILE, 8
    packs, pairs, extras = fields * lx // 16, fields * lx // 2, len(DEEP) * lx // TILE
    npeer = ngy * ngz
    f32 = jnp.float32
    planes = (nx + 1, rows, lz)
    vmem = pl.BlockSpec(memory_space=pltpu.VMEM)
    hbm = pl.BlockSpec(memory_space=pltpu.HBM)
    dma = pltpu.SemaphoreType.DMA

    def room(*shape):
        return pltpu.VMEM(shape, f32)

    results = pl.pallas_call(
        functools.partial(kernel, sizes),
        out_shape=(
            pltpu.VMEM((3, lx, ly, lz), f32),
            pltpu.VMEM((lx, ly, lz), f32),
            pltpu.VMEM((lx, ly, lz), f32),
        ),
        in_specs=[hbm] * 6,
        out_specs=(vmem,) * 3,
        scratch_shapes=[
            room(3, lx, ly, lz),
            room(3, lx, ly, lz),
            room(lx, ly, lz),
            room(lx, ly, lz),
            pltpu.VMEM((lx, ly, lz), jnp.int32),
            pltpu.VMEM((lx, ly, lz), jnp.int32),
            room(fields, lx, ly, lz),
            room(fields, lx, ly, lz),
            room(pairs + extras, TILE, 128),
            room(pairs, TILE, 128),
            room(pairs + extras, TILE, 128),
            room(pairs, TILE, 128),
            room(pairs + extras, TILE, 128),
            room(pairs, TILE, 128),
            room(2, packs, ly, 128),
            room(2, packs, wide, 128),
            room(2, packs, wide, 128),
            room(4, wide, 128),
            room(5, rows, 128),
            room(12, *planes),
            room(3 * DISP_ITERS, *planes),
            room(3 * (DISP_ITERS - 2), lx, ly, lz),
            room(3, lx, ly, lz),
            room(*planes),
            room(*planes),
            room(*planes),
            room(*planes),
            room(*planes),
            room(DMG_ITERS, *planes),
            room(lx, ly, lz),
            room(2 * npeer, 1, 128),
            dma((6,)),
            dma((2,)),
            dma((2,)),
            dma((2,)),
            dma((2,)),
            dma((4,)),
            dma((4,)),
            dma((4,)),
            dma((4,)),
            dma((2 * npeer,)),
            dma((2 * npeer,)),
            pltpu.SemaphoreType.REGULAR,
        ],
        compiler_params=pltpu.CompilerParams(
            collective_id=0, has_side_effects=True, vmem_limit_bytes=VMEM_LIMIT
        ),
    )(*[pltpu.with_memory_space_constraint(a, pltpu.HBM) for a in arrays])
    return pl.pallas_call(
        hand_on,
        out_shape=tuple(jax.ShapeDtypeStruct(r.shape, f32) for r in results),
        in_specs=[vmem] * 3,
        out_specs=(hbm,) * 3,
        scratch_shapes=[dma((3,))],
        compiler_params=pltpu.CompilerParams(vmem_limit_bytes=1024 * 1024),
    )(*[pltpu.with_memory_space_constraint(r, pltpu.VMEM) for r in results])


VMEM_LIMIT = 24 * 1024 * 1024


def solution(mesh):
    shape = dict(mesh.shape)

    def body(*arrays):
        lx, ly, lz = arrays[2].shape
        fits = shape["gx"] == 2 and shape["gy"] * shape["gz"] > 1
        fits = fits and max(shape["gy"], shape["gz"]) <= 4
        fits = fits and lx == 4 and ly % 8 == 0 and lz == 128
        if fits:
            return body_fused((shape["gy"], shape["gz"], lx, ly, lz), *arrays)
        return body_any_mesh(*arrays)

    return jax.shard_map(
        body,
        mesh=mesh,
        in_specs=(
            P(None, "gx", "gy", "gz"),
            P(None, "gx", "gy", "gz"),
            P("gx", "gy", "gz"),
            P("gx", "gy", "gz"),
            P("gx", "gy", "gz"),
            P("gx", "gy", "gz"),
        ),
        out_specs=(P(None, "gx", "gy", "gz"), P("gx", "gy", "gz"), P("gx", "gy", "gz")),
        check_vma=False,
    )
```

```python
import functools
import jax
import jax.numpy as jnp
import numpy as np
from jax import lax
from jax.experimental import pallas as pl
from jax.experimental.pallas import tpu as pltpu
from jax.sharding import PartitionSpec as P

DISP_ITERS = 4
DMG_ITERS = 2


LAME_LAMBDA = 0.5769230769230769
LAME_MU = 0.38461538461538464
BULK_MODULUS = LAME_LAMBDA + 2.0 * LAME_MU / 3.0
RESIDUAL_STIFFNESS = 0.001
TOUGHNESS = 1.0
LENGTH_SCALE = 2.0
CRACK_HISTORY = 40.0


def padded_2(cells, sides, width):
    for axis, dim in sides:
        count = lax.axis_size(axis)
        ends = count - 1
        head = lax.slice_in_dim(cells, 0, width, axis=dim)
        tail = lax.slice_in_dim(cells, cells.shape[dim] - width, cells.shape[dim], axis=dim)
        cells = jnp.concatenate(
            [
                lax.ppermute(tail, axis, [(i, (i + 1) % count) for i in range(ends)]),
                cells,
                lax.ppermute(head, axis, [((i + 1) % count, i) for i in range(ends)]),
            ],
            axis=dim,
        )
    return cells


def corner_offsets(corner):
    return (corner >> 2 & 1, corner >> 1 & 1, corner & 1)


def shape_gradients(sample):
    gradient = np.zeros((3, 8))
    for corner in range(8):
        offsets = corner_offsets(corner)
        values = [sample[k] if offsets[k] else 1.0 - sample[k] for k in range(3)]
        slopes = [1.0 if offsets[k] else -1.0 for k in range(3)]
        gradient[0, corner] = slopes[0] * values[1] * values[2]
        gradient[1, corner] = values[0] * slopes[1] * values[2]
        gradient[2, corner] = values[0] * values[1] * slopes[2]
    return gradient


def strain_matrix(gradient):
    strain = np.zeros((6, 24))
    for corner in range(8):
        column = 3 * corner
        strain[0, column] = gradient[0, corner]
        strain[1, column + 1] = gradient[1, corner]
        strain[2, column + 2] = gradient[2, corner]
        strain[3, column] = gradient[1, corner]
        strain[3, column + 1] = gradient[0, corner]
        strain[4, column + 1] = gradient[2, corner]
        strain[4, column + 2] = gradient[1, corner]
        strain[5, column] = gradient[2, corner]
        strain[5, column + 2] = gradient[0, corner]
    return strain


def element_tables():
    moduli = np.zeros((6, 6))
    moduli[:3, :3] = LAME_LAMBDA
    for k in range(3):
        moduli[k, k] += 2.0 * LAME_MU
        moduli[k + 3, k + 3] = LAME_MU
    points = [0.5 - 0.5 / np.sqrt(3.0), 0.5 + 0.5 / np.sqrt(3.0)]
    stiff_table = np.zeros((24, 24))
    laplace_table = np.zeros((8, 8))
    for sample_index in range(8):
        sample = tuple((points[k] for k in corner_offsets(sample_index)))
        gradient = shape_gradients(sample)
        strain = strain_matrix(gradient)
        stiff_table += 0.125 * strain.T @ moduli @ strain
        laplace_table += 0.125 * gradient.T @ gradient
    centre_table = strain_matrix(shape_gradients((0.5, 0.5, 0.5)))
    return (
        stiff_table.astype(np.float32),
        laplace_table.astype(np.float32),
        centre_table.astype(np.float32),
    )


def corner_views(padded, element_shape):
    corner_list = []
    for corner in range(8):
        offx, offy, offz = corner_offsets(corner)
        corner_list.append(
            padded[
                ...,
                offx : offx + element_shape[0],
                offy : offy + element_shape[1],
                offz : offz + element_shape[2],
            ]
        )
    return corner_list


def assemble_nodes(pieces):
    running = None
    for corner in range(8):
        offx, offy, offz = corner_offsets(corner)
        leading = [(0, 0)] * (pieces[corner].ndim - 3)
        placed = jnp.pad(
            pieces[corner], leading + [(offx, 1 - offx), (offy, 1 - offy), (offz, 1 - offz)]
        )
        running = placed if running is None else running + placed
    return running


def line_valid(position, devices, count):
    index = position * count + jnp.arange(count + 1, dtype=jnp.int32) - 1
    return ((index >= 0) & (index <= devices * count - 2)).astype(jnp.float32)


def strain_energy(strain):
    trace = strain[0] + strain[1] + strain[2]
    deviator = strain[:3] - trace[None] / 3.0
    shear = strain[3:]
    tensile = jnp.maximum(trace, 0.0)
    return 0.5 * BULK_MODULUS * tensile * tensile + LAME_MU * (
        jnp.sum(deviator * deviator, axis=0) + 0.5 * jnp.sum(shear * shear, axis=0)
    )


def forces_to_nodes(forces, stiffness):
    pieces = [stiffness[None] * forces[3 * target : 3 * target + 3] for target in range(8)]
    return assemble_nodes(pieces)


def element_apply(padded, stiffness, stiff_table):
    element_shape = stiffness.shape
    flat = jnp.stack(corner_views(padded, element_shape)).reshape(24, -1)
    forces = jnp.dot(stiff_table, flat, precision=lax.Precision.HIGHEST).reshape(
        (24,) + element_shape
    )
    return forces_to_nodes(forces, stiffness)


def laplace_apply(padded, element_valid, laplace_table):
    element_shape = element_valid.shape
    flat = jnp.stack(corner_views(padded, element_shape)).reshape(8, -1)
    forces = jnp.dot(laplace_table, flat, precision=lax.Precision.HIGHEST).reshape(
        (8,) + element_shape
    )
    return assemble_nodes([element_valid * forces[target] for target in range(8)])


def single_pair(pair):
    return tuple(lax.psum(pair, ("gx", "gy", "gz")))


def conjugate(solutions, residuals, inverses, counts, apply_fn):
    solutions = list(solutions)
    residuals = list(residuals)
    number = len(solutions)
    steps = max(counts)

    def pair_totals(pairs):
        return [single_pair(pairs[0])]

    precs = [inverses[0] * residuals[0]]
    applied = apply_fn(precs, list(range(number)))
    pairs = pair_totals([(jnp.sum(residuals[0] * precs[0]), jnp.sum(precs[0] * applied[0]))])
    norms = [pair[0] for pair in pairs]
    lengths = [pair[0] / pair[1] for pair in pairs]
    directions = list(precs)
    alongs = list(applied)
    for step in range(steps):
        active = [i for i in range(number) if step < counts[i]]
        for i in active:
            solutions[i] = solutions[i] + lengths[i] * directions[i]
            residuals[i] = residuals[i] - lengths[i] * alongs[i]
        later = [i for i in active if step + 1 < counts[i]]
        if later:
            i = later[0]
            precs[i] = inverses[i] * residuals[i]
            images = apply_fn([precs[i] for i in later], later)
            pairs = pair_totals(
                [
                    (jnp.sum(residuals[i] * precs[i]), jnp.sum(precs[i] * images[k]))
                    for k, i in enumerate(later)
                ]
            )
            for k, i in enumerate(later):
                norm_next, curve_sum = pairs[k]
                ratio = norm_next / norms[i]
                lengths[i] = norm_next / (curve_sum - ratio * norm_next / lengths[i])
                directions[i] = precs[i] + ratio * directions[i]
                alongs[i] = images[k] + ratio * alongs[i]
                norms[i] = norm_next
    return solutions


def body_any_mesh(displacement_start, external_force, damage_old, history_old, crack_labels, fixed_flags):
    tables = element_tables()
    stiff_table = jnp.asarray(tables[0], jnp.float32)
    laplace_table = jnp.asarray(tables[1], jnp.float32)
    centre_table = jnp.asarray(tables[2], jnp.float32)
    highest = lax.Precision.HIGHEST
    size_x, size_y, size_z = damage_old.shape
    free_mask = 1.0 - fixed_flags.astype(jnp.float32)
    start_disp = displacement_start * free_mask[None]
    element_valid = (
        line_valid(lax.axis_index("gx"), lax.axis_size("gx"), size_x)[:, None, None]
        * line_valid(lax.axis_index("gy"), lax.axis_size("gy"), size_y)[None, :, None]
        * line_valid(lax.axis_index("gz"), lax.axis_size("gz"), size_z)[None, None, :]
    )
    element_shape = element_valid.shape
    start_pad = padded_2(
        jnp.concatenate([start_disp, damage_old[None]], axis=0),
        (("gx", 1), ("gy", 2), ("gz", 3)),
        1,
    )
    corner_list = corner_views(start_pad, element_shape)
    damage_mean = sum((view[3] for view in corner_list)) / 8.0
    stiffness = ((1.0 - damage_mean) ** 2 + RESIDUAL_STIFFNESS) * element_valid
    flat = jnp.stack([view[:3] for view in corner_list]).reshape(24, -1)
    combined = jnp.dot(
        jnp.concatenate([stiff_table, centre_table], axis=0), flat, precision=highest
    )
    forces = combined[:24].reshape((24,) + element_shape)
    strain = combined[24:].reshape((6,) + element_shape)
    start_image = forces_to_nodes(forces, stiffness)[:, 1:-1, 1:-1, 1:-1]
    energy = strain_energy(strain) * element_valid
    nodal_energy = assemble_nodes([energy] * 8)[1:-1, 1:-1, 1:-1] / 8.0
    history = jnp.maximum(
        jnp.maximum(history_old, nodal_energy), CRACK_HISTORY * crack_labels.astype(jnp.float32)
    )
    stiff_diag = jnp.diagonal(stiff_table)
    diag_pieces = [
        stiffness[None] * stiff_diag[3 * target : 3 * target + 3][:, None, None, None]
        for target in range(8)
    ]
    elastic_diag = assemble_nodes(diag_pieces)[:, 1:-1, 1:-1, 1:-1]
    inverse_elastic = 1.0 / (free_mask[None] * elastic_diag + (1.0 - free_mask[None]))

    def constrained(nodal_field):
        masked = free_mask[None] * nodal_field
        padded = padded_2(masked, (("gx", 1), ("gy", 2), ("gz", 3)), 1)
        nodes = element_apply(padded, stiffness, stiff_table)[:, 1:-1, 1:-1, 1:-1]
        return free_mask[None] * nodes + (1.0 - free_mask[None]) * nodal_field

    reaction = TOUGHNESS / LENGTH_SCALE + 2.0 * history
    laplace_diag = assemble_nodes(
        [element_valid * laplace_table[target, target] for target in range(8)]
    )[1:-1, 1:-1, 1:-1]
    inverse_damage = 1.0 / (TOUGHNESS * LENGTH_SCALE * laplace_diag + reaction)
    residual = free_mask[None] * (external_force - start_image)
    start_lap = laplace_apply(start_pad[3], element_valid, laplace_table)[1:-1, 1:-1, 1:-1]
    damage_residual = 2.0 * history - (TOUGHNESS * LENGTH_SCALE * start_lap + reaction * damage_old)

    def damage_operator(nodal_field):
        padded = padded_2(nodal_field, (("gx", 0), ("gy", 1), ("gz", 2)), 1)
        lap_nodes = laplace_apply(padded, element_valid, laplace_table)[1:-1, 1:-1, 1:-1]
        return TOUGHNESS * LENGTH_SCALE * lap_nodes + reaction * nodal_field

    def single_elastic(fields, active):
        return [constrained(fields[0])]

    def single_damage(fields, active):
        return [damage_operator(fields[0])]

    displacement = conjugate(
        [start_disp], [residual], [inverse_elastic], [DISP_ITERS], single_elastic
    )[0]
    damage = conjugate(
        [damage_old], [damage_residual], [inverse_damage], [DMG_ITERS], single_damage
    )[0]
    return (displacement, damage, history)


SPECTRUM = 3.2
TILE = 8
GHOST = 4
DEEP = 4
MESH = pl.DeviceIdType.MESH


def walsh_tables():
    stiff, laplace, _ = element_tables()
    signs = np.array(
        [
            [np.prod([1.0 if c >> k & 1 else (-1.0 if m >> k & 1 else 1.0) for k in range(3)]) for c in range(8)]
            for m in range(8)
        ]
    )
    wide = np.kron(signs, np.eye(3))
    stiff_modes = wide @ stiff.astype(np.float64) @ wide.T / 64.0
    return stiff_modes, float(stiff[0, 0]), float(laplace[0, 0])


def kernel(
    sizes,
    disp_in,
    force_in,
    damage_in,
    history_in,
    labels_in,
    flags_in,
    out_disp,
    out_damage,
    out_history,
    disp_ref,
    force_ref,
    damage_ref,
    history_ref,
    labels_ref,
    flags_ref,
    full_deep,
    full_flat,
    down_deep,
    up_deep,
    down_flat,
    up_flat,
    ghost_deep,
    ghost_flat,
    zsend_deep,
    zsend_flat,
    zbuf_deep,
    zbuf_flat,
    gz_wide,
    gz_rows,
    modes,
    basis,
    images,
    resid,
    stiff,
    inverse,
    hist,
    react,
    dinverse,
    dbasis,
    dresid,
    basis_part,
    dbasis_part,
    react_part,
    sums,
    in_sem,
    ysend_sem,
    yrecv_sem,
    zsend_sem,
    zrecv_sem,
    csend_sem,
    crecv_sem,
    xsend_sem,
    xrecv_sem,
    asend_sem,
    arecv_sem,
    hop_sem,
):
    ngy, ngz, lx, ly, lz = sizes
    nx = 2 * lx
    fields = 8
    npeer = ngy * ngz
    pairs = DEEP * lx // 2
    packs = fields * lx // 16
    extras = DEEP * lx // TILE
    wide, rows = 3 * TILE, 2 * TILE
    GZ = nx
    f32 = jnp.float32
    stiff_modes, stiff_diag, laplace_diag = walsh_tables()
    gx, gy, gz = lax.axis_index("gx"), lax.axis_index("gy"), lax.axis_index("gz")
    me = gy * ngz + gz
    partner = (1 - gx, gy, gz)
    outward = 2 * gx - 1
    full, zsend, zbuf = (full_deep, full_flat), (zsend_deep, zsend_flat), (zbuf_deep, zbuf_flat)

    def there(dy, dz):
        y, z = gy + dy, gz + dz
        return (y >= 0) & (y < ngy) & (z >= 0) & (z < ngz)

    def device(core, dy, dz):
        return core, lax.rem(gy + dy + ngy, ngy), lax.rem(gz + dz + ngz, ngz)

    near = [(dy, dz) for dy in (-1, 0, 1) for dz in (-1, 0, 1) if dy or dz]
    number_near = 2 * sum(there(dy, dz).astype(jnp.int32) for dy, dz in near)

    barrier = pltpu.get_barrier_semaphore()

    def greet(semaphore):
        for dy, dz in near:

            @pl.when(there(dy, dz))
            def _():
                for core in (gx, 1 - gx):
                    pl.semaphore_signal(
                        semaphore, inc=1, device_id=device(core, dy, dz), device_id_type=MESH
                    )

    greet(barrier)
    pl.semaphore_signal(barrier, inc=1, device_id=partner, device_id_type=MESH)

    loads = [
        pltpu.make_async_copy(source, target, in_sem.at[i])
        for i, (source, target) in enumerate(
            [
                (flags_in, flags_ref),
                (disp_in, disp_ref),
                (force_in, force_ref),
                (damage_in, damage_ref),
                (history_in, history_ref),
                (labels_in, labels_ref),
            ]
        )
    ]
    for load in loads:
        load.start()

    zero = jnp.zeros((TILE, 128), f32)
    for dz, side in ((1, 0), (-1, 1)):

        @pl.when(jnp.logical_not(there(0, dz)))
        def _():
            for core in range(2):
                for ref in zbuf:
                    ref[core, side, 0:2] = jnp.zeros((2, TILE, 128), f32)

        @pl.when(jnp.logical_not(there(outward, dz)))
        def _():
            for core in range(2):
                for ref in zbuf:
                    ref[core, side, 2] = zero

    @pl.when(jnp.logical_not(there(outward, 0)))
    def _():
        ghost_deep[...] = jnp.zeros(ghost_deep.shape, f32)
        ghost_flat[...] = jnp.zeros(ghost_flat.shape, f32)

    for load in loads:
        load.wait()

    values = []
    for p in range(lx):
        flag = flags_ref[p].astype(f32)
        free = 1.0 - flag
        top = jnp.maximum(history_ref[p], CRACK_HISTORY * labels_ref[p].astype(f32))
        here = [free * disp_ref[c, p] for c in range(3)]
        here += [damage_ref[p]] + [force_ref[c, p] for c in range(3)] + [top * (free - flag)]
        for f in range(fields):
            for half in range(2):
                full[f // DEEP][f % DEEP, half, gx * lx + p] = here[f][TILE * half : TILE * half + TILE]
        values.append(here)

    sub = lax.broadcasted_iota(jnp.int32, (TILE, 128), 0)

    def spin(a, shift, axis):
        shift = shift % a.shape[axis]
        return pltpu.roll(a, shift, axis) if shift else a

    def spot(f, q):
        return 8 * (f % 4 // 2) + 2 * q + f % 2

    group = lax.broadcasted_iota(jnp.int32, (ly, 128), 1) // 8
    for j in range(packs):
        low = jnp.zeros((ly, 128), f32)
        high = jnp.zeros((ly, 128), f32)
        for f in range(4 * j, 4 * j + 4):
            for q in range(lx):
                k = spot(f, q)
                turned = spin(values[q][f], 8 * k + 8, 1)
                low = jnp.where(group == (k + 1) % 16, turned, low)
                high = jnp.where(group == k, turned, high)
        for half in range(2):
            zsend[j][0, half] = low[TILE * half : TILE * half + TILE]
            zsend[j][1, half] = high[TILE * half : TILE * half + TILE]
    for first, down, up in ((0, down_deep, up_deep), (DEEP, down_flat, up_flat)):
        for j in range(pairs):
            fa, qa = divmod(2 * j, lx)
            fb, qb = divmod(2 * j + 1, lx)
            a, b = values[qa][first + fa], values[qb][first + fb]
            down[j] = jnp.where(sub < GHOST, a[0:TILE], spin(b[0:TILE], GHOST, 0))
            up[j] = jnp.where(sub < GHOST, spin(b[ly - TILE : ly], GHOST, 0), a[ly - TILE : ly])
    for e in range(extras):
        tile = jnp.zeros((TILE, 128), f32)
        for s in range(TILE):
            f, q = divmod(TILE * e + s, lx)
            tile = jnp.where(sub == s, spin(values[q][f][0:TILE], s - GHOST, 0), tile)
        down_deep[pairs + e] = tile

    pl.semaphore_wait(barrier, number_near + 1)

    def remote(src, dst, send, recv, target):
        return pltpu.make_async_remote_copy(
            src_ref=src, dst_ref=dst, send_sem=send, recv_sem=recv,
            device_id=target, device_id_type=MESH,
        )

    def xcopy(src, dst, k):
        return remote(src, dst, xsend_sem.at[k], xrecv_sem.at[k], partner)

    def zcopy(source, dz, pack, core):
        side = 0 if dz < 0 else 1
        return remote(
            zsend[pack].at[side], zbuf[pack].at[source, side, 0:2],
            zsend_sem.at[4 * core + 2 * side + pack], zrecv_sem.at[4 * source + 2 * side + pack],
            device(core, 0, dz),
        )

    def corner(source, dy, dz, pack):
        side = 0 if dz < 0 else 1
        return remote(
            zsend[pack].at[side, int(dy > 0)], zbuf[pack].at[source, side, 2],
            csend_sem.at[4 * (dy > 0) + 2 * side + pack],
            crecv_sem.at[4 * source + 2 * side + pack],
            device(int(dy < 0), dy, dz),
        )

    def ycopy(source, dy, flat):
        if flat:
            src, dst = (down_flat if dy < 0 else up_flat), ghost_flat.at[source]
        elif dy < 0:
            src, dst = down_deep, ghost_deep.at[source]
        else:
            src, dst = up_deep, ghost_deep.at[source, 0:pairs]
        return remote(
            src, dst, ysend_sem.at[2 * flat + (dy > 0)], yrecv_sem.at[2 * flat + source],
            device(int(dy < 0), dy, 0),
        )

    own = pl.ds(gx * lx, lx)
    x_own = [
        xcopy(full[flat].at[:, :, own], full[flat].at[:, :, own], flat) for flat in range(2)
    ]
    halos = [[], []]
    for flat in (0, 1):
        for source in (0, 1):
            ways = [((dy, dz), corner(source, dy, dz, flat)) for dy in (-1, 1) for dz in (-1, 1)]
            ways += [((dy, 0), ycopy(source, dy, flat)) for dy in (-1, 1)]
            ways += [((0, dz), zcopy(source, dz, flat, core)) for dz in (-1, 1) for core in (0, 1)]
            halos[flat] += [((gx == source) & there(*way), copy) for way, copy in ways]
    for flat in (0, 1):
        x_own[flat].start()
        for guard, copy in halos[flat]:
            pl.when(guard)(copy.start)

    def arrive(flat):
        for dz in (-1, 1):
            for source in range(2):
                pl.when(there(0, -dz))(zcopy(source, dz, flat, 0).wait_recv)
        x_own[flat].wait_recv()
        for dz in (-1, 1):
            for source in range(2):
                pl.when(there(outward, -dz))(corner(source, 1, dz, flat).wait_recv)
        for core in range(2):
            for source in range(2):
                pl.when((gx == core) & there(outward, 0))(
                    ycopy(source, -1 if core else 1, flat).wait_recv
                )

    arrive(0)

    lane_w = lax.broadcasted_iota(jnp.int32, (wide, 128), 1)
    odd = lane_w // 8 % 2

    def merge(a):
        return jnp.concatenate(
            [a[0:TILE], jnp.where(sub < GHOST, a[TILE : 2 * TILE], a[2 * TILE :])], axis=0
        )

    is_lower = sub + TILE * gx < TILE
    from_theirs = (sub + GHOST * gx) % TILE < GHOST

    def order(lower, upper):
        return jnp.where(is_lower, lower, upper), jnp.where(is_lower, upper, lower)

    def ghost_tiles(f):
        halves = []
        for source in range(2):
            ref = zbuf[f // 4]
            low, high = (
                jnp.concatenate([ref[source, side, k] for k in range(3)], axis=0) for side in range(2)
            )
            both = jnp.where(odd == f % 2, high, low)
            halves.append(spin(both, 8 * (2 * lx * source - spot(f, 0)), 1))
        whole = jnp.where(lane_w < 16 * lx, *halves)
        return *order(whole[0:TILE], whole[TILE : 2 * TILE]), whole[2 * TILE :]

    def line_wide(tile, other, up, down):
        return jnp.concatenate(
            [tile, jnp.where(is_lower, other, up), jnp.where(is_lower, down, other)], axis=0
        )

    def line_rows(tile, other, ghost):
        return jnp.concatenate([tile, jnp.where(from_theirs, other, ghost)], axis=0)

    for f in range(DEEP):
        tile, other, ghost = ghost_tiles(f)
        gz_wide[f] = line_wide(tile, other, ghost, ghost)
    gz_rows[0] = merge(gz_wide[DEEP - 1])

    def pieces(f, q):
        source, p = divmod(q, lx)
        j, half = divmod(f % DEEP * lx + p, 2)
        ghost = ghost_deep[source, j] if f < DEEP else ghost_flat[source, j]
        ref = full[f // DEEP]
        return *order(ref[f % DEEP, 0, q], ref[f % DEEP, 1, q]), spin(ghost, GHOST * half, 0)

    def load_wide(f, q):
        tile, other, ghost = pieces(f, q)
        e, s = divmod(f * lx + q % lx, TILE)
        extra = spin(ghost_deep[q // lx, pairs + e], GHOST - s, 0)
        return line_wide(tile, other, jnp.where(sub == GHOST, extra, ghost), ghost)

    def load_rows(f, q):
        if q == GZ:
            return gz_rows[f - DEEP + 1]
        return line_rows(*pieces(f, q))

    row = lax.broadcasted_iota(jnp.int32, (rows, 128), 0)
    lane = lax.broadcasted_iota(jnp.int32, (rows, 128), 1)
    inside = lane % 16
    ypos = gy * ly + gx * TILE + jnp.where(row < TILE + GHOST, row, row - rows)
    zpos = gz * lz + lane
    zghost = gz * lz + jnp.where(inside < 8, inside - 8, inside + (lz - 8))

    def element_at(pos, count):
        return jnp.where((pos >= 0) & (pos <= count - 2), 1.0, 0.0)

    yvalid = element_at(ypos, ngy * ly)
    valid = yvalid * element_at(zpos, ngz * lz)
    gvalid = jnp.where(lane < 16 * (nx - 1), yvalid * element_at(zghost, ngz * lz), 0.0)

    def y_up(a):
        return pltpu.roll(a, a.shape[0] - 1, 0)

    def y_dn(a):
        return pltpu.roll(a, 1, 0)

    def lanes(a):
        return lane_w if a.shape[0] == wide else lane

    def z_up(a, ghost, p):
        return jnp.where(lanes(a) == 127, spin(ghost, 119 - 16 * p, 1), pltpu.roll(a, 127, 1))

    def z_up_take(acc, a, p):
        return jnp.where(lanes(a) == 16 * p + 7, spin(a, 16 * p + 7, 1), acc)

    def z_dn(a, ghost, p):
        return jnp.where(lanes(a) == 0, spin(ghost, 121 - 16 * p, 1), pltpu.roll(a, 1, 1))

    def z_dn_take(acc, a, p):
        return jnp.where(lanes(a) == 16 * p + 8, spin(a, 16 * p + 9, 1), acc)

    def plane_up(a):
        return pltpu.roll(a, 112, 1)

    def plane_dn(a):
        return pltpu.roll(a, 16, 1)

    blank = jnp.zeros((rows, 128), f32)

    def half_back(ss, yd, zd, yz):
        s = (ss - yd) + y_dn(ss + yd)
        d = (zd - yz) + y_dn(zd + yz)
        return s - d, s + d

    def damage_sum(q):
        a = load_wide(3, q)
        s = a + z_up(a, gz_wide[3], q)
        return merge(s + y_up(s)), a

    def rigidity(low, high, mask):
        rest = 1.0 - (low + high) * 0.125
        return (rest * rest + RESIDUAL_STIFFNESS) * mask

    low, a = damage_sum(0)
    taken = z_up_take(pltpu.roll(gz_wide[3], 127, 1), a, 0)
    for q in range(nx - 1):
        high, a = damage_sum(q + 1)
        stiff[q] = rigidity(low, high, valid)
        taken = z_up_take(taken, a, q + 1)
        low = high
    taken = gz_wide[3] + taken
    taken = merge(taken + y_up(taken))
    stiff[GZ] = rigidity(taken, plane_up(taken), gvalid)
    stiff[nx - 1] = blank

    def gather_back(ref, emit):
        ghost = ref[GZ]
        below = blank
        taken = pltpu.roll(ghost, 1, 1)
        for q in range(nx):
            a = ref[q]
            s = a + z_dn(a, ghost, q)
            here = s + y_dn(s)
            emit(q, below + here)
            below = here
            taken = z_dn_take(taken, a, q)
        s = ghost + taken
        s = s + y_dn(s)
        emit(GZ, s + plane_dn(s))

    def inv_emit(q, total):
        free = load_rows(7, q) > 0.0
        inverse[q] = jnp.where(free, 1.0 / jnp.where(free, stiff_diag * total, 1.0), 0.0)

    def forward(u, near_u, keep):
        zs, zd = u + near_u, near_u - u
        a, b = keep(y_up(zs)), keep(y_up(zd))
        zs, zd = keep(zs), keep(zd)
        return zs + a, a - zs, zd + b, b - zd

    def same(a):
        return a

    def pass_one(load, keep, height, with_ghost):
        for c in range(3):
            ghost = load(c, GZ)
            taken = pltpu.roll(ghost, 127, 1)
            for q in range(nx):
                u = load(c, q)
                out = forward(u, z_up(u, ghost, q), keep)
                for m in range(4):
                    modes[4 * c + m, q, 0:height] = out[m][0:height]
                if with_ghost:
                    taken = z_up_take(taken, u, q)
            if with_ghost:
                out = forward(ghost, taken, keep)
                for m in range(4):
                    modes[4 * c + m, GZ] = out[m]

    def sm(mode_a, comp_a, mode_b, comp_b):
        return float(stiff_modes[3 * mode_a + comp_a, 3 * mode_b + comp_b])

    k_lame = sm(4, 0, 2, 1)
    k_two = sm(4, 0, 4, 0) - k_lame
    k_shear = sm(2, 0, 2, 0)
    k_twist = sm(3, 0, 5, 1)
    k_bend = sm(3, 1, 3, 1)
    k_cross = sm(3, 1, 5, 0)
    k_last = sm(7, 0, 7, 0)

    def element(low, high, g, energy_at):
        S = [low[m] + high[m] if m % 4 else None for m in range(12)]
        D = [high[m] - low[m] for m in range(12)]
        xX, xXY, xXZ, xXYZ = D[0:4]
        yX, yXY, yXZ, yXYZ = D[4:8]
        zX, zXY, zXZ, zXYZ = D[8:12]
        _, xY, xZ, xYZ = S[0:4]
        _, yY, yZ, yYZ = S[4:8]
        _, zY, zZ, zYZ = S[8:12]
        div = xX + yY + zZ
        sxy, sxz, syz = xY + yX, xZ + zX, yZ + zY
        if energy_at is not None:
            trace = 0.25 * div
            tens = jnp.maximum(trace, 0.0)
            third = trace / 3.0
            ex, ey, ez = 0.25 * xX - third, 0.25 * yY - third, 0.25 * zZ - third
            dev = ex * ex + ey * ey + ez * ez
            she = (sxy * sxy + sxz * sxz + syz * syz) * 0.0625
            energy = 0.5 * BULK_MODULUS * tens * tens + LAME_MU * (dev + 0.5 * she)
            hist[energy_at] = jnp.where(g > 0.0, energy, 0.0)
        gl, g2, gs = k_lame * g, k_two * g, k_shear * g
        gt, gb, gc, g3 = k_twist * g, k_bend * g, k_cross * g, k_last * g
        pressure = gl * div
        fxX, fyY, fzZ = pressure + g2 * xX, pressure + g2 * yY, pressure + g2 * zZ
        txy, txz, tyz = gs * sxy, gs * sxz, gs * syz
        tw = xYZ + yXZ + zXY
        fxYZ, fyXZ, fzXY = gt * (xYZ + tw), gt * (yXZ + tw), gt * (zXY + tw)
        fyYZ, fxXZ = gb * yYZ + gc * xXZ, gb * xXZ + gc * yYZ
        fzYZ, fxXY = gb * zYZ + gc * xXY, gb * xXY + gc * zYZ
        fyXY, fzXZ = gb * yXY + gc * zXZ, gb * zXZ + gc * yXY
        FD = [
            fxX, fxXY, fxXZ, g3 * xXYZ,
            txy, fyXY, fyXZ, g3 * yXYZ,
            txz, fzXY, fzXZ, g3 * zXYZ,
        ]
        FS = [
            None, txy, txz, fxYZ,
            None, fyY, tyz, fyYZ,
            None, tyz, fzZ, fzYZ,
        ]
        lows = [(-FD[m]) if FS[m] is None else FS[m] - FD[m] for m in range(12)]
        highs = [FD[m] if FS[m] is None else FS[m] + FD[m] for m in range(12)]
        return lows, highs

    def element_pass(with_energy):
        def step(chunk, carry):
            r = pl.ds(pl.multiple_of(chunk * TILE, TILE), TILE)
            low = [modes[m, 0, r, :] for m in range(12)]
            held = None
            for p in range(nx - 1):
                high = [modes[m, p + 1, r, :] for m in range(12)]
                lows, highs = element(
                    low, high, stiff[p, r, :], (p, r, slice(None)) if with_energy else None
                )
                for m in range(12):
                    modes[m, p, r, :] = lows[m] + held[m] if p else lows[m]
                held, low = highs, high
            for m in range(12):
                modes[m, nx - 1, r, :] = held[m]
            low = [modes[m, GZ, r, :] for m in range(12)]
            lows, highs = element(
                low, [plane_up(a) for a in low], stiff[GZ, r, :],
                (GZ, r, slice(None)) if with_energy else None,
            )
            for m in range(12):
                modes[m, GZ, r, :] = lows[m] + plane_dn(highs[m])
            return carry

        lax.fori_loop(0, rows // TILE, step, 0, unroll=True)

    def each_node(emit, carry):
        ghosts = [half_back(*(modes[4 * c + m, GZ] for m in range(4))) for c in range(3)]
        taken = [pltpu.roll(g[1], 1, 1) for g in ghosts]
        for q in range(nx):
            got = []
            for c in range(3):
                near_w, far_w = half_back(*(modes[4 * c + m, q] for m in range(4)))
                got.append(near_w + z_dn(far_w, ghosts[c][1], q))
                taken[c] = z_dn_take(taken[c], far_w, q)
            carry = emit(q, got, carry)
        emit(GZ, [ghosts[c][0] + taken[c] for c in range(3)], carry)
        return carry

    nd, ng = DISP_ITERS, DMG_ITERS
    gram, vector = {}, {}

    def load_start(c, q):
        return gz_wide[c] if q == GZ else load_wide(c, q)

    pass_one(load_start, merge, rows, True)
    element_pass(True)
    hist[nx - 1] = blank
    arrive(1)
    greet(hop_sem)
    for f in range(DEEP, fields):
        gz_rows[f - DEEP + 1] = line_rows(*ghost_tiles(f))
    gather_back(stiff, inv_emit)

    def start_emit(q, got, dot):
        inv = inverse[q]
        for c in range(3):
            r = load_rows(DEEP + c, q) - got[c]
            v = inv * r
            basis[c, q] = v
            if q < nx:
                resid[c, q] = r[0:TILE]
                dot = dot + v[0:TILE] * r[0:TILE]
        return dot

    vector[0] = each_node(start_emit, zero)

    def hist_emit(q, total):
        react[q] = jnp.maximum(jnp.abs(load_rows(7, q)), 0.125 * total)

    gather_back(hist, hist_emit)

    for k in range(nd - 1):
        pass_one(lambda c, q, k=k: basis[3 * k + c, q], same, rows, True)
        element_pass(False)

        def apply_emit(q, got, carry, k=k):
            carry = list(carry)
            inv = inverse[q] * (2.0 / SPECTRUM)
            for c in range(3):
                w = got[c]
                here = basis[3 * k + c, q]
                v = inv * w - here
                if k:
                    v = 2.0 * v - basis[3 * (k - 1) + c, q]
                basis[3 * (k + 1) + c, q] = v
                if q < nx:
                    wi, vi = w[0:TILE], v[0:TILE]
                    if k + 2 < nd:
                        images[3 * k + c, q] = wi
                    carry[0] = carry[0] + here[0:TILE] * wi
                    carry[1] = carry[1] + vi * resid[c, q]
                    carry[2] = carry[2] + vi * wi
                    for j in range(k):
                        carry[3 + j] = carry[3 + j] + vi * images[3 * j + c, q]
            return tuple(carry)

        got = each_node(apply_emit, (zero,) * (3 + k))
        gram[k, k], vector[k + 1], gram[k + 1, k] = got[:3]
        for j in range(k):
            gram[k + 1, j] = got[3 + j]

    across = pl.ds((1 - gx) * lx, lx)
    x_basis = xcopy(basis.at[:, across, 0:TILE], basis_part, 2)
    x_basis.start()

    def last_energy():
        pass_one(lambda c, q: basis[3 * (nd - 1) + c, q], same, TILE, False)
        total = zero
        for r in (slice(0, TILE),):
            low = [modes[m, 0, r, :] for m in range(12)]
            for p in range(nx - 1):
                high = [modes[m, p + 1, r, :] for m in range(12)]
                S = [low[m] + high[m] if m % 4 else None for m in range(12)]
                D = [high[m] - low[m] for m in range(12)]
                xX, xXY, xXZ, xXYZ = D[0:4]
                yX, yXY, yXZ, yXYZ = D[4:8]
                zX, zXY, zXZ, zXYZ = D[8:12]
                _, xY, xZ, xYZ = S[0:4]
                _, yY, yZ, yYZ = S[4:8]
                _, zY, zZ, zYZ = S[8:12]
                div = xX + yY + zZ
                sxy, sxz, syz = xY + yX, xZ + zX, yZ + zY
                tw = xYZ + yXZ + zXY
                sum_two = xX * xX + yY * yY + zZ * zZ
                sum_shear = sxy * sxy + sxz * sxz + syz * syz
                sum_twist = xYZ * xYZ + yXZ * yXZ + zXY * zXY + tw * tw
                sum_bend = (yYZ * yYZ + xXZ * xXZ) + (zYZ * zYZ + xXY * xXY) + (yXY * yXY + zXZ * zXZ)
                sum_cross = yYZ * xXZ + zYZ * xXY + yXY * zXZ
                sum_last = xXYZ * xXYZ + yXYZ * yXYZ + zXYZ * zXYZ
                energy = (
                    (k_lame * (div * div) + k_two * sum_two)
                    + (k_shear * sum_shear + k_twist * sum_twist)
                    + (k_bend * sum_bend + (2.0 * k_cross) * sum_cross)
                    + k_last * sum_last
                ) * stiff[p, r, :]
                total = total + energy
                low = high
        return total

    gram[nd - 1, nd - 1] = last_energy()

    cy = yvalid + element_at(ypos - 1, ngy * ly)
    cz = element_at(zpos, ngz * lz) + element_at(zpos - 1, ngz * lz)
    czg = element_at(zghost, ngz * lz) + element_at(zghost - 1, ngz * lz)
    cxg = jnp.where((lane < 16) | (lane >= 16 * (nx - 1)), 1.0, 2.0)
    node = jnp.where(cy * cz > 0.0, 1.0, 0.0)
    gnode = jnp.where(cy * czg > 0.0, 1.0, 0.0)
    diag_scale = laplace_diag * TOUGHNESS * LENGTH_SCALE
    lap_scale = TOUGHNESS * LENGTH_SCALE / 36.0

    def lines(d, after, before, count_z):
        s, n = after + before, count_z * d
        mass, slope = 2.0 * n + s, n - s
        s, n = y_up(mass) + y_dn(mass), cy * mass
        both = 2.0 * n + s
        mixed = (n - s) + (2.0 * (cy * slope) + (y_up(slope) + y_dn(slope)))
        return 2.0 * mixed + both, mixed - both

    def laplace_pass(load, emit, carry, with_ghost):
        ghost = load(GZ)
        after = pltpu.roll(ghost, 127, 1)
        before = pltpu.roll(ghost, 1, 1)
        ahead = []
        for q in range(nx):
            d = load(q)
            ahead.append(lines(d, z_up(d, ghost, q), z_dn(d, ghost, q), cz))
            if with_ghost:
                after = z_up_take(after, d, q)
                before = z_dn_take(before, d, q)
            p = q - 1
            if p >= 0:
                total = ahead[p][0] if p == 0 else 2.0 * ahead[p][0] + ahead[p - 1][1]
                carry = emit(p, lap_scale * (total + ahead[q][1]), carry)
        carry = emit(nx - 1, lap_scale * (ahead[nx - 1][0] + ahead[nx - 2][1]), carry)
        if with_ghost:
            inner, outer = lines(ghost, after, before, czg)
            total = cxg * inner + jnp.where(lane >= 16, plane_dn(outer), 0.0)
            total = total + jnp.where(lane < 16 * (nx - 1), plane_up(outer), 0.0)
            emit(GZ, lap_scale * total, carry)
        return carry

    def reaction_of(q):
        return TOUGHNESS / LENGTH_SCALE + 2.0 * react[q]

    def old_damage(q):
        return load_rows(3, q)

    def dstart(q, lap, dot):
        reaction = reaction_of(q)
        if q == GZ:
            count, mask = cxg * cy * czg, gnode
        else:
            count, mask = (cy * cz if q in (0, nx - 1) else 2.0 * cy * cz), node
        inv = mask / (diag_scale * count + reaction)
        dinverse[q] = inv
        r = 2.0 * react[q] - (lap + reaction * old_damage(q))
        v = inv * r
        dbasis[0, q] = v
        if q < nx:
            dresid[q] = r[0:TILE]
            dot = dot + v[0:TILE] * r[0:TILE]
        return dot

    dvector, dgram = {}, {}
    dvector[0] = laplace_pass(old_damage, dstart, zero, True)
    for k in range(ng):
        more = k + 1 < ng

        def dstep(q, lap, carry, k=k, more=more):
            carry = list(carry)
            here = dbasis[k, q]
            w = lap + reaction_of(q) * here
            if q < nx:
                carry[0] = carry[0] + here[0:TILE] * w[0:TILE]
            if more:
                v = dinverse[q] * w - here
                if k:
                    v = 2.0 * v - dbasis[k - 1, q]
                dbasis[k + 1, q] = v
                if q < nx:
                    carry[1] = carry[1] + v[0:TILE] * dresid[q]
                    carry[2] = carry[2] + v[0:TILE] * w[0:TILE]
            return tuple(carry)

        got = laplace_pass(
            lambda q, k=k: dbasis[k, q], dstep, (zero,) * (3 if more else 1), more
        )
        dgram[k, k] = got[0]
        if more:
            dvector[k + 1], dgram[k + 1, k] = got[1:]

    parts = [vector[i] for i in range(nd)] + [dvector[i] for i in range(ng)]
    parts += [gram[i, j] for i in range(nd) for j in range(i + 1)]
    parts += [dgram[i, j] for i in range(ng) for j in range(i + 1)]
    at = lax.broadcasted_iota(jnp.int32, (1, 128), 1)
    packed = jnp.zeros((1, 128), f32)
    for i, piece in enumerate(parts):
        line = jnp.sum(piece, axis=0, keepdims=True)
        packed = jnp.where(at == i, jnp.sum(line, axis=1, keepdims=True), packed)
    slot_mine = gx * npeer + me
    sums[slot_mine] = packed
    pl.semaphore_wait(hop_sem, number_near)

    def peer(dy, dz):
        return lax.rem(gy + dy, ngy), lax.rem(gz + dz, ngz)

    def peer_copy(side, dy, dz, slot):
        k = side * npeer + dy * ngz + dz
        return remote(
            sums.at[slot_mine], sums.at[slot], asend_sem.at[k], arecv_sem.at[k],
            (gx if side == 0 else 1 - gx, *peer(dy, dz)),
        )

    offsets = sorted(
        [(dy, dz) for dy in range(ngy) for dz in range(ngz)],
        key=lambda o: -(2 * (o[1] % 2) + (o[1] > 0) + o[0] % 2 + (o[0] > 0)),
    )
    peers = [(side, dy, dz) for dy, dz in offsets for side in (0, 1) if side or dy or dz]
    sends = [peer_copy(side, dy, dz, slot_mine) for side, dy, dz in peers]
    for s in sends:
        s.start()
    x_damage = xcopy(dbasis.at[:, across, 0:TILE], dbasis_part, 3)
    x_damage.start()
    x_react = xcopy(react.at[across, 0:TILE], react_part, 4)
    x_react.start()
    x_parts = [x_basis, x_damage, x_react]
    for passed in x_parts:
        passed.wait_recv()

    def both_tiles(near_tile, far_tile):
        return jnp.concatenate(order(near_tile, far_tile), axis=0)

    for p in range(lx):
        out_history[p] = both_tiles(react[gx * lx + p, 0:TILE], react_part[p])
    for side, dy, dz in peers:
        from_x = gx if side == 0 else 1 - gx
        from_y, from_z = peer(ngy - dy, ngz - dz)
        peer_copy(side, dy, dz, from_x * npeer + from_y * ngz + from_z).wait_recv()
    layer = [sums[i] for i in range(2 * npeer)]
    while len(layer) > 1:
        layer = [a + b for a, b in zip(layer[::2], layer[1::2])] + layer[len(layer) & ~1 :]
    whole = layer[0]

    scalars = [
        jnp.sum(jnp.where(at == i, whole, 0.0), axis=1, keepdims=True) for i in range(len(parts))
    ]

    def solve(rhs, lower):
        n = len(rhs)
        A = [[lower[max(i, j)][min(i, j)] for j in range(n)] for i in range(n)]
        b = list(rhs)
        for i in range(n):
            pivot = 1.0 / A[i][i]
            for r in range(i + 1, n):
                ratio = A[r][i] * pivot
                for c in range(i + 1, n):
                    A[r][c] = A[r][c] - ratio * A[i][c]
                b[r] = b[r] - ratio * b[i]
        out = [None] * n
        for i in reversed(range(n)):
            s = b[i]
            for j in range(i + 1, n):
                s = s - A[i][j] * out[j]
            out[i] = s / A[i][i]
        return out

    def triangle(flat, n):
        return [[flat[k * (k + 1) // 2 + j] for j in range(k + 1)] for k in range(n)]

    rest = scalars[nd + ng :]
    cut = nd * (nd + 1) // 2
    weights = solve(scalars[:nd], triangle(rest[:cut], nd))
    dweights = solve(scalars[nd : nd + ng], triangle(rest[cut:], ng))
    for p in range(lx):
        at_x = gx * lx + p
        for c in range(3):
            near_x = far_x = zero
            for k in range(nd):
                near_x = near_x + weights[k] * basis[3 * k + c, at_x, 0:TILE]
                far_x = far_x + weights[k] * basis_part[3 * k + c, p]
            lower, upper = order(near_x, far_x)
            out_disp[c, p, 0:TILE] = full_deep[c, 0, at_x] + lower
            out_disp[c, p, TILE:ly] = full_deep[c, 1, at_x] + upper
        near_d = far_d = zero
        for k in range(ng):
            near_d = near_d + dweights[k] * dbasis[k, at_x, 0:TILE]
            far_d = far_d + dweights[k] * dbasis_part[k, p]
        lower, upper = order(near_d, far_d)
        out_damage[p, 0:TILE] = full_deep[3, 0, at_x] + lower
        out_damage[p, TILE:ly] = full_deep[3, 1, at_x] + upper

    for guard, copy in halos[0] + halos[1]:
        pl.when(guard)(copy.wait_send)
    for passed in x_own + x_parts:
        passed.wait_send()
    for s in sends:
        s.wait_send()


def hand_on(*refs):
    sources, targets, sem = refs[:3], refs[3:6], refs[6]
    copies = [
        pltpu.make_async_copy(source, target, sem.at[i])
        for i, (source, target) in enumerate(zip(sources, targets))
    ]
    for copy in copies:
        copy.start()
    for copy in copies:
        copy.wait()


def body_fused(sizes, *arrays):
    ngy, ngz, lx, ly, lz = sizes
    nx, rows, wide, fields = 2 * lx, 2 * TILE, 3 * TILE, 8
    packs, pairs, extras = fields * lx // 16, DEEP * lx // 2, DEEP * lx // TILE
    npeer = ngy * ngz
    f32 = jnp.float32
    planes = (nx + 1, rows, lz)
    vmem = pl.BlockSpec(memory_space=pltpu.VMEM)
    hbm = pl.BlockSpec(memory_space=pltpu.HBM)
    dma = pltpu.SemaphoreType.DMA

    def room(*shape):
        return pltpu.VMEM(shape, f32)

    results = pl.pallas_call(
        functools.partial(kernel, sizes),
        out_shape=(
            pltpu.VMEM((3, lx, ly, lz), f32),
            pltpu.VMEM((lx, ly, lz), f32),
            pltpu.VMEM((lx, ly, lz), f32),
        ),
        in_specs=[hbm] * 6,
        out_specs=(vmem,) * 3,
        scratch_shapes=[
            room(3, lx, ly, lz),
            room(3, lx, ly, lz),
            room(lx, ly, lz),
            room(lx, ly, lz),
            pltpu.VMEM((lx, ly, lz), jnp.int32),
            pltpu.VMEM((lx, ly, lz), jnp.int32),
            room(DEEP, 2, nx, TILE, lz),
            room(DEEP, 2, nx, TILE, lz),
            room(pairs + extras, TILE, 128),
            room(pairs, TILE, 128),
            room(pairs, TILE, 128),
            room(pairs, TILE, 128),
            room(2, pairs + extras, TILE, 128),
            room(2, pairs, TILE, 128),
            room(2, 2, TILE, 128),
            room(2, 2, TILE, 128),
            room(2, 2, 3, TILE, 128),
            room(2, 2, 3, TILE, 128),
            room(4, wide, 128),
            room(5, rows, 128),
            room(12, *planes),
            room(3 * DISP_ITERS, *planes),
            room(3 * (DISP_ITERS - 2), nx, TILE, lz),
            room(3, nx, TILE, lz),
            room(*planes),
            room(*planes),
            room(*planes),
            room(*planes),
            room(*planes),
            room(DMG_ITERS, *planes),
            room(nx, TILE, lz),
            room(3 * DISP_ITERS, lx, TILE, lz),
            room(DMG_ITERS, lx, TILE, lz),
            room(lx, TILE, lz),
            room(2 * npeer, 1, 128),
            dma((6,)),
            dma((4,)),
            dma((4,)),
            dma((8,)),
            dma((8,)),
            dma((8,)),
            dma((8,)),
            dma((5,)),
            dma((5,)),
            dma((2 * npeer,)),
            dma((2 * npeer,)),
            pltpu.SemaphoreType.REGULAR,
        ],
        compiler_params=pltpu.CompilerParams(
            collective_id=0, has_side_effects=True, vmem_limit_bytes=VMEM_LIMIT
        ),
    )(*[pltpu.with_memory_space_constraint(a, pltpu.HBM) for a in arrays])
    return pl.pallas_call(
        hand_on,
        out_shape=tuple(jax.ShapeDtypeStruct(r.shape, f32) for r in results),
        in_specs=[vmem] * 3,
        out_specs=(hbm,) * 3,
        scratch_shapes=[dma((3,))],
        compiler_params=pltpu.CompilerParams(vmem_limit_bytes=1024 * 1024),
    )(*[pltpu.with_memory_space_constraint(r, pltpu.VMEM) for r in results])


VMEM_LIMIT = 24 * 1024 * 1024


def solution(mesh):
    shape = dict(mesh.shape)

    def body(*arrays):
        lx, ly, lz = arrays[2].shape
        fits = shape["gx"] == 2 and shape["gy"] * shape["gz"] > 1
        fits = fits and max(shape["gy"], shape["gz"]) <= 4
        fits = fits and lx == 4 and ly == 2 * TILE and lz == 128
        if fits:
            return body_fused((shape["gy"], shape["gz"], lx, ly, lz), *arrays)
        return body_any_mesh(*arrays)

    return jax.shard_map(
        body,
        mesh=mesh,
        in_specs=(
            P(None, "gx", "gy", "gz"),
            P(None, "gx", "gy", "gz"),
            P("gx", "gy", "gz"),
            P("gx", "gy", "gz"),
            P("gx", "gy", "gz"),
            P("gx", "gy", "gz"),
        ),
        out_specs=(P(None, "gx", "gy", "gz"), P("gx", "gy", "gz"), P("gx", "gy", "gz")),
        check_vma=False,
    )
```

```python
import functools
import jax
import jax.numpy as jnp
import numpy as np
from jax import lax
from jax.experimental import pallas as pl
from jax.experimental.pallas import tpu as pltpu
from jax.sharding import PartitionSpec as P

DISP_ITERS = 4
DMG_ITERS = 2


LAME_LAMBDA = 0.5769230769230769
LAME_MU = 0.38461538461538464
BULK_MODULUS = LAME_LAMBDA + 2.0 * LAME_MU / 3.0
RESIDUAL_STIFFNESS = 0.001
TOUGHNESS = 1.0
LENGTH_SCALE = 2.0
CRACK_HISTORY = 40.0


def padded_2(cells, sides, width):
    for axis, dim in sides:
        count = lax.axis_size(axis)
        ends = count - 1
        head = lax.slice_in_dim(cells, 0, width, axis=dim)
        tail = lax.slice_in_dim(cells, cells.shape[dim] - width, cells.shape[dim], axis=dim)
        cells = jnp.concatenate(
            [
                lax.ppermute(tail, axis, [(i, (i + 1) % count) for i in range(ends)]),
                cells,
                lax.ppermute(head, axis, [((i + 1) % count, i) for i in range(ends)]),
            ],
            axis=dim,
        )
    return cells


def corner_offsets(corner):
    return (corner >> 2 & 1, corner >> 1 & 1, corner & 1)


def shape_gradients(sample):
    gradient = np.zeros((3, 8))
    for corner in range(8):
        offsets = corner_offsets(corner)
        values = [sample[k] if offsets[k] else 1.0 - sample[k] for k in range(3)]
        slopes = [1.0 if offsets[k] else -1.0 for k in range(3)]
        gradient[0, corner] = slopes[0] * values[1] * values[2]
        gradient[1, corner] = values[0] * slopes[1] * values[2]
        gradient[2, corner] = values[0] * values[1] * slopes[2]
    return gradient


def strain_matrix(gradient):
    strain = np.zeros((6, 24))
    for corner in range(8):
        column = 3 * corner
        strain[0, column] = gradient[0, corner]
        strain[1, column + 1] = gradient[1, corner]
        strain[2, column + 2] = gradient[2, corner]
        strain[3, column] = gradient[1, corner]
        strain[3, column + 1] = gradient[0, corner]
        strain[4, column + 1] = gradient[2, corner]
        strain[4, column + 2] = gradient[1, corner]
        strain[5, column] = gradient[2, corner]
        strain[5, column + 2] = gradient[0, corner]
    return strain


def element_tables():
    moduli = np.zeros((6, 6))
    moduli[:3, :3] = LAME_LAMBDA
    for k in range(3):
        moduli[k, k] += 2.0 * LAME_MU
        moduli[k + 3, k + 3] = LAME_MU
    points = [0.5 - 0.5 / np.sqrt(3.0), 0.5 + 0.5 / np.sqrt(3.0)]
    stiff_table = np.zeros((24, 24))
    laplace_table = np.zeros((8, 8))
    for sample_index in range(8):
        sample = tuple((points[k] for k in corner_offsets(sample_index)))
        gradient = shape_gradients(sample)
        strain = strain_matrix(gradient)
        stiff_table += 0.125 * strain.T @ moduli @ strain
        laplace_table += 0.125 * gradient.T @ gradient
    centre_table = strain_matrix(shape_gradients((0.5, 0.5, 0.5)))
    return (
        stiff_table.astype(np.float32),
        laplace_table.astype(np.float32),
        centre_table.astype(np.float32),
    )


def corner_views(padded, element_shape):
    corner_list = []
    for corner in range(8):
        offx, offy, offz = corner_offsets(corner)
        corner_list.append(
            padded[
                ...,
                offx : offx + element_shape[0],
                offy : offy + element_shape[1],
                offz : offz + element_shape[2],
            ]
        )
    return corner_list


def assemble_nodes(pieces):
    running = None
    for corner in range(8):
        offx, offy, offz = corner_offsets(corner)
        leading = [(0, 0)] * (pieces[corner].ndim - 3)
        placed = jnp.pad(
            pieces[corner], leading + [(offx, 1 - offx), (offy, 1 - offy), (offz, 1 - offz)]
        )
        running = placed if running is None else running + placed
    return running


def line_valid(position, devices, count):
    index = position * count + jnp.arange(count + 1, dtype=jnp.int32) - 1
    return ((index >= 0) & (index <= devices * count - 2)).astype(jnp.float32)


def strain_energy(strain):
    trace = strain[0] + strain[1] + strain[2]
    deviator = strain[:3] - trace[None] / 3.0
    shear = strain[3:]
    tensile = jnp.maximum(trace, 0.0)
    return 0.5 * BULK_MODULUS * tensile * tensile + LAME_MU * (
        jnp.sum(deviator * deviator, axis=0) + 0.5 * jnp.sum(shear * shear, axis=0)
    )


def forces_to_nodes(forces, stiffness):
    pieces = [stiffness[None] * forces[3 * target : 3 * target + 3] for target in range(8)]
    return assemble_nodes(pieces)


def element_apply(padded, stiffness, stiff_table):
    element_shape = stiffness.shape
    flat = jnp.stack(corner_views(padded, element_shape)).reshape(24, -1)
    forces = jnp.dot(stiff_table, flat, precision=lax.Precision.HIGHEST).reshape(
        (24,) + element_shape
    )
    return forces_to_nodes(forces, stiffness)


def laplace_apply(padded, element_valid, laplace_table):
    element_shape = element_valid.shape
    flat = jnp.stack(corner_views(padded, element_shape)).reshape(8, -1)
    forces = jnp.dot(laplace_table, flat, precision=lax.Precision.HIGHEST).reshape(
        (8,) + element_shape
    )
    return assemble_nodes([element_valid * forces[target] for target in range(8)])


def single_pair(pair):
    return tuple(lax.psum(pair, ("gx", "gy", "gz")))


def conjugate(solutions, residuals, inverses, counts, apply_fn):
    solutions = list(solutions)
    residuals = list(residuals)
    number = len(solutions)
    steps = max(counts)

    def pair_totals(pairs):
        return [single_pair(pairs[0])]

    precs = [inverses[0] * residuals[0]]
    applied = apply_fn(precs, list(range(number)))
    pairs = pair_totals([(jnp.sum(residuals[0] * precs[0]), jnp.sum(precs[0] * applied[0]))])
    norms = [pair[0] for pair in pairs]
    lengths = [pair[0] / pair[1] for pair in pairs]
    directions = list(precs)
    alongs = list(applied)
    for step in range(steps):
        active = [i for i in range(number) if step < counts[i]]
        for i in active:
            solutions[i] = solutions[i] + lengths[i] * directions[i]
            residuals[i] = residuals[i] - lengths[i] * alongs[i]
        later = [i for i in active if step + 1 < counts[i]]
        if later:
            i = later[0]
            precs[i] = inverses[i] * residuals[i]
            images = apply_fn([precs[i] for i in later], later)
            pairs = pair_totals(
                [
                    (jnp.sum(residuals[i] * precs[i]), jnp.sum(precs[i] * images[k]))
                    for k, i in enumerate(later)
                ]
            )
            for k, i in enumerate(later):
                norm_next, curve_sum = pairs[k]
                ratio = norm_next / norms[i]
                lengths[i] = norm_next / (curve_sum - ratio * norm_next / lengths[i])
                directions[i] = precs[i] + ratio * directions[i]
                alongs[i] = images[k] + ratio * alongs[i]
                norms[i] = norm_next
    return solutions


def body_any_mesh(displacement_start, external_force, damage_old, history_old, crack_labels, fixed_flags):
    tables = element_tables()
    stiff_table = jnp.asarray(tables[0], jnp.float32)
    laplace_table = jnp.asarray(tables[1], jnp.float32)
    centre_table = jnp.asarray(tables[2], jnp.float32)
    highest = lax.Precision.HIGHEST
    size_x, size_y, size_z = damage_old.shape
    free_mask = 1.0 - fixed_flags.astype(jnp.float32)
    start_disp = displacement_start * free_mask[None]
    element_valid = (
        line_valid(lax.axis_index("gx"), lax.axis_size("gx"), size_x)[:, None, None]
        * line_valid(lax.axis_index("gy"), lax.axis_size("gy"), size_y)[None, :, None]
        * line_valid(lax.axis_index("gz"), lax.axis_size("gz"), size_z)[None, None, :]
    )
    element_shape = element_valid.shape
    start_pad = padded_2(
        jnp.concatenate([start_disp, damage_old[None]], axis=0),
        (("gx", 1), ("gy", 2), ("gz", 3)),
        1,
    )
    corner_list = corner_views(start_pad, element_shape)
    damage_mean = sum((view[3] for view in corner_list)) / 8.0
    stiffness = ((1.0 - damage_mean) ** 2 + RESIDUAL_STIFFNESS) * element_valid
    flat = jnp.stack([view[:3] for view in corner_list]).reshape(24, -1)
    combined = jnp.dot(
        jnp.concatenate([stiff_table, centre_table], axis=0), flat, precision=highest
    )
    forces = combined[:24].reshape((24,) + element_shape)
    strain = combined[24:].reshape((6,) + element_shape)
    start_image = forces_to_nodes(forces, stiffness)[:, 1:-1, 1:-1, 1:-1]
    energy = strain_energy(strain) * element_valid
    nodal_energy = assemble_nodes([energy] * 8)[1:-1, 1:-1, 1:-1] / 8.0
    history = jnp.maximum(
        jnp.maximum(history_old, nodal_energy), CRACK_HISTORY * crack_labels.astype(jnp.float32)
    )
    stiff_diag = jnp.diagonal(stiff_table)
    diag_pieces = [
        stiffness[None] * stiff_diag[3 * target : 3 * target + 3][:, None, None, None]
        for target in range(8)
    ]
    elastic_diag = assemble_nodes(diag_pieces)[:, 1:-1, 1:-1, 1:-1]
    inverse_elastic = 1.0 / (free_mask[None] * elastic_diag + (1.0 - free_mask[None]))

    def constrained(nodal_field):
        masked = free_mask[None] * nodal_field
        padded = padded_2(masked, (("gx", 1), ("gy", 2), ("gz", 3)), 1)
        nodes = element_apply(padded, stiffness, stiff_table)[:, 1:-1, 1:-1, 1:-1]
        return free_mask[None] * nodes + (1.0 - free_mask[None]) * nodal_field

    reaction = TOUGHNESS / LENGTH_SCALE + 2.0 * history
    laplace_diag = assemble_nodes(
        [element_valid * laplace_table[target, target] for target in range(8)]
    )[1:-1, 1:-1, 1:-1]
    inverse_damage = 1.0 / (TOUGHNESS * LENGTH_SCALE * laplace_diag + reaction)
    residual = free_mask[None] * (external_force - start_image)
    start_lap = laplace_apply(start_pad[3], element_valid, laplace_table)[1:-1, 1:-1, 1:-1]
    damage_residual = 2.0 * history - (TOUGHNESS * LENGTH_SCALE * start_lap + reaction * damage_old)

    def damage_operator(nodal_field):
        padded = padded_2(nodal_field, (("gx", 0), ("gy", 1), ("gz", 2)), 1)
        lap_nodes = laplace_apply(padded, element_valid, laplace_table)[1:-1, 1:-1, 1:-1]
        return TOUGHNESS * LENGTH_SCALE * lap_nodes + reaction * nodal_field

    def single_elastic(fields, active):
        return [constrained(fields[0])]

    def single_damage(fields, active):
        return [damage_operator(fields[0])]

    displacement = conjugate(
        [start_disp], [residual], [inverse_elastic], [DISP_ITERS], single_elastic
    )[0]
    damage = conjugate(
        [damage_old], [damage_residual], [inverse_damage], [DMG_ITERS], single_damage
    )[0]
    return (displacement, damage, history)


SPECTRUM = 3.2
TILE = 8
GHOST = 4
DEEP = 4
MESH = pl.DeviceIdType.MESH


def walsh_tables():
    stiff, laplace, _ = element_tables()
    signs = np.array(
        [
            [np.prod([1.0 if c >> k & 1 else (-1.0 if m >> k & 1 else 1.0) for k in range(3)]) for c in range(8)]
            for m in range(8)
        ]
    )
    wide = np.kron(signs, np.eye(3))
    stiff_modes = wide @ stiff.astype(np.float64) @ wide.T / 64.0
    return stiff_modes, float(stiff[0, 0]), float(laplace[0, 0])


def kernel(
    sizes,
    disp_in,
    force_in,
    damage_in,
    history_in,
    labels_in,
    flags_in,
    out_disp,
    out_damage,
    out_history,
    disp_ref,
    force_ref,
    damage_ref,
    history_ref,
    labels_ref,
    flags_ref,
    full_deep,
    full_flat,
    down_deep,
    up_deep,
    down_flat,
    up_flat,
    ghost_deep,
    ghost_flat,
    zsend_deep,
    zsend_flat,
    zbuf_deep,
    zbuf_flat,
    gz_wide,
    gz_rows,
    modes,
    basis,
    images,
    resid,
    stiff,
    inverse,
    hist,
    react,
    dinverse,
    dbasis,
    dresid,
    basis_part,
    dbasis_part,
    react_part,
    sums,
    in_sem,
    ysend_sem,
    yrecv_sem,
    zsend_sem,
    zrecv_sem,
    csend_sem,
    crecv_sem,
    xsend_sem,
    xrecv_sem,
    asend_sem,
    arecv_sem,
    hop_sem,
):
    ngy, ngz, lx, ly, lz = sizes
    nx = 2 * lx
    fields = 8
    npeer = ngy * ngz
    pairs = DEEP * lx // 2
    packs = fields * lx // 16
    extras = DEEP * lx // TILE
    wide, rows = 3 * TILE, 2 * TILE
    GZ = nx
    f32 = jnp.float32
    stiff_modes, stiff_diag, laplace_diag = walsh_tables()
    gx, gy, gz = lax.axis_index("gx"), lax.axis_index("gy"), lax.axis_index("gz")
    me = gy * ngz + gz
    partner = (1 - gx, gy, gz)
    outward = 2 * gx - 1
    full, zsend, zbuf = (full_deep, full_flat), (zsend_deep, zsend_flat), (zbuf_deep, zbuf_flat)

    def there(dy, dz):
        y, z = gy + dy, gz + dz
        return (y >= 0) & (y < ngy) & (z >= 0) & (z < ngz)

    def device(core, dy, dz):
        return core, lax.rem(gy + dy + ngy, ngy), lax.rem(gz + dz + ngz, ngz)

    near = [(dy, dz) for dy in (-1, 0, 1) for dz in (-1, 0, 1) if dy or dz]
    number_near = 2 * sum(there(dy, dz).astype(jnp.int32) for dy, dz in near)

    barrier = pltpu.get_barrier_semaphore()

    def greet(semaphore):
        for dy, dz in near:

            @pl.when(there(dy, dz))
            def _():
                for core in (gx, 1 - gx):
                    pl.semaphore_signal(
                        semaphore, inc=1, device_id=device(core, dy, dz), device_id_type=MESH
                    )

    greet(barrier)
    pl.semaphore_signal(barrier, inc=1, device_id=partner, device_id_type=MESH)

    loads = [
        pltpu.make_async_copy(source, target, in_sem.at[i])
        for i, (source, target) in enumerate(
            [
                (flags_in, flags_ref),
                (disp_in, disp_ref),
                (force_in, force_ref),
                (damage_in, damage_ref),
                (history_in, history_ref),
                (labels_in, labels_ref),
            ]
        )
    ]
    for load in loads:
        load.start()

    zero = jnp.zeros((TILE, 128), f32)
    for dz, side in ((1, 0), (-1, 1)):

        @pl.when(jnp.logical_not(there(0, dz)))
        def _():
            for core in range(2):
                for ref in zbuf:
                    ref[core, side, 0:2] = jnp.zeros((2, TILE, 128), f32)

        @pl.when(jnp.logical_not(there(outward, dz)))
        def _():
            for core in range(2):
                for ref in zbuf:
                    ref[core, side, 2] = zero

    @pl.when(jnp.logical_not(there(outward, 0)))
    def _():
        ghost_deep[...] = jnp.zeros(ghost_deep.shape, f32)
        ghost_flat[...] = jnp.zeros(ghost_flat.shape, f32)

    for load in loads:
        load.wait()

    values = []
    for p in range(lx):
        flag = flags_ref[p].astype(f32)
        free = 1.0 - flag
        top = jnp.maximum(history_ref[p], CRACK_HISTORY * labels_ref[p].astype(f32))
        here = [free * disp_ref[c, p] for c in range(3)]
        here += [damage_ref[p]] + [force_ref[c, p] for c in range(3)] + [top * (free - flag)]
        for f in range(fields):
            for half in range(2):
                full[f // DEEP][f % DEEP, half, gx * lx + p] = here[f][TILE * half : TILE * half + TILE]
        values.append(here)

    sub = lax.broadcasted_iota(jnp.int32, (TILE, 128), 0)

    def spin(a, shift, axis):
        shift = shift % a.shape[axis]
        return pltpu.roll(a, shift, axis) if shift else a

    def spot(f, q):
        return 8 * (f % 4 // 2) + 2 * q + f % 2

    group = lax.broadcasted_iota(jnp.int32, (ly, 128), 1) // 8
    for j in range(packs):
        low = jnp.zeros((ly, 128), f32)
        high = jnp.zeros((ly, 128), f32)
        for f in range(4 * j, 4 * j + 4):
            for q in range(lx):
                k = spot(f, q)
                turned = spin(values[q][f], 8 * k + 8, 1)
                low = jnp.where(group == (k + 1) % 16, turned, low)
                high = jnp.where(group == k, turned, high)
        for half in range(2):
            zsend[j][0, half] = low[TILE * half : TILE * half + TILE]
            zsend[j][1, half] = high[TILE * half : TILE * half + TILE]
    for first, down, up in ((0, down_deep, up_deep), (DEEP, down_flat, up_flat)):
        for j in range(pairs):
            fa, qa = divmod(2 * j, lx)
            fb, qb = divmod(2 * j + 1, lx)
            a, b = values[qa][first + fa], values[qb][first + fb]
            down[j] = jnp.where(sub < GHOST, a[0:TILE], spin(b[0:TILE], GHOST, 0))
            up[j] = jnp.where(sub < GHOST, spin(b[ly - TILE : ly], GHOST, 0), a[ly - TILE : ly])
    for e in range(extras):
        tile = jnp.zeros((TILE, 128), f32)
        for s in range(TILE):
            f, q = divmod(TILE * e + s, lx)
            tile = jnp.where(sub == s, spin(values[q][f][0:TILE], s - GHOST, 0), tile)
        down_deep[pairs + e] = tile

    pl.semaphore_wait(barrier, number_near + 1)

    def remote(src, dst, send, recv, target):
        return pltpu.make_async_remote_copy(
            src_ref=src, dst_ref=dst, send_sem=send, recv_sem=recv,
            device_id=target, device_id_type=MESH,
        )

    def xcopy(src, dst, k):
        return remote(src, dst, xsend_sem.at[k], xrecv_sem.at[k], partner)

    def zcopy(source, dz, pack, core):
        side = 0 if dz < 0 else 1
        return remote(
            zsend[pack].at[side], zbuf[pack].at[source, side, 0:2],
            zsend_sem.at[side], zrecv_sem.at[2 * side + pack],
            device(core, 0, dz),
        )

    def corner(source, dy, dz, pack):
        side = 0 if dz < 0 else 1
        return remote(
            zsend[pack].at[side, int(dy > 0)], zbuf[pack].at[source, side, 2],
            csend_sem.at[2 * (dy > 0) + side],
            crecv_sem.at[2 * side + pack],
            device(int(dy < 0), dy, dz),
        )

    def ycopy(source, dy, flat):
        if flat:
            src, dst = (down_flat if dy < 0 else up_flat), ghost_flat.at[source]
        elif dy < 0:
            src, dst = down_deep, ghost_deep.at[source]
        else:
            src, dst = up_deep, ghost_deep.at[source, 0:pairs]
        return remote(
            src, dst, ysend_sem.at[2 * flat + (dy > 0)], yrecv_sem.at[flat],
            device(int(dy < 0), dy, 0),
        )

    own = pl.ds(gx * lx, lx)
    x_own = [
        xcopy(full[flat].at[:, :, own], full[flat].at[:, :, own], flat) for flat in range(2)
    ]
    halos = [[], []]
    for flat in (0, 1):
        for source in (0, 1):
            ways = [((dy, dz), corner(source, dy, dz, flat)) for dy in (-1, 1) for dz in (-1, 1)]
            ways += [((dy, 0), ycopy(source, dy, flat)) for dy in (-1, 1)]
            ways += [((0, dz), zcopy(source, dz, flat, core)) for dz in (-1, 1) for core in (0, 1)]
            halos[flat] += [((gx == source) & there(*way), copy) for way, copy in ways]
    for flat in (0, 1):
        x_own[flat].start()
        for guard, copy in halos[flat]:
            pl.when(guard)(copy.start)

    def drain(ref, send, recv):
        return remote(ref, ref, send, recv, partner)

    def arrive(flat):
        for side, dz in ((0, -1), (1, 1)):
            faces = zbuf[flat].at[:, side, 0:2]
            pl.when(there(0, -dz))(
                drain(faces, zsend_sem.at[side], zrecv_sem.at[2 * side + flat]).wait_recv
            )
        x_own[flat].wait_recv()
        for side, dz in ((0, -1), (1, 1)):
            edges = zbuf[flat].at[:, side, 2]
            pl.when(there(outward, -dz))(
                drain(edges, csend_sem.at[side], crecv_sem.at[2 * side + flat]).wait_recv
            )
        rows_in = [ghost_flat] * 2 if flat else [ghost_deep.at[:, 0:pairs], ghost_deep]
        for core in range(2):
            pl.when((gx == core) & there(outward, 0))(
                drain(rows_in[core], ysend_sem.at[flat], yrecv_sem.at[flat]).wait_recv
            )

    arrive(0)

    lane_w = lax.broadcasted_iota(jnp.int32, (wide, 128), 1)
    odd = lane_w // 8 % 2

    def merge(a):
        return jnp.concatenate(
            [a[0:TILE], jnp.where(sub < GHOST, a[TILE : 2 * TILE], a[2 * TILE :])], axis=0
        )

    is_lower = sub + TILE * gx < TILE
    from_theirs = (sub + GHOST * gx) % TILE < GHOST

    def order(lower, upper):
        return jnp.where(is_lower, lower, upper), jnp.where(is_lower, upper, lower)

    def ghost_tiles(f):
        halves = []
        for source in range(2):
            ref = zbuf[f // 4]
            low, high = (
                jnp.concatenate([ref[source, side, k] for k in range(3)], axis=0) for side in range(2)
            )
            both = jnp.where(odd == f % 2, high, low)
            halves.append(spin(both, 8 * (2 * lx * source - spot(f, 0)), 1))
        whole = jnp.where(lane_w < 16 * lx, *halves)
        return *order(whole[0:TILE], whole[TILE : 2 * TILE]), whole[2 * TILE :]

    def line_wide(tile, other, up, down):
        return jnp.concatenate(
            [tile, jnp.where(is_lower, other, up), jnp.where(is_lower, down, other)], axis=0
        )

    def line_rows(tile, other, ghost):
        return jnp.concatenate([tile, jnp.where(from_theirs, other, ghost)], axis=0)

    for f in range(DEEP):
        tile, other, ghost = ghost_tiles(f)
        gz_wide[f] = line_wide(tile, other, ghost, ghost)
    gz_rows[0] = merge(gz_wide[DEEP - 1])

    def pieces(f, q):
        source, p = divmod(q, lx)
        j, half = divmod(f % DEEP * lx + p, 2)
        ghost = ghost_deep[source, j] if f < DEEP else ghost_flat[source, j]
        ref = full[f // DEEP]
        return *order(ref[f % DEEP, 0, q], ref[f % DEEP, 1, q]), spin(ghost, GHOST * half, 0)

    def load_wide(f, q):
        tile, other, ghost = pieces(f, q)
        e, s = divmod(f * lx + q % lx, TILE)
        extra = spin(ghost_deep[q // lx, pairs + e], GHOST - s, 0)
        return line_wide(tile, other, jnp.where(sub == GHOST, extra, ghost), ghost)

    def load_rows(f, q):
        if q == GZ:
            return gz_rows[f - DEEP + 1]
        return line_rows(*pieces(f, q))

    row = lax.broadcasted_iota(jnp.int32, (rows, 128), 0)
    lane = lax.broadcasted_iota(jnp.int32, (rows, 128), 1)
    inside = lane % 16
    ypos = gy * ly + gx * TILE + jnp.where(row < TILE + GHOST, row, row - rows)
    zpos = gz * lz + lane
    zghost = gz * lz + jnp.where(inside < 8, inside - 8, inside + (lz - 8))

    def element_at(pos, count):
        return jnp.where((pos >= 0) & (pos <= count - 2), 1.0, 0.0)

    yvalid = element_at(ypos, ngy * ly)
    valid = yvalid * element_at(zpos, ngz * lz)
    gvalid = jnp.where(lane < 16 * (nx - 1), yvalid * element_at(zghost, ngz * lz), 0.0)

    def y_up(a):
        return pltpu.roll(a, a.shape[0] - 1, 0)

    def y_dn(a):
        return pltpu.roll(a, 1, 0)

    def lanes(a):
        return lane_w if a.shape[0] == wide else lane

    def z_up(a, ghost, p):
        return jnp.where(lanes(a) == 127, spin(ghost, 119 - 16 * p, 1), pltpu.roll(a, 127, 1))

    def z_up_take(acc, a, p):
        return jnp.where(lanes(a) == 16 * p + 7, spin(a, 16 * p + 7, 1), acc)

    def z_dn(a, ghost, p):
        return jnp.where(lanes(a) == 0, spin(ghost, 121 - 16 * p, 1), pltpu.roll(a, 1, 1))

    def z_dn_take(acc, a, p):
        return jnp.where(lanes(a) == 16 * p + 8, spin(a, 16 * p + 9, 1), acc)

    def plane_up(a):
        return pltpu.roll(a, 112, 1)

    def plane_dn(a):
        return pltpu.roll(a, 16, 1)

    blank = jnp.zeros((rows, 128), f32)

    def half_back(ss, yd, zd, yz):
        s = (ss - yd) + y_dn(ss + yd)
        d = (zd - yz) + y_dn(zd + yz)
        return s - d, s + d

    def damage_sum(q):
        a = load_wide(3, q)
        s = a + z_up(a, gz_wide[3], q)
        return merge(s + y_up(s)), a

    def rigidity(low, high, mask):
        rest = 1.0 - (low + high) * 0.125
        return (rest * rest + RESIDUAL_STIFFNESS) * mask

    low, a = damage_sum(0)
    taken = z_up_take(pltpu.roll(gz_wide[3], 127, 1), a, 0)
    for q in range(nx - 1):
        high, a = damage_sum(q + 1)
        stiff[q] = rigidity(low, high, valid)
        taken = z_up_take(taken, a, q + 1)
        low = high
    taken = gz_wide[3] + taken
    taken = merge(taken + y_up(taken))
    stiff[GZ] = rigidity(taken, plane_up(taken), gvalid)
    stiff[nx - 1] = blank

    def gather_back(ref, emit):
        ghost = ref[GZ]
        below = blank
        taken = pltpu.roll(ghost, 1, 1)
        for q in range(nx):
            a = ref[q]
            s = a + z_dn(a, ghost, q)
            here = s + y_dn(s)
            emit(q, below + here)
            below = here
            taken = z_dn_take(taken, a, q)
        s = ghost + taken
        s = s + y_dn(s)
        emit(GZ, s + plane_dn(s))

    def inv_emit(q, total):
        free = load_rows(7, q) > 0.0
        inverse[q] = jnp.where(free, 1.0 / jnp.where(free, stiff_diag * total, 1.0), 0.0)

    def forward(u, near_u, keep):
        zs, zd = u + near_u, near_u - u
        a, b = keep(y_up(zs)), keep(y_up(zd))
        zs, zd = keep(zs), keep(zd)
        return zs + a, a - zs, zd + b, b - zd

    def same(a):
        return a

    def pass_one(load, keep, height, with_ghost):
        for c in range(3):
            ghost = load(c, GZ)
            taken = pltpu.roll(ghost, 127, 1)
            for q in range(nx):
                u = load(c, q)
                out = forward(u, z_up(u, ghost, q), keep)
                for m in range(4):
                    modes[4 * c + m, q, 0:height] = out[m][0:height]
                if with_ghost:
                    taken = z_up_take(taken, u, q)
            if with_ghost:
                out = forward(ghost, taken, keep)
                for m in range(4):
                    modes[4 * c + m, GZ] = out[m]

    def sm(mode_a, comp_a, mode_b, comp_b):
        return float(stiff_modes[3 * mode_a + comp_a, 3 * mode_b + comp_b])

    k_lame = sm(4, 0, 2, 1)
    k_two = sm(4, 0, 4, 0) - k_lame
    k_shear = sm(2, 0, 2, 0)
    k_twist = sm(3, 0, 5, 1)
    k_bend = sm(3, 1, 3, 1)
    k_cross = sm(3, 1, 5, 0)
    k_last = sm(7, 0, 7, 0)

    def element(low, high, g, energy_at):
        S = [low[m] + high[m] if m % 4 else None for m in range(12)]
        D = [high[m] - low[m] for m in range(12)]
        xX, xXY, xXZ, xXYZ = D[0:4]
        yX, yXY, yXZ, yXYZ = D[4:8]
        zX, zXY, zXZ, zXYZ = D[8:12]
        _, xY, xZ, xYZ = S[0:4]
        _, yY, yZ, yYZ = S[4:8]
        _, zY, zZ, zYZ = S[8:12]
        div = xX + yY + zZ
        sxy, sxz, syz = xY + yX, xZ + zX, yZ + zY
        if energy_at is not None:
            trace = 0.25 * div
            tens = jnp.maximum(trace, 0.0)
            third = trace / 3.0
            ex, ey, ez = 0.25 * xX - third, 0.25 * yY - third, 0.25 * zZ - third
            dev = ex * ex + ey * ey + ez * ez
            she = (sxy * sxy + sxz * sxz + syz * syz) * 0.0625
            energy = 0.5 * BULK_MODULUS * tens * tens + LAME_MU * (dev + 0.5 * she)
            hist[energy_at] = jnp.where(g > 0.0, energy, 0.0)
        gl, g2, gs = k_lame * g, k_two * g, k_shear * g
        gt, gb, gc, g3 = k_twist * g, k_bend * g, k_cross * g, k_last * g
        pressure = gl * div
        fxX, fyY, fzZ = pressure + g2 * xX, pressure + g2 * yY, pressure + g2 * zZ
        txy, txz, tyz = gs * sxy, gs * sxz, gs * syz
        tw = xYZ + yXZ + zXY
        fxYZ, fyXZ, fzXY = gt * (xYZ + tw), gt * (yXZ + tw), gt * (zXY + tw)
        fyYZ, fxXZ = gb * yYZ + gc * xXZ, gb * xXZ + gc * yYZ
        fzYZ, fxXY = gb * zYZ + gc * xXY, gb * xXY + gc * zYZ
        fyXY, fzXZ = gb * yXY + gc * zXZ, gb * zXZ + gc * yXY
        FD = [
            fxX, fxXY, fxXZ, g3 * xXYZ,
            txy, fyXY, fyXZ, g3 * yXYZ,
            txz, fzXY, fzXZ, g3 * zXYZ,
        ]
        FS = [
            None, txy, txz, fxYZ,
            None, fyY, tyz, fyYZ,
            None, tyz, fzZ, fzYZ,
        ]
        lows = [(-FD[m]) if FS[m] is None else FS[m] - FD[m] for m in range(12)]
        highs = [FD[m] if FS[m] is None else FS[m] + FD[m] for m in range(12)]
        return lows, highs

    def element_pass(with_energy):
        def step(chunk, carry):
            r = pl.ds(pl.multiple_of(chunk * TILE, TILE), TILE)
            low = [modes[m, 0, r, :] for m in range(12)]
            held = None
            for p in range(nx - 1):
                high = [modes[m, p + 1, r, :] for m in range(12)]
                lows, highs = element(
                    low, high, stiff[p, r, :], (p, r, slice(None)) if with_energy else None
                )
                for m in range(12):
                    modes[m, p, r, :] = lows[m] + held[m] if p else lows[m]
                held, low = highs, high
            for m in range(12):
                modes[m, nx - 1, r, :] = held[m]
            low = [modes[m, GZ, r, :] for m in range(12)]
            lows, highs = element(
                low, [plane_up(a) for a in low], stiff[GZ, r, :],
                (GZ, r, slice(None)) if with_energy else None,
            )
            for m in range(12):
                modes[m, GZ, r, :] = lows[m] + plane_dn(highs[m])
            return carry

        lax.fori_loop(0, rows // TILE, step, 0, unroll=True)

    def each_node(emit, carry):
        ghosts = [half_back(*(modes[4 * c + m, GZ] for m in range(4))) for c in range(3)]
        taken = [pltpu.roll(g[1], 1, 1) for g in ghosts]
        for q in range(nx):
            got = []
            for c in range(3):
                near_w, far_w = half_back(*(modes[4 * c + m, q] for m in range(4)))
                got.append(near_w + z_dn(far_w, ghosts[c][1], q))
                taken[c] = z_dn_take(taken[c], far_w, q)
            carry = emit(q, got, carry)
        emit(GZ, [ghosts[c][0] + taken[c] for c in range(3)], carry)
        return carry

    nd, ng = DISP_ITERS, DMG_ITERS
    gram, vector = {}, {}

    def load_start(c, q):
        return gz_wide[c] if q == GZ else load_wide(c, q)

    pass_one(load_start, merge, rows, True)
    element_pass(True)
    hist[nx - 1] = blank
    arrive(1)
    greet(hop_sem)
    for f in range(DEEP, fields):
        gz_rows[f - DEEP + 1] = line_rows(*ghost_tiles(f))
    gather_back(stiff, inv_emit)

    def start_emit(q, got, dot):
        inv = inverse[q]
        for c in range(3):
            r = load_rows(DEEP + c, q) - got[c]
            v = inv * r
            basis[c, q] = v
            if q < nx:
                resid[c, q] = r[0:TILE]
                dot = dot + v[0:TILE] * r[0:TILE]
        return dot

    vector[0] = each_node(start_emit, zero)

    def hist_emit(q, total):
        react[q] = jnp.maximum(jnp.abs(load_rows(7, q)), 0.125 * total)

    gather_back(hist, hist_emit)

    for k in range(nd - 1):
        pass_one(lambda c, q, k=k: basis[3 * k + c, q], same, rows, True)
        element_pass(False)

        def apply_emit(q, got, carry, k=k):
            carry = list(carry)
            inv = inverse[q] * (2.0 / SPECTRUM)
            for c in range(3):
                w = got[c]
                here = basis[3 * k + c, q]
                v = inv * w - here
                if k:
                    v = 2.0 * v - basis[3 * (k - 1) + c, q]
                basis[3 * (k + 1) + c, q] = v
                if q < nx:
                    wi, vi = w[0:TILE], v[0:TILE]
                    if k + 2 < nd:
                        images[3 * k + c, q] = wi
                    carry[0] = carry[0] + here[0:TILE] * wi
                    carry[1] = carry[1] + vi * resid[c, q]
                    carry[2] = carry[2] + vi * wi
                    for j in range(k):
                        carry[3 + j] = carry[3 + j] + vi * images[3 * j + c, q]
            return tuple(carry)

        got = each_node(apply_emit, (zero,) * (3 + k))
        gram[k, k], vector[k + 1], gram[k + 1, k] = got[:3]
        for j in range(k):
            gram[k + 1, j] = got[3 + j]

    across = pl.ds((1 - gx) * lx, lx)
    x_basis = xcopy(basis.at[:, across, 0:TILE], basis_part, 2)
    x_basis.start()

    def last_energy():
        pass_one(lambda c, q: basis[3 * (nd - 1) + c, q], same, TILE, False)
        total = zero
        for r in (slice(0, TILE),):
            low = [modes[m, 0, r, :] for m in range(12)]
            for p in range(nx - 1):
                high = [modes[m, p + 1, r, :] for m in range(12)]
                S = [low[m] + high[m] if m % 4 else None for m in range(12)]
                D = [high[m] - low[m] for m in range(12)]
                xX, xXY, xXZ, xXYZ = D[0:4]
                yX, yXY, yXZ, yXYZ = D[4:8]
                zX, zXY, zXZ, zXYZ = D[8:12]
                _, xY, xZ, xYZ = S[0:4]
                _, yY, yZ, yYZ = S[4:8]
                _, zY, zZ, zYZ = S[8:12]
                div = xX + yY + zZ
                sxy, sxz, syz = xY + yX, xZ + zX, yZ + zY
                tw = xYZ + yXZ + zXY
                sum_two = xX * xX + yY * yY + zZ * zZ
                sum_shear = sxy * sxy + sxz * sxz + syz * syz
                sum_twist = xYZ * xYZ + yXZ * yXZ + zXY * zXY + tw * tw
                sum_bend = (yYZ * yYZ + xXZ * xXZ) + (zYZ * zYZ + xXY * xXY) + (yXY * yXY + zXZ * zXZ)
                sum_cross = yYZ * xXZ + zYZ * xXY + yXY * zXZ
                sum_last = xXYZ * xXYZ + yXYZ * yXYZ + zXYZ * zXYZ
                energy = (
                    (k_lame * (div * div) + k_two * sum_two)
                    + (k_shear * sum_shear + k_twist * sum_twist)
                    + (k_bend * sum_bend + (2.0 * k_cross) * sum_cross)
                    + k_last * sum_last
                ) * stiff[p, r, :]
                total = total + energy
                low = high
        return total

    gram[nd - 1, nd - 1] = last_energy()

    cy = yvalid + element_at(ypos - 1, ngy * ly)
    cz = element_at(zpos, ngz * lz) + element_at(zpos - 1, ngz * lz)
    czg = element_at(zghost, ngz * lz) + element_at(zghost - 1, ngz * lz)
    cxg = jnp.where((lane < 16) | (lane >= 16 * (nx - 1)), 1.0, 2.0)
    node = jnp.where(cy * cz > 0.0, 1.0, 0.0)
    gnode = jnp.where(cy * czg > 0.0, 1.0, 0.0)
    diag_scale = laplace_diag * TOUGHNESS * LENGTH_SCALE
    lap_scale = TOUGHNESS * LENGTH_SCALE / 36.0

    def lines(d, after, before, count_z):
        s, n = after + before, count_z * d
        mass, slope = 2.0 * n + s, n - s
        s, n = y_up(mass) + y_dn(mass), cy * mass
        both = 2.0 * n + s
        mixed = (n - s) + (2.0 * (cy * slope) + (y_up(slope) + y_dn(slope)))
        return 2.0 * mixed + both, mixed - both

    def laplace_pass(load, emit, carry, with_ghost):
        ghost = load(GZ)
        after = pltpu.roll(ghost, 127, 1)
        before = pltpu.roll(ghost, 1, 1)
        ahead = []
        for q in range(nx):
            d = load(q)
            ahead.append(lines(d, z_up(d, ghost, q), z_dn(d, ghost, q), cz))
            if with_ghost:
                after = z_up_take(after, d, q)
                before = z_dn_take(before, d, q)
            p = q - 1
            if p >= 0:
                total = ahead[p][0] if p == 0 else 2.0 * ahead[p][0] + ahead[p - 1][1]
                carry = emit(p, lap_scale * (total + ahead[q][1]), carry)
        carry = emit(nx - 1, lap_scale * (ahead[nx - 1][0] + ahead[nx - 2][1]), carry)
        if with_ghost:
            inner, outer = lines(ghost, after, before, czg)
            total = cxg * inner + jnp.where(lane >= 16, plane_dn(outer), 0.0)
            total = total + jnp.where(lane < 16 * (nx - 1), plane_up(outer), 0.0)
            emit(GZ, lap_scale * total, carry)
        return carry

    def reaction_of(q):
        return TOUGHNESS / LENGTH_SCALE + 2.0 * react[q]

    def old_damage(q):
        return load_rows(3, q)

    def dstart(q, lap, dot):
        reaction = reaction_of(q)
        if q == GZ:
            count, mask = cxg * cy * czg, gnode
        else:
            count, mask = (cy * cz if q in (0, nx - 1) else 2.0 * cy * cz), node
        inv = mask / (diag_scale * count + reaction)
        dinverse[q] = inv
        r = 2.0 * react[q] - (lap + reaction * old_damage(q))
        v = inv * r
        dbasis[0, q] = v
        if q < nx:
            dresid[q] = r[0:TILE]
            dot = dot + v[0:TILE] * r[0:TILE]
        return dot

    dvector, dgram = {}, {}
    dvector[0] = laplace_pass(old_damage, dstart, zero, True)
    for k in range(ng):
        more = k + 1 < ng

        def dstep(q, lap, carry, k=k, more=more):
            carry = list(carry)
            here = dbasis[k, q]
            w = lap + reaction_of(q) * here
            if q < nx:
                carry[0] = carry[0] + here[0:TILE] * w[0:TILE]
            if more:
                v = dinverse[q] * w - here
                if k:
                    v = 2.0 * v - dbasis[k - 1, q]
                dbasis[k + 1, q] = v
                if q < nx:
                    carry[1] = carry[1] + v[0:TILE] * dresid[q]
                    carry[2] = carry[2] + v[0:TILE] * w[0:TILE]
            return tuple(carry)

        got = laplace_pass(
            lambda q, k=k: dbasis[k, q], dstep, (zero,) * (3 if more else 1), more
        )
        dgram[k, k] = got[0]
        if more:
            dvector[k + 1], dgram[k + 1, k] = got[1:]

    parts = [vector[i] for i in range(nd)] + [dvector[i] for i in range(ng)]
    parts += [gram[i, j] for i in range(nd) for j in range(i + 1)]
    parts += [dgram[i, j] for i in range(ng) for j in range(i + 1)]
    at = lax.broadcasted_iota(jnp.int32, (1, 128), 1)
    packed = jnp.zeros((1, 128), f32)
    for i, piece in enumerate(parts):
        line = jnp.sum(piece, axis=0, keepdims=True)
        packed = jnp.where(at == i, jnp.sum(line, axis=1, keepdims=True), packed)
    slot_mine = gx * npeer + me
    sums[slot_mine] = packed
    pl.semaphore_wait(hop_sem, number_near)

    def peer(dy, dz):
        return lax.rem(gy + dy, ngy), lax.rem(gz + dz, ngz)

    def peer_copy(side, dy, dz, slot):
        return remote(
            sums.at[slot_mine], sums.at[slot], asend_sem.at[0], arecv_sem.at[0],
            (gx if side == 0 else 1 - gx, *peer(dy, dz)),
        )

    offsets = sorted(
        [(dy, dz) for dy in range(ngy) for dz in range(ngz)],
        key=lambda o: -(2 * (o[1] % 2) + (o[1] > 0) + o[0] % 2 + (o[0] > 0)),
    )
    peers = [(side, dy, dz) for dy, dz in offsets for side in (0, 1) if side or dy or dz]
    sends = [peer_copy(side, dy, dz, slot_mine) for side, dy, dz in peers]
    for s in sends:
        s.start()
    x_damage = xcopy(dbasis.at[:, across, 0:TILE], dbasis_part, 3)
    x_damage.start()
    x_react = xcopy(react.at[across, 0:TILE], react_part, 4)
    x_react.start()
    x_parts = [x_basis, x_damage, x_react]
    for passed in x_parts:
        passed.wait_recv()

    def both_tiles(near_tile, far_tile):
        return jnp.concatenate(order(near_tile, far_tile), axis=0)

    for p in range(lx):
        out_history[p] = both_tiles(react[gx * lx + p, 0:TILE], react_part[p])
    everyone = drain(sums.at[0 : 2 * npeer - 1], asend_sem.at[0], arecv_sem.at[0])
    everyone.wait_recv()
    layer = [sums[i] for i in range(2 * npeer)]
    while len(layer) > 1:
        layer = [a + b for a, b in zip(layer[::2], layer[1::2])] + layer[len(layer) & ~1 :]
    whole = layer[0]

    scalars = [
        jnp.sum(jnp.where(at == i, whole, 0.0), axis=1, keepdims=True) for i in range(len(parts))
    ]

    def solve(rhs, lower):
        n = len(rhs)
        A = [[lower[max(i, j)][min(i, j)] for j in range(n)] for i in range(n)]
        b = list(rhs)
        for i in range(n):
            pivot = 1.0 / A[i][i]
            for r in range(i + 1, n):
                ratio = A[r][i] * pivot
                for c in range(i + 1, n):
                    A[r][c] = A[r][c] - ratio * A[i][c]
                b[r] = b[r] - ratio * b[i]
        out = [None] * n
        for i in reversed(range(n)):
            s = b[i]
            for j in range(i + 1, n):
                s = s - A[i][j] * out[j]
            out[i] = s / A[i][i]
        return out

    def triangle(flat, n):
        return [[flat[k * (k + 1) // 2 + j] for j in range(k + 1)] for k in range(n)]

    rest = scalars[nd + ng :]
    cut = nd * (nd + 1) // 2
    weights = solve(scalars[:nd], triangle(rest[:cut], nd))
    dweights = solve(scalars[nd : nd + ng], triangle(rest[cut:], ng))
    for p in range(lx):
        at_x = gx * lx + p
        for c in range(3):
            near_x = far_x = zero
            for k in range(nd):
                near_x = near_x + weights[k] * basis[3 * k + c, at_x, 0:TILE]
                far_x = far_x + weights[k] * basis_part[3 * k + c, p]
            lower, upper = order(near_x, far_x)
            out_disp[c, p, 0:TILE] = full_deep[c, 0, at_x] + lower
            out_disp[c, p, TILE:ly] = full_deep[c, 1, at_x] + upper
        near_d = far_d = zero
        for k in range(ng):
            near_d = near_d + dweights[k] * dbasis[k, at_x, 0:TILE]
            far_d = far_d + dweights[k] * dbasis_part[k, p]
        lower, upper = order(near_d, far_d)
        out_damage[p, 0:TILE] = full_deep[3, 0, at_x] + lower
        out_damage[p, TILE:ly] = full_deep[3, 1, at_x] + upper

    for side, dz in ((0, -1), (1, 1)):
        pl.when(there(0, dz))(
            drain(full_deep.at[0, 0], zsend_sem.at[side], zrecv_sem.at[0]).wait_send
        )
        for dy in (-1, 1):
            pl.when(there(dy, dz))(
                drain(zsend_deep.at[side], csend_sem.at[2 * (dy > 0) + side], crecv_sem.at[0]).wait_send
            )
    for flat in range(2):
        for dy in (-1, 1):
            pl.when(there(dy, 0))(ycopy(0, dy, flat).wait_send)
    for passed in x_own + x_parts:
        passed.wait_send()
    everyone.wait_send()


def hand_on(*refs):
    sources, targets, sem = refs[:3], refs[3:6], refs[6]
    copies = [
        pltpu.make_async_copy(source, target, sem.at[i])
        for i, (source, target) in enumerate(zip(sources, targets))
    ]
    for copy in copies:
        copy.start()
    for copy in copies:
        copy.wait()


def body_fused(sizes, *arrays):
    ngy, ngz, lx, ly, lz = sizes
    nx, rows, wide, fields = 2 * lx, 2 * TILE, 3 * TILE, 8
    packs, pairs, extras = fields * lx // 16, DEEP * lx // 2, DEEP * lx // TILE
    npeer = ngy * ngz
    f32 = jnp.float32
    planes = (nx + 1, rows, lz)
    vmem = pl.BlockSpec(memory_space=pltpu.VMEM)
    hbm = pl.BlockSpec(memory_space=pltpu.HBM)
    dma = pltpu.SemaphoreType.DMA

    def room(*shape):
        return pltpu.VMEM(shape, f32)

    results = pl.pallas_call(
        functools.partial(kernel, sizes),
        out_shape=(
            pltpu.VMEM((3, lx, ly, lz), f32),
            pltpu.VMEM((lx, ly, lz), f32),
            pltpu.VMEM((lx, ly, lz), f32),
        ),
        in_specs=[hbm] * 6,
        out_specs=(vmem,) * 3,
        scratch_shapes=[
            room(3, lx, ly, lz),
            room(3, lx, ly, lz),
            room(lx, ly, lz),
            room(lx, ly, lz),
            pltpu.VMEM((lx, ly, lz), jnp.int32),
            pltpu.VMEM((lx, ly, lz), jnp.int32),
            room(DEEP, 2, nx, TILE, lz),
            room(DEEP, 2, nx, TILE, lz),
            room(pairs + extras, TILE, 128),
            room(pairs, TILE, 128),
            room(pairs, TILE, 128),
            room(pairs, TILE, 128),
            room(2, pairs + extras, TILE, 128),
            room(2, pairs, TILE, 128),
            room(2, 2, TILE, 128),
            room(2, 2, TILE, 128),
            room(2, 2, 3, TILE, 128),
            room(2, 2, 3, TILE, 128),
            room(4, wide, 128),
            room(5, rows, 128),
            room(12, *planes),
            room(3 * DISP_ITERS, *planes),
            room(3 * (DISP_ITERS - 2), nx, TILE, lz),
            room(3, nx, TILE, lz),
            room(*planes),
            room(*planes),
            room(*planes),
            room(*planes),
            room(*planes),
            room(DMG_ITERS, *planes),
            room(nx, TILE, lz),
            room(3 * DISP_ITERS, lx, TILE, lz),
            room(DMG_ITERS, lx, TILE, lz),
            room(lx, TILE, lz),
            room(2 * npeer, 1, 128),
            dma((6,)),
            dma((4,)),
            dma((2,)),
            dma((2,)),
            dma((4,)),
            dma((4,)),
            dma((4,)),
            dma((5,)),
            dma((5,)),
            dma((1,)),
            dma((1,)),
            pltpu.SemaphoreType.REGULAR,
        ],
        compiler_params=pltpu.CompilerParams(
            collective_id=0, has_side_effects=True, vmem_limit_bytes=VMEM_LIMIT
        ),
    )(*[pltpu.with_memory_space_constraint(a, pltpu.HBM) for a in arrays])
    return pl.pallas_call(
        hand_on,
        out_shape=tuple(jax.ShapeDtypeStruct(r.shape, f32) for r in results),
        in_specs=[vmem] * 3,
        out_specs=(hbm,) * 3,
        scratch_shapes=[dma((3,))],
        compiler_params=pltpu.CompilerParams(vmem_limit_bytes=1024 * 1024),
    )(*[pltpu.with_memory_space_constraint(r, pltpu.VMEM) for r in results])


VMEM_LIMIT = 24 * 1024 * 1024


def solution(mesh):
    shape = dict(mesh.shape)

    def body(*arrays):
        lx, ly, lz = arrays[2].shape
        fits = shape["gx"] == 2 and shape["gy"] * shape["gz"] > 1
        fits = fits and max(shape["gy"], shape["gz"]) <= 4
        fits = fits and lx == 4 and ly == 2 * TILE and lz == 128
        if fits:
            return body_fused((shape["gy"], shape["gz"], lx, ly, lz), *arrays)
        return body_any_mesh(*arrays)

    return jax.shard_map(
        body,
        mesh=mesh,
        in_specs=(
            P(None, "gx", "gy", "gz"),
            P(None, "gx", "gy", "gz"),
            P("gx", "gy", "gz"),
            P("gx", "gy", "gz"),
            P("gx", "gy", "gz"),
            P("gx", "gy", "gz"),
        ),
        out_specs=(P(None, "gx", "gy", "gz"), P("gx", "gy", "gz"), P("gx", "gy", "gz")),
        check_vma=False,
    )
```

```python
import functools
import jax
import jax.numpy as jnp
import numpy as np
from jax import lax
from jax.experimental import pallas as pl
from jax.experimental.pallas import tpu as pltpu
from jax.sharding import PartitionSpec as P

DISP_ITERS = 4
DMG_ITERS = 2


LAME_LAMBDA = 0.5769230769230769
LAME_MU = 0.38461538461538464
BULK_MODULUS = LAME_LAMBDA + 2.0 * LAME_MU / 3.0
RESIDUAL_STIFFNESS = 0.001
TOUGHNESS = 1.0
LENGTH_SCALE = 2.0
CRACK_HISTORY = 40.0


def padded_2(cells, sides, width):
    for axis, dim in sides:
        count = lax.axis_size(axis)
        ends = count - 1
        head = lax.slice_in_dim(cells, 0, width, axis=dim)
        tail = lax.slice_in_dim(cells, cells.shape[dim] - width, cells.shape[dim], axis=dim)
        cells = jnp.concatenate(
            [
                lax.ppermute(tail, axis, [(i, (i + 1) % count) for i in range(ends)]),
                cells,
                lax.ppermute(head, axis, [((i + 1) % count, i) for i in range(ends)]),
            ],
            axis=dim,
        )
    return cells


def corner_offsets(corner):
    return (corner >> 2 & 1, corner >> 1 & 1, corner & 1)


def shape_gradients(sample):
    gradient = np.zeros((3, 8))
    for corner in range(8):
        offsets = corner_offsets(corner)
        values = [sample[k] if offsets[k] else 1.0 - sample[k] for k in range(3)]
        slopes = [1.0 if offsets[k] else -1.0 for k in range(3)]
        gradient[0, corner] = slopes[0] * values[1] * values[2]
        gradient[1, corner] = values[0] * slopes[1] * values[2]
        gradient[2, corner] = values[0] * values[1] * slopes[2]
    return gradient


def strain_matrix(gradient):
    strain = np.zeros((6, 24))
    for corner in range(8):
        column = 3 * corner
        strain[0, column] = gradient[0, corner]
        strain[1, column + 1] = gradient[1, corner]
        strain[2, column + 2] = gradient[2, corner]
        strain[3, column] = gradient[1, corner]
        strain[3, column + 1] = gradient[0, corner]
        strain[4, column + 1] = gradient[2, corner]
        strain[4, column + 2] = gradient[1, corner]
        strain[5, column] = gradient[2, corner]
        strain[5, column + 2] = gradient[0, corner]
    return strain


def element_tables():
    moduli = np.zeros((6, 6))
    moduli[:3, :3] = LAME_LAMBDA
    for k in range(3):
        moduli[k, k] += 2.0 * LAME_MU
        moduli[k + 3, k + 3] = LAME_MU
    points = [0.5 - 0.5 / np.sqrt(3.0), 0.5 + 0.5 / np.sqrt(3.0)]
    stiff_table = np.zeros((24, 24))
    laplace_table = np.zeros((8, 8))
    for sample_index in range(8):
        sample = tuple((points[k] for k in corner_offsets(sample_index)))
        gradient = shape_gradients(sample)
        strain = strain_matrix(gradient)
        stiff_table += 0.125 * strain.T @ moduli @ strain
        laplace_table += 0.125 * gradient.T @ gradient
    centre_table = strain_matrix(shape_gradients((0.5, 0.5, 0.5)))
    return (
        stiff_table.astype(np.float32),
        laplace_table.astype(np.float32),
        centre_table.astype(np.float32),
    )


def corner_views(padded, element_shape):
    corner_list = []
    for corner in range(8):
        offx, offy, offz = corner_offsets(corner)
        corner_list.append(
            padded[
                ...,
                offx : offx + element_shape[0],
                offy : offy + element_shape[1],
                offz : offz + element_shape[2],
            ]
        )
    return corner_list


def assemble_nodes(pieces):
    running = None
    for corner in range(8):
        offx, offy, offz = corner_offsets(corner)
        leading = [(0, 0)] * (pieces[corner].ndim - 3)
        placed = jnp.pad(
            pieces[corner], leading + [(offx, 1 - offx), (offy, 1 - offy), (offz, 1 - offz)]
        )
        running = placed if running is None else running + placed
    return running


def line_valid(position, devices, count):
    index = position * count + jnp.arange(count + 1, dtype=jnp.int32) - 1
    return ((index >= 0) & (index <= devices * count - 2)).astype(jnp.float32)


def strain_energy(strain):
    trace = strain[0] + strain[1] + strain[2]
    deviator = strain[:3] - trace[None] / 3.0
    shear = strain[3:]
    tensile = jnp.maximum(trace, 0.0)
    return 0.5 * BULK_MODULUS * tensile * tensile + LAME_MU * (
        jnp.sum(deviator * deviator, axis=0) + 0.5 * jnp.sum(shear * shear, axis=0)
    )


def forces_to_nodes(forces, stiffness):
    pieces = [stiffness[None] * forces[3 * target : 3 * target + 3] for target in range(8)]
    return assemble_nodes(pieces)


def element_apply(padded, stiffness, stiff_table):
    element_shape = stiffness.shape
    flat = jnp.stack(corner_views(padded, element_shape)).reshape(24, -1)
    forces = jnp.dot(stiff_table, flat, precision=lax.Precision.HIGHEST).reshape(
        (24,) + element_shape
    )
    return forces_to_nodes(forces, stiffness)


def laplace_apply(padded, element_valid, laplace_table):
    element_shape = element_valid.shape
    flat = jnp.stack(corner_views(padded, element_shape)).reshape(8, -1)
    forces = jnp.dot(laplace_table, flat, precision=lax.Precision.HIGHEST).reshape(
        (8,) + element_shape
    )
    return assemble_nodes([element_valid * forces[target] for target in range(8)])


def single_pair(pair):
    return tuple(lax.psum(pair, ("gx", "gy", "gz")))


def conjugate(solutions, residuals, inverses, counts, apply_fn):
    solutions = list(solutions)
    residuals = list(residuals)
    number = len(solutions)
    steps = max(counts)

    def pair_totals(pairs):
        return [single_pair(pairs[0])]

    precs = [inverses[0] * residuals[0]]
    applied = apply_fn(precs, list(range(number)))
    pairs = pair_totals([(jnp.sum(residuals[0] * precs[0]), jnp.sum(precs[0] * applied[0]))])
    norms = [pair[0] for pair in pairs]
    lengths = [pair[0] / pair[1] for pair in pairs]
    directions = list(precs)
    alongs = list(applied)
    for step in range(steps):
        active = [i for i in range(number) if step < counts[i]]
        for i in active:
            solutions[i] = solutions[i] + lengths[i] * directions[i]
            residuals[i] = residuals[i] - lengths[i] * alongs[i]
        later = [i for i in active if step + 1 < counts[i]]
        if later:
            i = later[0]
            precs[i] = inverses[i] * residuals[i]
            images = apply_fn([precs[i] for i in later], later)
            pairs = pair_totals(
                [
                    (jnp.sum(residuals[i] * precs[i]), jnp.sum(precs[i] * images[k]))
                    for k, i in enumerate(later)
                ]
            )
            for k, i in enumerate(later):
                norm_next, curve_sum = pairs[k]
                ratio = norm_next / norms[i]
                lengths[i] = norm_next / (curve_sum - ratio * norm_next / lengths[i])
                directions[i] = precs[i] + ratio * directions[i]
                alongs[i] = images[k] + ratio * alongs[i]
                norms[i] = norm_next
    return solutions


def body_any_mesh(displacement_start, external_force, damage_old, history_old, crack_labels, fixed_flags):
    tables = element_tables()
    stiff_table = jnp.asarray(tables[0], jnp.float32)
    laplace_table = jnp.asarray(tables[1], jnp.float32)
    centre_table = jnp.asarray(tables[2], jnp.float32)
    highest = lax.Precision.HIGHEST
    size_x, size_y, size_z = damage_old.shape
    free_mask = 1.0 - fixed_flags.astype(jnp.float32)
    start_disp = displacement_start * free_mask[None]
    element_valid = (
        line_valid(lax.axis_index("gx"), lax.axis_size("gx"), size_x)[:, None, None]
        * line_valid(lax.axis_index("gy"), lax.axis_size("gy"), size_y)[None, :, None]
        * line_valid(lax.axis_index("gz"), lax.axis_size("gz"), size_z)[None, None, :]
    )
    element_shape = element_valid.shape
    start_pad = padded_2(
        jnp.concatenate([start_disp, damage_old[None]], axis=0),
        (("gx", 1), ("gy", 2), ("gz", 3)),
        1,
    )
    corner_list = corner_views(start_pad, element_shape)
    damage_mean = sum((view[3] for view in corner_list)) / 8.0
    stiffness = ((1.0 - damage_mean) ** 2 + RESIDUAL_STIFFNESS) * element_valid
    flat = jnp.stack([view[:3] for view in corner_list]).reshape(24, -1)
    combined = jnp.dot(
        jnp.concatenate([stiff_table, centre_table], axis=0), flat, precision=highest
    )
    forces = combined[:24].reshape((24,) + element_shape)
    strain = combined[24:].reshape((6,) + element_shape)
    start_image = forces_to_nodes(forces, stiffness)[:, 1:-1, 1:-1, 1:-1]
    energy = strain_energy(strain) * element_valid
    nodal_energy = assemble_nodes([energy] * 8)[1:-1, 1:-1, 1:-1] / 8.0
    history = jnp.maximum(
        jnp.maximum(history_old, nodal_energy), CRACK_HISTORY * crack_labels.astype(jnp.float32)
    )
    stiff_diag = jnp.diagonal(stiff_table)
    diag_pieces = [
        stiffness[None] * stiff_diag[3 * target : 3 * target + 3][:, None, None, None]
        for target in range(8)
    ]
    elastic_diag = assemble_nodes(diag_pieces)[:, 1:-1, 1:-1, 1:-1]
    inverse_elastic = 1.0 / (free_mask[None] * elastic_diag + (1.0 - free_mask[None]))

    def constrained(nodal_field):
        masked = free_mask[None] * nodal_field
        padded = padded_2(masked, (("gx", 1), ("gy", 2), ("gz", 3)), 1)
        nodes = element_apply(padded, stiffness, stiff_table)[:, 1:-1, 1:-1, 1:-1]
        return free_mask[None] * nodes + (1.0 - free_mask[None]) * nodal_field

    reaction = TOUGHNESS / LENGTH_SCALE + 2.0 * history
    laplace_diag = assemble_nodes(
        [element_valid * laplace_table[target, target] for target in range(8)]
    )[1:-1, 1:-1, 1:-1]
    inverse_damage = 1.0 / (TOUGHNESS * LENGTH_SCALE * laplace_diag + reaction)
    residual = free_mask[None] * (external_force - start_image)
    start_lap = laplace_apply(start_pad[3], element_valid, laplace_table)[1:-1, 1:-1, 1:-1]
    damage_residual = 2.0 * history - (TOUGHNESS * LENGTH_SCALE * start_lap + reaction * damage_old)

    def damage_operator(nodal_field):
        padded = padded_2(nodal_field, (("gx", 0), ("gy", 1), ("gz", 2)), 1)
        lap_nodes = laplace_apply(padded, element_valid, laplace_table)[1:-1, 1:-1, 1:-1]
        return TOUGHNESS * LENGTH_SCALE * lap_nodes + reaction * nodal_field

    def single_elastic(fields, active):
        return [constrained(fields[0])]

    def single_damage(fields, active):
        return [damage_operator(fields[0])]

    displacement = conjugate(
        [start_disp], [residual], [inverse_elastic], [DISP_ITERS], single_elastic
    )[0]
    damage = conjugate(
        [damage_old], [damage_residual], [inverse_damage], [DMG_ITERS], single_damage
    )[0]
    return (displacement, damage, history)


SPECTRUM = 3.2
TILE = 8
GHOST = 4
DEEP = 4
MESH = pl.DeviceIdType.MESH


def walsh_tables():
    stiff, laplace, _ = element_tables()
    signs = np.array(
        [
            [np.prod([1.0 if c >> k & 1 else (-1.0 if m >> k & 1 else 1.0) for k in range(3)]) for c in range(8)]
            for m in range(8)
        ]
    )
    wide = np.kron(signs, np.eye(3))
    stiff_modes = wide @ stiff.astype(np.float64) @ wide.T / 64.0
    return stiff_modes, float(stiff[0, 0]), float(laplace[0, 0])


def kernel(
    sizes,
    disp_in,
    force_in,
    damage_in,
    history_in,
    labels_in,
    flags_in,
    out_disp,
    out_damage,
    out_history,
    disp_ref,
    force_ref,
    damage_ref,
    history_ref,
    labels_ref,
    flags_ref,
    full_deep,
    full_flat,
    down_deep,
    up_deep,
    down_flat,
    up_flat,
    ghost_deep,
    ghost_flat,
    zsend_deep,
    zsend_flat,
    zbuf_deep,
    zbuf_flat,
    gz_wide,
    gz_rows,
    modes,
    basis,
    images,
    resid,
    stiff,
    inverse,
    hist,
    react,
    dinverse,
    dbasis,
    dresid,
    basis_part,
    dbasis_part,
    react_part,
    sums,
    in_sem,
    ysend_sem,
    yrecv_sem,
    zsend_sem,
    zrecv_sem,
    csend_sem,
    crecv_sem,
    xsend_sem,
    xrecv_sem,
    asend_sem,
    arecv_sem,
    hop_sem,
):
    ngy, ngz, lx, ly, lz = sizes
    nx = 2 * lx
    fields = 8
    npeer = ngy * ngz
    pairs = DEEP * lx // 2
    packs = fields * lx // 16
    extras = DEEP * lx // TILE
    wide, rows = 3 * TILE, 2 * TILE
    GZ = nx
    f32 = jnp.float32
    stiff_modes, stiff_diag, laplace_diag = walsh_tables()
    gx, gy, gz = lax.axis_index("gx"), lax.axis_index("gy"), lax.axis_index("gz")
    me = gy * ngz + gz
    partner = (1 - gx, gy, gz)
    outward = 2 * gx - 1
    full, zsend, zbuf = (full_deep, full_flat), (zsend_deep, zsend_flat), (zbuf_deep, zbuf_flat)

    def there(dy, dz):
        y, z = gy + dy, gz + dz
        return (y >= 0) & (y < ngy) & (z >= 0) & (z < ngz)

    def device(core, dy, dz):
        return core, lax.rem(gy + dy + ngy, ngy), lax.rem(gz + dz + ngz, ngz)

    near = [(dy, dz) for dy in (-1, 0, 1) for dz in (-1, 0, 1) if dy or dz]
    number_near = 2 * sum(there(dy, dz).astype(jnp.int32) for dy, dz in near)

    barrier = pltpu.get_barrier_semaphore()

    def greet(semaphore):
        for dy, dz in near:

            @pl.when(there(dy, dz))
            def _():
                for core in (gx, 1 - gx):
                    pl.semaphore_signal(
                        semaphore, inc=1, device_id=device(core, dy, dz), device_id_type=MESH
                    )

    loads = [
        pltpu.make_async_copy(source, target, in_sem.at[i])
        for source, target, i in (
            (flags_in, flags_ref, 1),
            (disp_in, disp_ref, 0),
            (damage_in, damage_ref, 1),
            (force_in, force_ref, 0),
            (history_in, history_ref, 1),
            (labels_in, labels_ref, 1),
        )
    ]
    for load in loads:
        load.start()
    greet(barrier)
    pl.semaphore_signal(barrier, inc=1, device_id=partner, device_id_type=MESH)

    zero = jnp.zeros((TILE, 128), f32)
    for dz, side in ((1, 0), (-1, 1)):

        @pl.when(jnp.logical_not(there(0, dz)))
        def _():
            for core in range(2):
                for ref in zbuf:
                    ref[core, side, 0:2] = jnp.zeros((2, TILE, 128), f32)

        @pl.when(jnp.logical_not(there(outward, dz)))
        def _():
            for core in range(2):
                for ref in zbuf:
                    ref[core, side, 2] = zero

    @pl.when(jnp.logical_not(there(outward, 0)))
    def _():
        ghost_deep[...] = jnp.zeros(ghost_deep.shape, f32)
        ghost_flat[...] = jnp.zeros(ghost_flat.shape, f32)

    for i, room in enumerate((basis_part, full_deep.at[0:2])):
        pltpu.make_async_copy(room, room, in_sem.at[i]).wait()

    values = []
    for p in range(lx):
        flag = flags_ref[p].astype(f32)
        free = 1.0 - flag
        top = jnp.maximum(history_ref[p], CRACK_HISTORY * labels_ref[p].astype(f32))
        here = [free * disp_ref[c, p] for c in range(3)]
        here += [damage_ref[p]] + [force_ref[c, p] for c in range(3)] + [top * (free - flag)]
        for f in range(fields):
            for half in range(2):
                full[f // DEEP][f % DEEP, half, gx * lx + p] = here[f][TILE * half : TILE * half + TILE]
        values.append(here)

    sub = lax.broadcasted_iota(jnp.int32, (TILE, 128), 0)

    def spin(a, shift, axis):
        shift = shift % a.shape[axis]
        return pltpu.roll(a, shift, axis) if shift else a

    def spot(f, q):
        return 8 * (f % 4 // 2) + 2 * q + f % 2

    group = lax.broadcasted_iota(jnp.int32, (ly, 128), 1) // 8
    for j in range(packs):
        low = jnp.zeros((ly, 128), f32)
        high = jnp.zeros((ly, 128), f32)
        for f in range(4 * j, 4 * j + 4):
            for q in range(lx):
                k = spot(f, q)
                turned = spin(values[q][f], 8 * k + 8, 1)
                low = jnp.where(group == (k + 1) % 16, turned, low)
                high = jnp.where(group == k, turned, high)
        for half in range(2):
            zsend[j][0, half] = low[TILE * half : TILE * half + TILE]
            zsend[j][1, half] = high[TILE * half : TILE * half + TILE]
    for first, skip, down, up in ((0, extras, down_deep, up_deep), (DEEP, 0, down_flat, up_flat)):
        for j in range(pairs):
            fa, qa = divmod(2 * j, lx)
            fb, qb = divmod(2 * j + 1, lx)
            a, b = values[qa][first + fa], values[qb][first + fb]
            down[skip + j] = jnp.where(sub < GHOST, a[0:TILE], spin(b[0:TILE], GHOST, 0))
            up[skip + j] = jnp.where(sub < GHOST, spin(b[ly - TILE : ly], GHOST, 0), a[ly - TILE : ly])
    for e in range(extras):
        tile = jnp.zeros((TILE, 128), f32)
        for s in range(TILE):
            f, q = divmod(TILE * e + s, lx)
            tile = jnp.where(sub == s, spin(values[q][f][0:TILE], s - GHOST, 0), tile)
        down_deep[e] = tile

    pl.semaphore_wait(barrier, number_near + 1)

    def remote(src, dst, send, recv, target):
        return pltpu.make_async_remote_copy(
            src_ref=src, dst_ref=dst, send_sem=send, recv_sem=recv,
            device_id=target, device_id_type=MESH,
        )

    def xcopy(src, dst, k):
        return remote(src, dst, xsend_sem.at[k], xrecv_sem.at[k], partner)

    def zcopy(source, dz, pack, core):
        side = 0 if dz < 0 else 1
        return remote(
            zsend[pack].at[side], zbuf[pack].at[source, side, 0:2],
            zsend_sem.at[side], zrecv_sem.at[2 * side + pack],
            device(core, 0, dz),
        )

    def corner(source, dy, dz, pack):
        side = 0 if dz < 0 else 1
        return remote(
            zsend[pack].at[side, int(dy > 0)], zbuf[pack].at[source, side, 2],
            csend_sem.at[2 * (dy > 0) + side],
            crecv_sem.at[2 * side + pack],
            device(int(dy < 0), dy, dz),
        )

    last = extras + 3 * lx // 2
    tiles_of = {0: slice(extras, last), 2: slice(last, extras + pairs)}

    def ycopy(source, dy, kind):
        if kind == 1:
            src, dst = (down_flat if dy < 0 else up_flat), ghost_flat.at[source]
        else:
            tiles = slice(0, last) if dy < 0 and kind == 0 else tiles_of[kind]
            src = (down_deep if dy < 0 else up_deep).at[tiles]
            dst = ghost_deep.at[source, tiles]
        return remote(
            src, dst, ysend_sem.at[2 * kind + (dy > 0)], yrecv_sem.at[kind],
            device(int(dy < 0), dy, 0),
        )

    own = pl.ds(gx * lx, lx)
    x_own = [
        xcopy(full[flat].at[:, :, own], full[flat].at[:, :, own], flat) for flat in range(2)
    ]
    halos = [[], []]
    for flat in (0, 1):
        for source in (0, 1):
            ways = []
            for dy in (1, -1):
                ways += [((dy, dz), corner(source, dy, dz, flat)) for dz in (-1, 1)]
                ways += [((dy, 0), ycopy(source, dy, kind)) for kind in ((1,) if flat else (0, 2))]
            ways += [((0, dz), zcopy(source, dz, flat, core)) for dz in (-1, 1) for core in (0, 1)]
            halos[flat] += [((gx == source) & there(*way), copy) for way, copy in ways]
    for flat in (0, 1):
        x_own[flat].start()
        for guard, copy in halos[flat]:
            pl.when(guard)(copy.start)

    def drain(ref, send, recv):
        return remote(ref, ref, send, recv, partner)

    def arrive(flat):
        for side, dz in ((0, -1), (1, 1)):
            faces = zbuf[flat].at[:, side, 0:2]
            pl.when(there(0, -dz))(
                drain(faces, zsend_sem.at[side], zrecv_sem.at[2 * side + flat]).wait_recv
            )
        x_own[flat].wait_recv()
        for side, dz in ((0, -1), (1, 1)):
            edges = zbuf[flat].at[:, side, 2]
            pl.when(there(outward, -dz))(
                drain(edges, csend_sem.at[side], crecv_sem.at[2 * side + flat]).wait_recv
            )
        rows_in = [ghost_flat] * 2 if flat else [ghost_deep.at[:, tiles_of[0]], ghost_deep.at[:, 0:last]]
        for core in range(2):
            pl.when((gx == core) & there(outward, 0))(
                drain(rows_in[core], ysend_sem.at[flat], yrecv_sem.at[flat]).wait_recv
            )

    arrive(0)

    lane_w = lax.broadcasted_iota(jnp.int32, (wide, 128), 1)
    odd = lane_w // 8 % 2

    def merge(a):
        return jnp.concatenate(
            [a[0:TILE], jnp.where(sub < GHOST, a[TILE : 2 * TILE], a[2 * TILE :])], axis=0
        )

    is_lower = sub + TILE * gx < TILE
    from_theirs = (sub + GHOST * gx) % TILE < GHOST

    def order(lower, upper):
        return jnp.where(is_lower, lower, upper), jnp.where(is_lower, upper, lower)

    def ghost_tiles(f):
        halves = []
        for source in range(2):
            ref = zbuf[f // 4]
            low, high = (
                jnp.concatenate([ref[source, side, k] for k in range(3)], axis=0) for side in range(2)
            )
            both = jnp.where(odd == f % 2, high, low)
            halves.append(spin(both, 8 * (2 * lx * source - spot(f, 0)), 1))
        whole = jnp.where(lane_w < 16 * lx, *halves)
        return *order(whole[0:TILE], whole[TILE : 2 * TILE]), whole[2 * TILE :]

    def line_wide(tile, other, up, down):
        return jnp.concatenate(
            [tile, jnp.where(is_lower, other, up), jnp.where(is_lower, down, other)], axis=0
        )

    def line_rows(tile, other, ghost):
        return jnp.concatenate([tile, jnp.where(from_theirs, other, ghost)], axis=0)

    for f in range(DEEP):
        tile, other, ghost = ghost_tiles(f)
        gz_wide[f] = line_wide(tile, other, ghost, ghost)
    gz_rows[0] = merge(gz_wide[DEEP - 1])

    def pieces(f, q):
        source, p = divmod(q, lx)
        j, half = divmod(f % DEEP * lx + p, 2)
        ghost = ghost_deep[source, extras + j] if f < DEEP else ghost_flat[source, j]
        ref = full[f // DEEP]
        return *order(ref[f % DEEP, 0, q], ref[f % DEEP, 1, q]), spin(ghost, GHOST * half, 0)

    def load_wide(f, q):
        tile, other, ghost = pieces(f, q)
        e, s = divmod(f * lx + q % lx, TILE)
        extra = spin(ghost_deep[q // lx, e], GHOST - s, 0)
        return line_wide(tile, other, jnp.where(sub == GHOST, extra, ghost), ghost)

    def load_rows(f, q):
        if q == GZ:
            return gz_rows[f - DEEP + 1]
        return line_rows(*pieces(f, q))

    row = lax.broadcasted_iota(jnp.int32, (rows, 128), 0)
    lane = lax.broadcasted_iota(jnp.int32, (rows, 128), 1)
    inside = lane % 16
    ypos = gy * ly + gx * TILE + jnp.where(row < TILE + GHOST, row, row - rows)
    zpos = gz * lz + lane
    zghost = gz * lz + jnp.where(inside < 8, inside - 8, inside + (lz - 8))

    def element_at(pos, count):
        return jnp.where((pos >= 0) & (pos <= count - 2), 1.0, 0.0)

    yvalid = element_at(ypos, ngy * ly)
    valid = yvalid * element_at(zpos, ngz * lz)
    gvalid = jnp.where(lane < 16 * (nx - 1), yvalid * element_at(zghost, ngz * lz), 0.0)

    def y_up(a):
        return pltpu.roll(a, a.shape[0] - 1, 0)

    def y_dn(a):
        return pltpu.roll(a, 1, 0)

    def lanes(a):
        return lane_w if a.shape[0] == wide else lane

    def z_up(a, ghost, p):
        return jnp.where(lanes(a) == 127, spin(ghost, 119 - 16 * p, 1), pltpu.roll(a, 127, 1))

    def z_up_take(acc, a, p):
        return jnp.where(lanes(a) == 16 * p + 7, spin(a, 16 * p + 7, 1), acc)

    def z_dn(a, ghost, p):
        return jnp.where(lanes(a) == 0, spin(ghost, 121 - 16 * p, 1), pltpu.roll(a, 1, 1))

    def z_dn_take(acc, a, p):
        return jnp.where(lanes(a) == 16 * p + 8, spin(a, 16 * p + 9, 1), acc)

    def plane_up(a):
        return pltpu.roll(a, 112, 1)

    def plane_dn(a):
        return pltpu.roll(a, 16, 1)

    blank = jnp.zeros((rows, 128), f32)

    def half_back(ss, yd, zd, yz):
        s = (ss - yd) + y_dn(ss + yd)
        d = (zd - yz) + y_dn(zd + yz)
        return s - d, s + d

    def damage_sum(q):
        a = load_wide(3, q)
        s = a + z_up(a, gz_wide[3], q)
        return merge(s + y_up(s)), a

    def rigidity(low, high, mask):
        rest = 1.0 - (low + high) * 0.125
        return (rest * rest + RESIDUAL_STIFFNESS) * mask


    def gather_back(ref, emit):
        ghost = ref[GZ]
        below = blank
        taken = pltpu.roll(ghost, 1, 1)
        for q in range(nx):
            a = ref[q]
            s = a + z_dn(a, ghost, q)
            here = s + y_dn(s)
            emit(q, below + here)
            below = here
            taken = z_dn_take(taken, a, q)
        s = ghost + taken
        s = s + y_dn(s)
        emit(GZ, s + plane_dn(s))

    def inv_emit(q, total):
        free = load_rows(7, q) > 0.0
        inverse[q] = jnp.where(free, 1.0 / jnp.where(free, stiff_diag * total, 1.0), 0.0)

    def forward(u, near_u, keep):
        zs, zd = u + near_u, near_u - u
        a, b = keep(y_up(zs)), keep(y_up(zd))
        zs, zd = keep(zs), keep(zd)
        return zs + a, a - zs, zd + b, b - zd

    def same(a):
        return a

    def pass_one(load, keep, height, with_ghost):
        for c in range(3):
            ghost = load(c, GZ)
            taken = pltpu.roll(ghost, 127, 1)
            for q in range(nx):
                u = load(c, q)
                out = forward(u, z_up(u, ghost, q), keep)
                for m in range(4):
                    modes[4 * c + m, q, 0:height] = out[m][0:height]
                if with_ghost:
                    taken = z_up_take(taken, u, q)
            if with_ghost:
                out = forward(ghost, taken, keep)
                for m in range(4):
                    modes[4 * c + m, GZ] = out[m]

    def sm(mode_a, comp_a, mode_b, comp_b):
        return float(stiff_modes[3 * mode_a + comp_a, 3 * mode_b + comp_b])

    k_lame = sm(4, 0, 2, 1)
    k_two = sm(4, 0, 4, 0) - k_lame
    k_shear = sm(2, 0, 2, 0)
    k_twist = sm(3, 0, 5, 1)
    k_bend = sm(3, 1, 3, 1)
    k_cross = sm(3, 1, 5, 0)
    k_last = sm(7, 0, 7, 0)

    def element(low, high, g, energy_at):
        S = [low[m] + high[m] if m % 4 else None for m in range(12)]
        D = [high[m] - low[m] for m in range(12)]
        xX, xXY, xXZ, xXYZ = D[0:4]
        yX, yXY, yXZ, yXYZ = D[4:8]
        zX, zXY, zXZ, zXYZ = D[8:12]
        _, xY, xZ, xYZ = S[0:4]
        _, yY, yZ, yYZ = S[4:8]
        _, zY, zZ, zYZ = S[8:12]
        div = xX + yY + zZ
        sxy, sxz, syz = xY + yX, xZ + zX, yZ + zY
        if energy_at is not None:
            trace = 0.25 * div
            tens = jnp.maximum(trace, 0.0)
            third = trace / 3.0
            ex, ey, ez = 0.25 * xX - third, 0.25 * yY - third, 0.25 * zZ - third
            dev = ex * ex + ey * ey + ez * ez
            she = (sxy * sxy + sxz * sxz + syz * syz) * 0.0625
            energy = 0.5 * BULK_MODULUS * tens * tens + LAME_MU * (dev + 0.5 * she)
            hist[energy_at] = jnp.where(g > 0.0, energy, 0.0)
        gl, g2, gs = k_lame * g, k_two * g, k_shear * g
        gt, gb, gc, g3 = k_twist * g, k_bend * g, k_cross * g, k_last * g
        pressure = gl * div
        fxX, fyY, fzZ = pressure + g2 * xX, pressure + g2 * yY, pressure + g2 * zZ
        txy, txz, tyz = gs * sxy, gs * sxz, gs * syz
        tw = xYZ + yXZ + zXY
        fxYZ, fyXZ, fzXY = gt * (xYZ + tw), gt * (yXZ + tw), gt * (zXY + tw)
        fyYZ, fxXZ = gb * yYZ + gc * xXZ, gb * xXZ + gc * yYZ
        fzYZ, fxXY = gb * zYZ + gc * xXY, gb * xXY + gc * zYZ
        fyXY, fzXZ = gb * yXY + gc * zXZ, gb * zXZ + gc * yXY
        FD = [
            fxX, fxXY, fxXZ, g3 * xXYZ,
            txy, fyXY, fyXZ, g3 * yXYZ,
            txz, fzXY, fzXZ, g3 * zXYZ,
        ]
        FS = [
            None, txy, txz, fxYZ,
            None, fyY, tyz, fyYZ,
            None, tyz, fzZ, fzYZ,
        ]
        lows = [(-FD[m]) if FS[m] is None else FS[m] - FD[m] for m in range(12)]
        highs = [FD[m] if FS[m] is None else FS[m] + FD[m] for m in range(12)]
        return lows, highs

    def element_pass(with_energy):
        def step(chunk, carry):
            r = pl.ds(pl.multiple_of(chunk * TILE, TILE), TILE)
            low = [modes[m, 0, r, :] for m in range(12)]
            held = None
            for p in range(nx - 1):
                high = [modes[m, p + 1, r, :] for m in range(12)]
                lows, highs = element(
                    low, high, stiff[p, r, :], (p, r, slice(None)) if with_energy else None
                )
                for m in range(12):
                    modes[m, p, r, :] = lows[m] + held[m] if p else lows[m]
                held, low = highs, high
            for m in range(12):
                modes[m, nx - 1, r, :] = held[m]
            low = [modes[m, GZ, r, :] for m in range(12)]
            lows, highs = element(
                low, [plane_up(a) for a in low], stiff[GZ, r, :],
                (GZ, r, slice(None)) if with_energy else None,
            )
            for m in range(12):
                modes[m, GZ, r, :] = lows[m] + plane_dn(highs[m])
            return carry

        lax.fori_loop(0, rows // TILE, step, 0, unroll=True)

    def each_node(emit, carry):
        ghosts = [half_back(*(modes[4 * c + m, GZ] for m in range(4))) for c in range(3)]
        taken = [pltpu.roll(g[1], 1, 1) for g in ghosts]
        for q in range(nx):
            got = []
            for c in range(3):
                near_w, far_w = half_back(*(modes[4 * c + m, q] for m in range(4)))
                got.append(near_w + z_dn(far_w, ghosts[c][1], q))
                taken[c] = z_dn_take(taken[c], far_w, q)
            carry = emit(q, got, carry)
        emit(GZ, [ghosts[c][0] + taken[c] for c in range(3)], carry)
        return carry

    nd, ng = DISP_ITERS, DMG_ITERS
    gram, vector = {}, {}

    def load_start(c, q):
        return gz_wide[c] if q == GZ else load_wide(c, q)

    pass_one(load_start, merge, rows, True)
    pl.when(there(outward, 0))(
        drain(ghost_deep.at[:, tiles_of[2]], ysend_sem.at[0], yrecv_sem.at[2]).wait_recv
    )
    low, a = damage_sum(0)
    taken = z_up_take(pltpu.roll(gz_wide[3], 127, 1), a, 0)
    for q in range(nx - 1):
        high, a = damage_sum(q + 1)
        stiff[q] = rigidity(low, high, valid)
        taken = z_up_take(taken, a, q + 1)
        low = high
    taken = gz_wide[3] + taken
    taken = merge(taken + y_up(taken))
    stiff[GZ] = rigidity(taken, plane_up(taken), gvalid)
    stiff[nx - 1] = blank
    element_pass(True)
    hist[nx - 1] = blank
    greet(hop_sem)
    arrive(1)
    for f in range(DEEP, fields):
        gz_rows[f - DEEP + 1] = line_rows(*ghost_tiles(f))
    gather_back(stiff, inv_emit)

    def start_emit(q, got, dot):
        inv = inverse[q]
        for c in range(3):
            r = load_rows(DEEP + c, q) - got[c]
            v = inv * r
            basis[c, q] = v
            if q < nx:
                resid[c, q] = r[0:TILE]
                dot = dot + v[0:TILE] * r[0:TILE]
        return dot

    vector[0] = each_node(start_emit, zero)

    def hist_emit(q, total):
        react[q] = jnp.maximum(jnp.abs(load_rows(7, q)), 0.125 * total)

    gather_back(hist, hist_emit)

    for k in range(nd - 1):
        pass_one(lambda c, q, k=k: basis[3 * k + c, q], same, rows, True)
        element_pass(False)

        def apply_emit(q, got, carry, k=k):
            carry = list(carry)
            inv = inverse[q] * (2.0 / SPECTRUM)
            for c in range(3):
                w = got[c]
                here = basis[3 * k + c, q]
                v = inv * w - here
                if k:
                    v = 2.0 * v - basis[3 * (k - 1) + c, q]
                basis[3 * (k + 1) + c, q] = v
                if q < nx:
                    wi, vi = w[0:TILE], v[0:TILE]
                    if k + 2 < nd:
                        images[3 * k + c, q] = wi
                    carry[0] = carry[0] + here[0:TILE] * wi
                    carry[1] = carry[1] + vi * resid[c, q]
                    carry[2] = carry[2] + vi * wi
                    for j in range(k):
                        carry[3 + j] = carry[3 + j] + vi * images[3 * j + c, q]
            return tuple(carry)

        got = each_node(apply_emit, (zero,) * (3 + k))
        gram[k, k], vector[k + 1], gram[k + 1, k] = got[:3]
        for j in range(k):
            gram[k + 1, j] = got[3 + j]

    across = pl.ds((1 - gx) * lx, lx)
    x_basis = xcopy(basis.at[:, across, 0:TILE], basis_part, 2)
    x_basis.start()

    def last_energy():
        pass_one(lambda c, q: basis[3 * (nd - 1) + c, q], same, TILE, False)
        total = zero
        for r in (slice(0, TILE),):
            low = [modes[m, 0, r, :] for m in range(12)]
            for p in range(nx - 1):
                high = [modes[m, p + 1, r, :] for m in range(12)]
                S = [low[m] + high[m] if m % 4 else None for m in range(12)]
                D = [high[m] - low[m] for m in range(12)]
                xX, xXY, xXZ, xXYZ = D[0:4]
                yX, yXY, yXZ, yXYZ = D[4:8]
                zX, zXY, zXZ, zXYZ = D[8:12]
                _, xY, xZ, xYZ = S[0:4]
                _, yY, yZ, yYZ = S[4:8]
                _, zY, zZ, zYZ = S[8:12]
                div = xX + yY + zZ
                sxy, sxz, syz = xY + yX, xZ + zX, yZ + zY
                tw = xYZ + yXZ + zXY
                sum_two = xX * xX + yY * yY + zZ * zZ
                sum_shear = sxy * sxy + sxz * sxz + syz * syz
                sum_twist = xYZ * xYZ + yXZ * yXZ + zXY * zXY + tw * tw
                sum_bend = (yYZ * yYZ + xXZ * xXZ) + (zYZ * zYZ + xXY * xXY) + (yXY * yXY + zXZ * zXZ)
                sum_cross = yYZ * xXZ + zYZ * xXY + yXY * zXZ
                sum_last = xXYZ * xXYZ + yXYZ * yXYZ + zXYZ * zXYZ
                energy = (
                    (k_lame * (div * div) + k_two * sum_two)
                    + (k_shear * sum_shear + k_twist * sum_twist)
                    + (k_bend * sum_bend + (2.0 * k_cross) * sum_cross)
                    + k_last * sum_last
                ) * stiff[p, r, :]
                total = total + energy
                low = high
        return total

    gram[nd - 1, nd - 1] = last_energy()

    cy = yvalid + element_at(ypos - 1, ngy * ly)
    cz = element_at(zpos, ngz * lz) + element_at(zpos - 1, ngz * lz)
    czg = element_at(zghost, ngz * lz) + element_at(zghost - 1, ngz * lz)
    cxg = jnp.where((lane < 16) | (lane >= 16 * (nx - 1)), 1.0, 2.0)
    node = jnp.where(cy * cz > 0.0, 1.0, 0.0)
    gnode = jnp.where(cy * czg > 0.0, 1.0, 0.0)
    diag_scale = laplace_diag * TOUGHNESS * LENGTH_SCALE
    lap_scale = TOUGHNESS * LENGTH_SCALE / 36.0

    def lines(d, after, before, count_z):
        s, n = after + before, count_z * d
        mass, slope = 2.0 * n + s, n - s
        s, n = y_up(mass) + y_dn(mass), cy * mass
        both = 2.0 * n + s
        mixed = (n - s) + (2.0 * (cy * slope) + (y_up(slope) + y_dn(slope)))
        return 2.0 * mixed + both, mixed - both

    def laplace_pass(load, emit, carry, with_ghost):
        ghost = load(GZ)
        after = pltpu.roll(ghost, 127, 1)
        before = pltpu.roll(ghost, 1, 1)
        ahead = []
        for q in range(nx):
            d = load(q)
            ahead.append(lines(d, z_up(d, ghost, q), z_dn(d, ghost, q), cz))
            if with_ghost:
                after = z_up_take(after, d, q)
                before = z_dn_take(before, d, q)
            p = q - 1
            if p >= 0:
                total = ahead[p][0] if p == 0 else 2.0 * ahead[p][0] + ahead[p - 1][1]
                carry = emit(p, lap_scale * (total + ahead[q][1]), carry)
        carry = emit(nx - 1, lap_scale * (ahead[nx - 1][0] + ahead[nx - 2][1]), carry)
        if with_ghost:
            inner, outer = lines(ghost, after, before, czg)
            total = cxg * inner + jnp.where(lane >= 16, plane_dn(outer), 0.0)
            total = total + jnp.where(lane < 16 * (nx - 1), plane_up(outer), 0.0)
            emit(GZ, lap_scale * total, carry)
        return carry

    def reaction_of(q):
        return TOUGHNESS / LENGTH_SCALE + 2.0 * react[q]

    def old_damage(q):
        return load_rows(3, q)

    def dstart(q, lap, dot):
        reaction = reaction_of(q)
        if q == GZ:
            count, mask = cxg * cy * czg, gnode
        else:
            count, mask = (cy * cz if q in (0, nx - 1) else 2.0 * cy * cz), node
        inv = mask / (diag_scale * count + reaction)
        dinverse[q] = inv
        r = 2.0 * react[q] - (lap + reaction * old_damage(q))
        v = inv * r
        dbasis[0, q] = v
        if q < nx:
            dresid[q] = r[0:TILE]
            dot = dot + v[0:TILE] * r[0:TILE]
        return dot

    dvector, dgram = {}, {}
    dvector[0] = laplace_pass(old_damage, dstart, zero, True)
    for k in range(ng):
        more = k + 1 < ng

        def dstep(q, lap, carry, k=k, more=more):
            carry = list(carry)
            here = dbasis[k, q]
            w = lap + reaction_of(q) * here
            if q < nx:
                carry[0] = carry[0] + here[0:TILE] * w[0:TILE]
            if more:
                v = dinverse[q] * w - here
                if k:
                    v = 2.0 * v - dbasis[k - 1, q]
                dbasis[k + 1, q] = v
                if q < nx:
                    carry[1] = carry[1] + v[0:TILE] * dresid[q]
                    carry[2] = carry[2] + v[0:TILE] * w[0:TILE]
            return tuple(carry)

        got = laplace_pass(
            lambda q, k=k: dbasis[k, q], dstep, (zero,) * (3 if more else 1), more
        )
        dgram[k, k] = got[0]
        if more:
            dvector[k + 1], dgram[k + 1, k] = got[1:]

    parts = [vector[i] for i in range(nd)] + [dvector[i] for i in range(ng)]
    parts += [gram[i, j] for i in range(nd) for j in range(i + 1)]
    parts += [dgram[i, j] for i in range(ng) for j in range(i + 1)]
    at = lax.broadcasted_iota(jnp.int32, (1, 128), 1)
    packed = jnp.zeros((1, 128), f32)
    for i, piece in enumerate(parts):
        line = jnp.sum(piece, axis=0, keepdims=True)
        packed = jnp.where(at == i, jnp.sum(line, axis=1, keepdims=True), packed)
    slot_mine = gx * npeer + me
    sums[slot_mine] = packed
    pl.semaphore_wait(hop_sem, number_near)

    def peer(dy, dz):
        return lax.rem(gy + dy, ngy), lax.rem(gz + dz, ngz)

    def peer_copy(side, dy, dz, slot):
        return remote(
            sums.at[slot_mine], sums.at[slot], asend_sem.at[0], arecv_sem.at[0],
            (gx if side == 0 else 1 - gx, *peer(dy, dz)),
        )

    offsets = sorted(
        [(dy, dz) for dy in range(ngy) for dz in range(ngz)],
        key=lambda o: -(2 * (o[1] % 2) + (o[1] > 0) + o[0] % 2 + (o[0] > 0)),
    )
    peers = [(side, dy, dz) for dy, dz in offsets for side in (0, 1) if side or dy or dz]
    sends = [peer_copy(side, dy, dz, slot_mine) for side, dy, dz in peers]
    for s in sends:
        s.start()
    x_damage = xcopy(dbasis.at[:, across, 0:TILE], dbasis_part, 3)
    x_damage.start()
    x_react = xcopy(react.at[across, 0:TILE], react_part, 4)
    x_react.start()
    x_parts = [x_basis, x_damage, x_react]
    for passed in x_parts:
        passed.wait_recv()

    def both_tiles(near_tile, far_tile):
        return jnp.concatenate(order(near_tile, far_tile), axis=0)

    for p in range(lx):
        out_history[p] = both_tiles(react[gx * lx + p, 0:TILE], react_part[p])
    everyone = drain(sums.at[0 : 2 * npeer - 1], asend_sem.at[0], arecv_sem.at[0])
    everyone.wait_recv()
    layer = [sums[i] for i in range(2 * npeer)]
    while len(layer) > 1:
        layer = [a + b for a, b in zip(layer[::2], layer[1::2])] + layer[len(layer) & ~1 :]
    whole = layer[0]

    scalars = [
        jnp.sum(jnp.where(at == i, whole, 0.0), axis=1, keepdims=True) for i in range(len(parts))
    ]

    def solve(rhs, lower):
        n = len(rhs)
        A = [[lower[max(i, j)][min(i, j)] for j in range(n)] for i in range(n)]
        b = list(rhs)
        for i in range(n):
            pivot = 1.0 / A[i][i]
            for r in range(i + 1, n):
                ratio = A[r][i] * pivot
                for c in range(i + 1, n):
                    A[r][c] = A[r][c] - ratio * A[i][c]
                b[r] = b[r] - ratio * b[i]
        out = [None] * n
        for i in reversed(range(n)):
            s = b[i]
            for j in range(i + 1, n):
                s = s - A[i][j] * out[j]
            out[i] = s / A[i][i]
        return out

    def triangle(flat, n):
        return [[flat[k * (k + 1) // 2 + j] for j in range(k + 1)] for k in range(n)]

    rest = scalars[nd + ng :]
    cut = nd * (nd + 1) // 2
    weights = solve(scalars[:nd], triangle(rest[:cut], nd))
    dweights = solve(scalars[nd : nd + ng], triangle(rest[cut:], ng))
    for p in range(lx):
        at_x = gx * lx + p
        for c in range(3):
            near_x = far_x = zero
            for k in range(nd):
                near_x = near_x + weights[k] * basis[3 * k + c, at_x, 0:TILE]
                far_x = far_x + weights[k] * basis_part[3 * k + c, p]
            lower, upper = order(near_x, far_x)
            out_disp[c, p, 0:TILE] = full_deep[c, 0, at_x] + lower
            out_disp[c, p, TILE:ly] = full_deep[c, 1, at_x] + upper
        near_d = far_d = zero
        for k in range(ng):
            near_d = near_d + dweights[k] * dbasis[k, at_x, 0:TILE]
            far_d = far_d + dweights[k] * dbasis_part[k, p]
        lower, upper = order(near_d, far_d)
        out_damage[p, 0:TILE] = full_deep[3, 0, at_x] + lower
        out_damage[p, TILE:ly] = full_deep[3, 1, at_x] + upper

    for side, dz in ((0, -1), (1, 1)):
        pl.when(there(0, dz))(
            drain(full_deep.at[0, 0], zsend_sem.at[side], zrecv_sem.at[0]).wait_send
        )
        for dy in (-1, 1):
            pl.when(there(dy, dz))(
                drain(zsend_deep.at[side], csend_sem.at[2 * (dy > 0) + side], crecv_sem.at[0]).wait_send
            )
    for kind in range(3):
        for dy in (-1, 1):
            pl.when(there(dy, 0))(ycopy(0, dy, kind).wait_send)
    for passed in x_own + x_parts:
        passed.wait_send()
    everyone.wait_send()


def hand_on(*refs):
    sources, targets, sem = refs[:3], refs[3:6], refs[6]
    copies = [
        pltpu.make_async_copy(source, target, sem.at[i])
        for i, (source, target) in enumerate(zip(sources, targets))
    ]
    for copy in copies:
        copy.start()
    for copy in copies:
        copy.wait()


def body_fused(sizes, *arrays):
    ngy, ngz, lx, ly, lz = sizes
    nx, rows, wide, fields = 2 * lx, 2 * TILE, 3 * TILE, 8
    packs, pairs, extras = fields * lx // 16, DEEP * lx // 2, DEEP * lx // TILE
    npeer = ngy * ngz
    f32 = jnp.float32
    planes = (nx + 1, rows, lz)
    vmem = pl.BlockSpec(memory_space=pltpu.VMEM)
    hbm = pl.BlockSpec(memory_space=pltpu.HBM)
    dma = pltpu.SemaphoreType.DMA

    def room(*shape):
        return pltpu.VMEM(shape, f32)

    results = pl.pallas_call(
        functools.partial(kernel, sizes),
        out_shape=(
            pltpu.VMEM((3, lx, ly, lz), f32),
            pltpu.VMEM((lx, ly, lz), f32),
            pltpu.VMEM((lx, ly, lz), f32),
        ),
        in_specs=[hbm] * 6,
        out_specs=(vmem,) * 3,
        scratch_shapes=[
            room(3, lx, ly, lz),
            room(3, lx, ly, lz),
            room(lx, ly, lz),
            room(lx, ly, lz),
            pltpu.VMEM((lx, ly, lz), jnp.int32),
            pltpu.VMEM((lx, ly, lz), jnp.int32),
            room(DEEP, 2, nx, TILE, lz),
            room(DEEP, 2, nx, TILE, lz),
            room(pairs + extras, TILE, 128),
            room(pairs + extras, TILE, 128),
            room(pairs, TILE, 128),
            room(pairs, TILE, 128),
            room(2, pairs + extras, TILE, 128),
            room(2, pairs, TILE, 128),
            room(2, 2, TILE, 128),
            room(2, 2, TILE, 128),
            room(2, 2, 3, TILE, 128),
            room(2, 2, 3, TILE, 128),
            room(4, wide, 128),
            room(5, rows, 128),
            room(12, *planes),
            room(3 * DISP_ITERS, *planes),
            room(3 * (DISP_ITERS - 2), nx, TILE, lz),
            room(3, nx, TILE, lz),
            room(*planes),
            room(*planes),
            room(*planes),
            room(*planes),
            room(*planes),
            room(DMG_ITERS, *planes),
            room(nx, TILE, lz),
            room(3 * DISP_ITERS, lx, TILE, lz),
            room(DMG_ITERS, lx, TILE, lz),
            room(lx, TILE, lz),
            room(2 * npeer, 1, 128),
            dma((2,)),
            dma((6,)),
            dma((3,)),
            dma((2,)),
            dma((4,)),
            dma((4,)),
            dma((4,)),
            dma((5,)),
            dma((5,)),
            dma((1,)),
            dma((1,)),
            pltpu.SemaphoreType.REGULAR,
        ],
        compiler_params=pltpu.CompilerParams(
            collective_id=0, has_side_effects=True, vmem_limit_bytes=VMEM_LIMIT
        ),
    )(*[pltpu.with_memory_space_constraint(a, pltpu.HBM) for a in arrays])
    return pl.pallas_call(
        hand_on,
        out_shape=tuple(jax.ShapeDtypeStruct(r.shape, f32) for r in results),
        in_specs=[vmem] * 3,
        out_specs=(hbm,) * 3,
        scratch_shapes=[dma((3,))],
        compiler_params=pltpu.CompilerParams(vmem_limit_bytes=1024 * 1024),
    )(*[pltpu.with_memory_space_constraint(r, pltpu.VMEM) for r in results])


VMEM_LIMIT = 24 * 1024 * 1024


def solution(mesh):
    shape = dict(mesh.shape)

    def body(*arrays):
        lx, ly, lz = arrays[2].shape
        fits = shape["gx"] == 2 and shape["gy"] * shape["gz"] > 1
        fits = fits and max(shape["gy"], shape["gz"]) <= 4
        fits = fits and lx == 4 and ly == 2 * TILE and lz == 128
        if fits:
            return body_fused((shape["gy"], shape["gz"], lx, ly, lz), *arrays)
        return body_any_mesh(*arrays)

    return jax.shard_map(
        body,
        mesh=mesh,
        in_specs=(
            P(None, "gx", "gy", "gz"),
            P(None, "gx", "gy", "gz"),
            P("gx", "gy", "gz"),
            P("gx", "gy", "gz"),
            P("gx", "gy", "gz"),
            P("gx", "gy", "gz"),
        ),
        out_specs=(P(None, "gx", "gy", "gz"), P("gx", "gy", "gz"), P("gx", "gy", "gz")),
        check_vma=False,
    )
```

```python
import functools
import jax
import jax.numpy as jnp
import numpy as np
from jax import lax
from jax.experimental import pallas as pl
from jax.experimental.pallas import tpu as pltpu
from jax.sharding import PartitionSpec as P

DISP_ITERS = 4
DMG_ITERS = 2


LAME_LAMBDA = 0.5769230769230769
LAME_MU = 0.38461538461538464
BULK_MODULUS = LAME_LAMBDA + 2.0 * LAME_MU / 3.0
RESIDUAL_STIFFNESS = 0.001
TOUGHNESS = 1.0
LENGTH_SCALE = 2.0
CRACK_HISTORY = 40.0


def padded_2(cells, sides, width):
    for axis, dim in sides:
        count = lax.axis_size(axis)
        ends = count - 1
        head = lax.slice_in_dim(cells, 0, width, axis=dim)
        tail = lax.slice_in_dim(cells, cells.shape[dim] - width, cells.shape[dim], axis=dim)
        cells = jnp.concatenate(
            [
                lax.ppermute(tail, axis, [(i, (i + 1) % count) for i in range(ends)]),
                cells,
                lax.ppermute(head, axis, [((i + 1) % count, i) for i in range(ends)]),
            ],
            axis=dim,
        )
    return cells


def corner_offsets(corner):
    return (corner >> 2 & 1, corner >> 1 & 1, corner & 1)


def shape_gradients(sample):
    gradient = np.zeros((3, 8))
    for corner in range(8):
        offsets = corner_offsets(corner)
        values = [sample[k] if offsets[k] else 1.0 - sample[k] for k in range(3)]
        slopes = [1.0 if offsets[k] else -1.0 for k in range(3)]
        gradient[0, corner] = slopes[0] * values[1] * values[2]
        gradient[1, corner] = values[0] * slopes[1] * values[2]
        gradient[2, corner] = values[0] * values[1] * slopes[2]
    return gradient


def strain_matrix(gradient):
    strain = np.zeros((6, 24))
    for corner in range(8):
        column = 3 * corner
        strain[0, column] = gradient[0, corner]
        strain[1, column + 1] = gradient[1, corner]
        strain[2, column + 2] = gradient[2, corner]
        strain[3, column] = gradient[1, corner]
        strain[3, column + 1] = gradient[0, corner]
        strain[4, column + 1] = gradient[2, corner]
        strain[4, column + 2] = gradient[1, corner]
        strain[5, column] = gradient[2, corner]
        strain[5, column + 2] = gradient[0, corner]
    return strain


def element_tables():
    moduli = np.zeros((6, 6))
    moduli[:3, :3] = LAME_LAMBDA
    for k in range(3):
        moduli[k, k] += 2.0 * LAME_MU
        moduli[k + 3, k + 3] = LAME_MU
    points = [0.5 - 0.5 / np.sqrt(3.0), 0.5 + 0.5 / np.sqrt(3.0)]
    stiff_table = np.zeros((24, 24))
    laplace_table = np.zeros((8, 8))
    for sample_index in range(8):
        sample = tuple((points[k] for k in corner_offsets(sample_index)))
        gradient = shape_gradients(sample)
        strain = strain_matrix(gradient)
        stiff_table += 0.125 * strain.T @ moduli @ strain
        laplace_table += 0.125 * gradient.T @ gradient
    centre_table = strain_matrix(shape_gradients((0.5, 0.5, 0.5)))
    return (
        stiff_table.astype(np.float32),
        laplace_table.astype(np.float32),
        centre_table.astype(np.float32),
    )


def corner_views(padded, element_shape):
    corner_list = []
    for corner in range(8):
        offx, offy, offz = corner_offsets(corner)
        corner_list.append(
            padded[
                ...,
                offx : offx + element_shape[0],
                offy : offy + element_shape[1],
                offz : offz + element_shape[2],
            ]
        )
    return corner_list


def assemble_nodes(pieces):
    running = None
    for corner in range(8):
        offx, offy, offz = corner_offsets(corner)
        leading = [(0, 0)] * (pieces[corner].ndim - 3)
        placed = jnp.pad(
            pieces[corner], leading + [(offx, 1 - offx), (offy, 1 - offy), (offz, 1 - offz)]
        )
        running = placed if running is None else running + placed
    return running


def line_valid(position, devices, count):
    index = position * count + jnp.arange(count + 1, dtype=jnp.int32) - 1
    return ((index >= 0) & (index <= devices * count - 2)).astype(jnp.float32)


def strain_energy(strain):
    trace = strain[0] + strain[1] + strain[2]
    deviator = strain[:3] - trace[None] / 3.0
    shear = strain[3:]
    tensile = jnp.maximum(trace, 0.0)
    return 0.5 * BULK_MODULUS * tensile * tensile + LAME_MU * (
        jnp.sum(deviator * deviator, axis=0) + 0.5 * jnp.sum(shear * shear, axis=0)
    )


def forces_to_nodes(forces, stiffness):
    pieces = [stiffness[None] * forces[3 * target : 3 * target + 3] for target in range(8)]
    return assemble_nodes(pieces)


def element_apply(padded, stiffness, stiff_table):
    element_shape = stiffness.shape
    flat = jnp.stack(corner_views(padded, element_shape)).reshape(24, -1)
    forces = jnp.dot(stiff_table, flat, precision=lax.Precision.HIGHEST).reshape(
        (24,) + element_shape
    )
    return forces_to_nodes(forces, stiffness)


def laplace_apply(padded, element_valid, laplace_table):
    element_shape = element_valid.shape
    flat = jnp.stack(corner_views(padded, element_shape)).reshape(8, -1)
    forces = jnp.dot(laplace_table, flat, precision=lax.Precision.HIGHEST).reshape(
        (8,) + element_shape
    )
    return assemble_nodes([element_valid * forces[target] for target in range(8)])


def single_pair(pair):
    return tuple(lax.psum(pair, ("gx", "gy", "gz")))


def conjugate(solutions, residuals, inverses, counts, apply_fn):
    solutions = list(solutions)
    residuals = list(residuals)
    number = len(solutions)
    steps = max(counts)

    def pair_totals(pairs):
        return [single_pair(pairs[0])]

    precs = [inverses[0] * residuals[0]]
    applied = apply_fn(precs, list(range(number)))
    pairs = pair_totals([(jnp.sum(residuals[0] * precs[0]), jnp.sum(precs[0] * applied[0]))])
    norms = [pair[0] for pair in pairs]
    lengths = [pair[0] / pair[1] for pair in pairs]
    directions = list(precs)
    alongs = list(applied)
    for step in range(steps):
        active = [i for i in range(number) if step < counts[i]]
        for i in active:
            solutions[i] = solutions[i] + lengths[i] * directions[i]
            residuals[i] = residuals[i] - lengths[i] * alongs[i]
        later = [i for i in active if step + 1 < counts[i]]
        if later:
            i = later[0]
            precs[i] = inverses[i] * residuals[i]
            images = apply_fn([precs[i] for i in later], later)
            pairs = pair_totals(
                [
                    (jnp.sum(residuals[i] * precs[i]), jnp.sum(precs[i] * images[k]))
                    for k, i in enumerate(later)
                ]
            )
            for k, i in enumerate(later):
                norm_next, curve_sum = pairs[k]
                ratio = norm_next / norms[i]
                lengths[i] = norm_next / (curve_sum - ratio * norm_next / lengths[i])
                directions[i] = precs[i] + ratio * directions[i]
                alongs[i] = images[k] + ratio * alongs[i]
                norms[i] = norm_next
    return solutions


def body_any_mesh(displacement_start, external_force, damage_old, history_old, crack_labels, fixed_flags):
    tables = element_tables()
    stiff_table = jnp.asarray(tables[0], jnp.float32)
    laplace_table = jnp.asarray(tables[1], jnp.float32)
    centre_table = jnp.asarray(tables[2], jnp.float32)
    highest = lax.Precision.HIGHEST
    size_x, size_y, size_z = damage_old.shape
    free_mask = 1.0 - fixed_flags.astype(jnp.float32)
    start_disp = displacement_start * free_mask[None]
    element_valid = (
        line_valid(lax.axis_index("gx"), lax.axis_size("gx"), size_x)[:, None, None]
        * line_valid(lax.axis_index("gy"), lax.axis_size("gy"), size_y)[None, :, None]
        * line_valid(lax.axis_index("gz"), lax.axis_size("gz"), size_z)[None, None, :]
    )
    element_shape = element_valid.shape
    start_pad = padded_2(
        jnp.concatenate([start_disp, damage_old[None]], axis=0),
        (("gx", 1), ("gy", 2), ("gz", 3)),
        1,
    )
    corner_list = corner_views(start_pad, element_shape)
    damage_mean = sum((view[3] for view in corner_list)) / 8.0
    stiffness = ((1.0 - damage_mean) ** 2 + RESIDUAL_STIFFNESS) * element_valid
    flat = jnp.stack([view[:3] for view in corner_list]).reshape(24, -1)
    combined = jnp.dot(
        jnp.concatenate([stiff_table, centre_table], axis=0), flat, precision=highest
    )
    forces = combined[:24].reshape((24,) + element_shape)
    strain = combined[24:].reshape((6,) + element_shape)
    start_image = forces_to_nodes(forces, stiffness)[:, 1:-1, 1:-1, 1:-1]
    energy = strain_energy(strain) * element_valid
    nodal_energy = assemble_nodes([energy] * 8)[1:-1, 1:-1, 1:-1] / 8.0
    history = jnp.maximum(
        jnp.maximum(history_old, nodal_energy), CRACK_HISTORY * crack_labels.astype(jnp.float32)
    )
    stiff_diag = jnp.diagonal(stiff_table)
    diag_pieces = [
        stiffness[None] * stiff_diag[3 * target : 3 * target + 3][:, None, None, None]
        for target in range(8)
    ]
    elastic_diag = assemble_nodes(diag_pieces)[:, 1:-1, 1:-1, 1:-1]
    inverse_elastic = 1.0 / (free_mask[None] * elastic_diag + (1.0 - free_mask[None]))

    def constrained(nodal_field):
        masked = free_mask[None] * nodal_field
        padded = padded_2(masked, (("gx", 1), ("gy", 2), ("gz", 3)), 1)
        nodes = element_apply(padded, stiffness, stiff_table)[:, 1:-1, 1:-1, 1:-1]
        return free_mask[None] * nodes + (1.0 - free_mask[None]) * nodal_field

    reaction = TOUGHNESS / LENGTH_SCALE + 2.0 * history
    laplace_diag = assemble_nodes(
        [element_valid * laplace_table[target, target] for target in range(8)]
    )[1:-1, 1:-1, 1:-1]
    inverse_damage = 1.0 / (TOUGHNESS * LENGTH_SCALE * laplace_diag + reaction)
    residual = free_mask[None] * (external_force - start_image)
    start_lap = laplace_apply(start_pad[3], element_valid, laplace_table)[1:-1, 1:-1, 1:-1]
    damage_residual = 2.0 * history - (TOUGHNESS * LENGTH_SCALE * start_lap + reaction * damage_old)

    def damage_operator(nodal_field):
        padded = padded_2(nodal_field, (("gx", 0), ("gy", 1), ("gz", 2)), 1)
        lap_nodes = laplace_apply(padded, element_valid, laplace_table)[1:-1, 1:-1, 1:-1]
        return TOUGHNESS * LENGTH_SCALE * lap_nodes + reaction * nodal_field

    def single_elastic(fields, active):
        return [constrained(fields[0])]

    def single_damage(fields, active):
        return [damage_operator(fields[0])]

    displacement = conjugate(
        [start_disp], [residual], [inverse_elastic], [DISP_ITERS], single_elastic
    )[0]
    damage = conjugate(
        [damage_old], [damage_residual], [inverse_damage], [DMG_ITERS], single_damage
    )[0]
    return (displacement, damage, history)


SPECTRUM = 3.2
TILE = 8
GHOST = 4
DEEP = 4
MESH = pl.DeviceIdType.MESH


def walsh_tables():
    stiff, laplace, _ = element_tables()
    signs = np.array(
        [
            [np.prod([1.0 if c >> k & 1 else (-1.0 if m >> k & 1 else 1.0) for k in range(3)]) for c in range(8)]
            for m in range(8)
        ]
    )
    wide = np.kron(signs, np.eye(3))
    stiff_modes = wide @ stiff.astype(np.float64) @ wide.T / 64.0
    return stiff_modes, float(stiff[0, 0]), float(laplace[0, 0])


def kernel(
    sizes,
    disp_in,
    force_in,
    damage_in,
    history_in,
    labels_in,
    flags_in,
    out_disp,
    out_damage,
    out_history,
    disp_ref,
    force_ref,
    damage_ref,
    history_ref,
    labels_ref,
    flags_ref,
    full_deep,
    full_flat,
    down_deep,
    up_deep,
    down_flat,
    up_flat,
    ghost_deep,
    ghost_flat,
    zsend_deep,
    zsend_flat,
    zbuf_deep,
    zbuf_flat,
    gz_wide,
    gz_rows,
    modes,
    basis,
    images,
    resid,
    stiff,
    inverse,
    hist,
    react,
    dinverse,
    dbasis,
    dresid,
    basis_part,
    dbasis_part,
    react_part,
    sums,
    in_sem,
    ysend_sem,
    yrecv_sem,
    zsend_sem,
    zrecv_sem,
    csend_sem,
    crecv_sem,
    xsend_sem,
    xrecv_sem,
    asend_sem,
    arecv_sem,
    hop_sem,
):
    ngy, ngz, lx, ly, lz = sizes
    nx = 2 * lx
    fields = 8
    npeer = ngy * ngz
    pairs = DEEP * lx // 2
    packs = fields * lx // 16
    extras = DEEP * lx // TILE
    wide, rows = 3 * TILE, 2 * TILE
    GZ = nx
    f32 = jnp.float32
    stiff_modes, stiff_diag, laplace_diag = walsh_tables()
    gx, gy, gz = lax.axis_index("gx"), lax.axis_index("gy"), lax.axis_index("gz")
    me = gy * ngz + gz
    partner = (1 - gx, gy, gz)
    outward = 2 * gx - 1
    full, zsend, zbuf = (full_deep, full_flat), (zsend_deep, zsend_flat), (zbuf_deep, zbuf_flat)

    def there(dy, dz):
        y, z = gy + dy, gz + dz
        return (y >= 0) & (y < ngy) & (z >= 0) & (z < ngz)

    def device(core, dy, dz):
        return core, lax.rem(gy + dy + ngy, ngy), lax.rem(gz + dz + ngz, ngz)

    near = [(dy, dz) for dy in (-1, 0, 1) for dz in (-1, 0, 1) if dy or dz]
    number_near = 2 * sum(there(dy, dz).astype(jnp.int32) for dy, dz in near)

    barrier = pltpu.get_barrier_semaphore()

    def greet(semaphore):
        for dy, dz in near:

            @pl.when(there(dy, dz))
            def _():
                for core in (gx, 1 - gx):
                    pl.semaphore_signal(
                        semaphore, inc=1, device_id=device(core, dy, dz), device_id_type=MESH
                    )

    loads = [
        pltpu.make_async_copy(source, target, in_sem.at[i])
        for source, target, i in (
            (flags_in, flags_ref, 1),
            (disp_in, disp_ref, 0),
            (damage_in, damage_ref, 1),
            (force_in, force_ref, 0),
            (history_in, history_ref, 1),
            (labels_in, labels_ref, 1),
        )
    ]
    for load in loads:
        load.start()
    greet(barrier)
    pl.semaphore_signal(barrier, inc=1, device_id=partner, device_id_type=MESH)

    zero = jnp.zeros((TILE, 128), f32)
    for dz, side in ((1, 0), (-1, 1)):

        @pl.when(jnp.logical_not(there(0, dz)))
        def _():
            for core in range(2):
                for ref in zbuf:
                    ref[core, side, 0:2] = jnp.zeros((2, TILE, 128), f32)

        @pl.when(jnp.logical_not(there(outward, dz)))
        def _():
            for core in range(2):
                for ref in zbuf:
                    ref[core, side, 2] = zero

    @pl.when(jnp.logical_not(there(outward, 0)))
    def _():
        ghost_deep[...] = jnp.zeros(ghost_deep.shape, f32)
        ghost_flat[...] = jnp.zeros(ghost_flat.shape, f32)

    for i, room in enumerate((basis_part, full_deep.at[0:2])):
        pltpu.make_async_copy(room, room, in_sem.at[i]).wait()

    values = []
    for p in range(lx):
        flag = flags_ref[p].astype(f32)
        free = 1.0 - flag
        top = jnp.maximum(history_ref[p], CRACK_HISTORY * labels_ref[p].astype(f32))
        here = [free * disp_ref[c, p] for c in range(3)]
        here += [damage_ref[p]] + [force_ref[c, p] for c in range(3)] + [top * (free - flag)]
        for f in range(fields):
            for half in range(2):
                full[f // DEEP][f % DEEP, half, gx * lx + p] = here[f][TILE * half : TILE * half + TILE]
        values.append(here)

    sub = lax.broadcasted_iota(jnp.int32, (TILE, 128), 0)

    def spin(a, shift, axis):
        shift = shift % a.shape[axis]
        return pltpu.roll(a, shift, axis) if shift else a

    def spot(f, q):
        return 8 * (f % 4 // 2) + 2 * q + f % 2

    group = lax.broadcasted_iota(jnp.int32, (ly, 128), 1) // 8
    for j in range(packs):
        low = jnp.zeros((ly, 128), f32)
        high = jnp.zeros((ly, 128), f32)
        for f in range(4 * j, 4 * j + 4):
            for q in range(lx):
                k = spot(f, q)
                turned = spin(values[q][f], 8 * k + 8, 1)
                low = jnp.where(group == (k + 1) % 16, turned, low)
                high = jnp.where(group == k, turned, high)
        for half in range(2):
            zsend[j][0, half] = low[TILE * half : TILE * half + TILE]
            zsend[j][1, half] = high[TILE * half : TILE * half + TILE]
    for first, skip, down, up in ((0, extras, down_deep, up_deep), (DEEP, 0, down_flat, up_flat)):
        for j in range(pairs):
            fa, qa = divmod(2 * j, lx)
            fb, qb = divmod(2 * j + 1, lx)
            a, b = values[qa][first + fa], values[qb][first + fb]
            down[skip + j] = jnp.where(sub < GHOST, a[0:TILE], spin(b[0:TILE], GHOST, 0))
            up[skip + j] = jnp.where(sub < GHOST, spin(b[ly - TILE : ly], GHOST, 0), a[ly - TILE : ly])
    for e in range(extras):
        tile = jnp.zeros((TILE, 128), f32)
        for s in range(TILE):
            f, q = divmod(TILE * e + s, lx)
            tile = jnp.where(sub == s, spin(values[q][f][0:TILE], s - GHOST, 0), tile)
        down_deep[e] = tile

    pl.semaphore_wait(barrier, number_near + 1)

    def remote(src, dst, send, recv, target):
        return pltpu.make_async_remote_copy(
            src_ref=src, dst_ref=dst, send_sem=send, recv_sem=recv,
            device_id=target, device_id_type=MESH,
        )

    def xcopy(src, dst, k):
        return remote(src, dst, xsend_sem.at[k], xrecv_sem.at[k], partner)

    def zcopy(source, dz, pack, core):
        side = 0 if dz < 0 else 1
        return remote(
            zsend[pack].at[side], zbuf[pack].at[source, side, 0:2],
            zsend_sem.at[side], zrecv_sem.at[2 * side + pack],
            device(core, 0, dz),
        )

    def corner(source, dy, dz, pack):
        side = 0 if dz < 0 else 1
        return remote(
            zsend[pack].at[side, int(dy > 0)], zbuf[pack].at[source, side, 2],
            csend_sem.at[2 * (dy > 0) + side],
            crecv_sem.at[2 * side + pack],
            device(int(dy < 0), dy, dz),
        )

    last = extras + 3 * lx // 2
    tiles_of = {0: slice(extras, last), 2: slice(last, extras + pairs)}

    def ycopy(source, dy, kind):
        if kind == 1:
            src, dst = (down_flat if dy < 0 else up_flat), ghost_flat.at[source]
        else:
            tiles = slice(0, last) if dy < 0 and kind == 0 else tiles_of[kind]
            src = (down_deep if dy < 0 else up_deep).at[tiles]
            dst = ghost_deep.at[source, tiles]
        return remote(
            src, dst, ysend_sem.at[2 * kind + (dy > 0)], yrecv_sem.at[kind],
            device(int(dy < 0), dy, 0),
        )

    own = pl.ds(gx * lx, lx)
    x_own = [
        xcopy(full[flat].at[:, :, own], full[flat].at[:, :, own], flat) for flat in range(2)
    ]
    halos = []
    for dy in (1, -1):
        for flat in (0, 1):
            for source in (0, 1):
                ways = [((dy, dz), corner(source, dy, dz, flat)) for dz in (-1, 1)]
                ways += [((dy, 0), ycopy(source, dy, kind)) for kind in ((1,) if flat else (0, 2))]
                if dy > 0:
                    ways += [
                        ((0, dz), zcopy(source, dz, flat, core)) for dz in (-1, 1) for core in (0, 1)
                    ]
                halos += [((gx == source) & there(*way), copy) for way, copy in ways]
    for exchange in x_own:
        exchange.start()
    for guard, copy in halos:
        pl.when(guard)(copy.start)

    def drain(ref, send, recv):
        return remote(ref, ref, send, recv, partner)

    def arrive(flat):
        for side, dz in ((0, -1), (1, 1)):
            faces = zbuf[flat].at[:, side, 0:2]
            pl.when(there(0, -dz))(
                drain(faces, zsend_sem.at[side], zrecv_sem.at[2 * side + flat]).wait_recv
            )
        x_own[flat].wait_recv()
        for side, dz in ((0, -1), (1, 1)):
            edges = zbuf[flat].at[:, side, 2]
            pl.when(there(outward, -dz))(
                drain(edges, csend_sem.at[side], crecv_sem.at[2 * side + flat]).wait_recv
            )
        rows_in = [ghost_flat] * 2 if flat else [ghost_deep.at[:, tiles_of[0]], ghost_deep.at[:, 0:last]]
        for core in range(2):
            pl.when((gx == core) & there(outward, 0))(
                drain(rows_in[core], ysend_sem.at[flat], yrecv_sem.at[flat]).wait_recv
            )

    arrive(0)

    lane_w = lax.broadcasted_iota(jnp.int32, (wide, 128), 1)
    odd = lane_w // 8 % 2

    def merge(a):
        return jnp.concatenate(
            [a[0:TILE], jnp.where(sub < GHOST, a[TILE : 2 * TILE], a[2 * TILE :])], axis=0
        )

    is_lower = sub + TILE * gx < TILE
    from_theirs = (sub + GHOST * gx) % TILE < GHOST

    def order(lower, upper):
        return jnp.where(is_lower, lower, upper), jnp.where(is_lower, upper, lower)

    def ghost_tiles(f):
        halves = []
        for source in range(2):
            ref = zbuf[f // 4]
            low, high = (
                jnp.concatenate([ref[source, side, k] for k in range(3)], axis=0) for side in range(2)
            )
            both = jnp.where(odd == f % 2, high, low)
            halves.append(spin(both, 8 * (2 * lx * source - spot(f, 0)), 1))
        whole = jnp.where(lane_w < 16 * lx, *halves)
        return *order(whole[0:TILE], whole[TILE : 2 * TILE]), whole[2 * TILE :]

    def line_wide(tile, other, up, down):
        return jnp.concatenate(
            [tile, jnp.where(is_lower, other, up), jnp.where(is_lower, down, other)], axis=0
        )

    def line_rows(tile, other, ghost):
        return jnp.concatenate([tile, jnp.where(from_theirs, other, ghost)], axis=0)

    for f in range(DEEP):
        tile, other, ghost = ghost_tiles(f)
        gz_wide[f] = line_wide(tile, other, ghost, ghost)
    gz_rows[0] = merge(gz_wide[DEEP - 1])

    def pieces(f, q):
        source, p = divmod(q, lx)
        j, half = divmod(f % DEEP * lx + p, 2)
        ghost = ghost_deep[source, extras + j] if f < DEEP else ghost_flat[source, j]
        ref = full[f // DEEP]
        return *order(ref[f % DEEP, 0, q], ref[f % DEEP, 1, q]), spin(ghost, GHOST * half, 0)

    def load_wide(f, q):
        tile, other, ghost = pieces(f, q)
        e, s = divmod(f * lx + q % lx, TILE)
        extra = spin(ghost_deep[q // lx, e], GHOST - s, 0)
        return line_wide(tile, other, jnp.where(sub == GHOST, extra, ghost), ghost)

    def load_rows(f, q):
        if q == GZ:
            return gz_rows[f - DEEP + 1]
        return line_rows(*pieces(f, q))

    row = lax.broadcasted_iota(jnp.int32, (rows, 128), 0)
    lane = lax.broadcasted_iota(jnp.int32, (rows, 128), 1)
    inside = lane % 16
    ypos = gy * ly + gx * TILE + jnp.where(row < TILE + GHOST, row, row - rows)
    zpos = gz * lz + lane
    zghost = gz * lz + jnp.where(inside < 8, inside - 8, inside + (lz - 8))

    def element_at(pos, count):
        return jnp.where((pos >= 0) & (pos <= count - 2), 1.0, 0.0)

    yvalid = element_at(ypos, ngy * ly)
    valid = yvalid * element_at(zpos, ngz * lz)
    gvalid = jnp.where(lane < 16 * (nx - 1), yvalid * element_at(zghost, ngz * lz), 0.0)

    def y_up(a):
        return pltpu.roll(a, a.shape[0] - 1, 0)

    def y_dn(a):
        return pltpu.roll(a, 1, 0)

    def lanes(a):
        return lane_w if a.shape[0] == wide else lane

    def z_up(a, ghost, p):
        return jnp.where(lanes(a) == 127, spin(ghost, 119 - 16 * p, 1), pltpu.roll(a, 127, 1))

    def z_up_take(acc, a, p):
        return jnp.where(lanes(a) == 16 * p + 7, spin(a, 16 * p + 7, 1), acc)

    def z_dn(a, ghost, p):
        return jnp.where(lanes(a) == 0, spin(ghost, 121 - 16 * p, 1), pltpu.roll(a, 1, 1))

    def z_dn_take(acc, a, p):
        return jnp.where(lanes(a) == 16 * p + 8, spin(a, 16 * p + 9, 1), acc)

    def plane_up(a):
        return pltpu.roll(a, 112, 1)

    def plane_dn(a):
        return pltpu.roll(a, 16, 1)

    blank = jnp.zeros((rows, 128), f32)

    def half_back(ss, yd, zd, yz):
        s = (ss - yd) + y_dn(ss + yd)
        d = (zd - yz) + y_dn(zd + yz)
        return s - d, s + d

    def damage_sum(q):
        a = load_wide(3, q)
        s = a + z_up(a, gz_wide[3], q)
        return merge(s + y_up(s)), a

    def rigidity(low, high, mask):
        rest = 1.0 - (low + high) * 0.125
        return (rest * rest + RESIDUAL_STIFFNESS) * mask


    def gather_back(ref, emit):
        ghost = ref[GZ]
        below = blank
        taken = pltpu.roll(ghost, 1, 1)
        for q in range(nx):
            a = ref[q]
            s = a + z_dn(a, ghost, q)
            here = s + y_dn(s)
            emit(q, below + here)
            below = here
            taken = z_dn_take(taken, a, q)
        s = ghost + taken
        s = s + y_dn(s)
        emit(GZ, s + plane_dn(s))

    def inv_emit(q, total):
        free = load_rows(7, q) > 0.0
        inverse[q] = jnp.where(free, 1.0 / jnp.where(free, stiff_diag * total, 1.0), 0.0)

    def forward(u, near_u, keep):
        zs, zd = u + near_u, near_u - u
        a, b = keep(y_up(zs)), keep(y_up(zd))
        zs, zd = keep(zs), keep(zd)
        return zs + a, a - zs, zd + b, b - zd

    def same(a):
        return a

    def pass_one(load, keep, height, with_ghost):
        for c in range(3):
            ghost = load(c, GZ)
            taken = pltpu.roll(ghost, 127, 1)
            for q in range(nx):
                u = load(c, q)
                out = forward(u, z_up(u, ghost, q), keep)
                for m in range(4):
                    modes[4 * c + m, q, 0:height] = out[m][0:height]
                if with_ghost:
                    taken = z_up_take(taken, u, q)
            if with_ghost:
                out = forward(ghost, taken, keep)
                for m in range(4):
                    modes[4 * c + m, GZ] = out[m]

    def sm(mode_a, comp_a, mode_b, comp_b):
        return float(stiff_modes[3 * mode_a + comp_a, 3 * mode_b + comp_b])

    k_lame = sm(4, 0, 2, 1)
    k_two = sm(4, 0, 4, 0) - k_lame
    k_shear = sm(2, 0, 2, 0)
    k_twist = sm(3, 0, 5, 1)
    k_bend = sm(3, 1, 3, 1)
    k_cross = sm(3, 1, 5, 0)
    k_last = sm(7, 0, 7, 0)

    def element(low, high, g, energy_at):
        S = [low[m] + high[m] if m % 4 else None for m in range(12)]
        D = [high[m] - low[m] for m in range(12)]
        xX, xXY, xXZ, xXYZ = D[0:4]
        yX, yXY, yXZ, yXYZ = D[4:8]
        zX, zXY, zXZ, zXYZ = D[8:12]
        _, xY, xZ, xYZ = S[0:4]
        _, yY, yZ, yYZ = S[4:8]
        _, zY, zZ, zYZ = S[8:12]
        div = xX + yY + zZ
        sxy, sxz, syz = xY + yX, xZ + zX, yZ + zY
        if energy_at is not None:
            trace = 0.25 * div
            tens = jnp.maximum(trace, 0.0)
            third = trace / 3.0
            ex, ey, ez = 0.25 * xX - third, 0.25 * yY - third, 0.25 * zZ - third
            dev = ex * ex + ey * ey + ez * ez
            she = (sxy * sxy + sxz * sxz + syz * syz) * 0.0625
            energy = 0.5 * BULK_MODULUS * tens * tens + LAME_MU * (dev + 0.5 * she)
            hist[energy_at] = jnp.where(g > 0.0, energy, 0.0)
        gl, g2, gs = k_lame * g, k_two * g, k_shear * g
        gt, gb, gc, g3 = k_twist * g, k_bend * g, k_cross * g, k_last * g
        pressure = gl * div
        fxX, fyY, fzZ = pressure + g2 * xX, pressure + g2 * yY, pressure + g2 * zZ
        txy, txz, tyz = gs * sxy, gs * sxz, gs * syz
        tw = xYZ + yXZ + zXY
        fxYZ, fyXZ, fzXY = gt * (xYZ + tw), gt * (yXZ + tw), gt * (zXY + tw)
        fyYZ, fxXZ = gb * yYZ + gc * xXZ, gb * xXZ + gc * yYZ
        fzYZ, fxXY = gb * zYZ + gc * xXY, gb * xXY + gc * zYZ
        fyXY, fzXZ = gb * yXY + gc * zXZ, gb * zXZ + gc * yXY
        FD = [
            fxX, fxXY, fxXZ, g3 * xXYZ,
            txy, fyXY, fyXZ, g3 * yXYZ,
            txz, fzXY, fzXZ, g3 * zXYZ,
        ]
        FS = [
            None, txy, txz, fxYZ,
            None, fyY, tyz, fyYZ,
            None, tyz, fzZ, fzYZ,
        ]
        lows = [(-FD[m]) if FS[m] is None else FS[m] - FD[m] for m in range(12)]
        highs = [FD[m] if FS[m] is None else FS[m] + FD[m] for m in range(12)]
        return lows, highs

    def element_pass(with_energy):
        def step(chunk, carry):
            r = pl.ds(pl.multiple_of(chunk * TILE, TILE), TILE)
            low = [modes[m, 0, r, :] for m in range(12)]
            held = None
            for p in range(nx - 1):
                high = [modes[m, p + 1, r, :] for m in range(12)]
                lows, highs = element(
                    low, high, stiff[p, r, :], (p, r, slice(None)) if with_energy else None
                )
                for m in range(12):
                    modes[m, p, r, :] = lows[m] + held[m] if p else lows[m]
                held, low = highs, high
            for m in range(12):
                modes[m, nx - 1, r, :] = held[m]
            low = [modes[m, GZ, r, :] for m in range(12)]
            lows, highs = element(
                low, [plane_up(a) for a in low], stiff[GZ, r, :],
                (GZ, r, slice(None)) if with_energy else None,
            )
            for m in range(12):
                modes[m, GZ, r, :] = lows[m] + plane_dn(highs[m])
            return carry

        lax.fori_loop(0, rows // TILE, step, 0, unroll=True)

    def each_node(emit, carry):
        ghosts = [half_back(*(modes[4 * c + m, GZ] for m in range(4))) for c in range(3)]
        taken = [pltpu.roll(g[1], 1, 1) for g in ghosts]
        for q in range(nx):
            got = []
            for c in range(3):
                near_w, far_w = half_back(*(modes[4 * c + m, q] for m in range(4)))
                got.append(near_w + z_dn(far_w, ghosts[c][1], q))
                taken[c] = z_dn_take(taken[c], far_w, q)
            carry = emit(q, got, carry)
        emit(GZ, [ghosts[c][0] + taken[c] for c in range(3)], carry)
        return carry

    cy = yvalid + element_at(ypos - 1, ngy * ly)
    cz = element_at(zpos, ngz * lz) + element_at(zpos - 1, ngz * lz)
    czg = element_at(zghost, ngz * lz) + element_at(zghost - 1, ngz * lz)
    cxg = jnp.where((lane < 16) | (lane >= 16 * (nx - 1)), 1.0, 2.0)
    node = jnp.where(cy * cz > 0.0, 1.0, 0.0)
    gnode = jnp.where(cy * czg > 0.0, 1.0, 0.0)
    diag_scale = laplace_diag * TOUGHNESS * LENGTH_SCALE
    lap_scale = TOUGHNESS * LENGTH_SCALE / 36.0

    def lines(d, after, before, count_z):
        s, n = after + before, count_z * d
        mass, slope = 2.0 * n + s, n - s
        s, n = y_up(mass) + y_dn(mass), cy * mass
        both = 2.0 * n + s
        mixed = (n - s) + (2.0 * (cy * slope) + (y_up(slope) + y_dn(slope)))
        return 2.0 * mixed + both, mixed - both

    def laplace_pass(load, emit, carry, with_ghost):
        ghost = load(GZ)
        after = pltpu.roll(ghost, 127, 1)
        before = pltpu.roll(ghost, 1, 1)
        ahead = []
        for q in range(nx):
            d = load(q)
            ahead.append(lines(d, z_up(d, ghost, q), z_dn(d, ghost, q), cz))
            if with_ghost:
                after = z_up_take(after, d, q)
                before = z_dn_take(before, d, q)
            p = q - 1
            if p >= 0:
                total = ahead[p][0] if p == 0 else 2.0 * ahead[p][0] + ahead[p - 1][1]
                carry = emit(p, lap_scale * (total + ahead[q][1]), carry)
        carry = emit(nx - 1, lap_scale * (ahead[nx - 1][0] + ahead[nx - 2][1]), carry)
        if with_ghost:
            inner, outer = lines(ghost, after, before, czg)
            total = cxg * inner + jnp.where(lane >= 16, plane_dn(outer), 0.0)
            total = total + jnp.where(lane < 16 * (nx - 1), plane_up(outer), 0.0)
            emit(GZ, lap_scale * total, carry)
        return carry

    def reaction_of(q):
        return TOUGHNESS / LENGTH_SCALE + 2.0 * react[q]

    def old_damage(q):
        return load_rows(3, q)

    nd, ng = DISP_ITERS, DMG_ITERS
    gram, vector = {}, {}

    def load_start(c, q):
        return gz_wide[c] if q == GZ else load_wide(c, q)

    pass_one(load_start, merge, rows, True)
    pl.when(there(outward, 0))(
        drain(ghost_deep.at[:, tiles_of[2]], ysend_sem.at[0], yrecv_sem.at[2]).wait_recv
    )
    low, a = damage_sum(0)
    taken = z_up_take(pltpu.roll(gz_wide[3], 127, 1), a, 0)
    for q in range(nx - 1):
        high, a = damage_sum(q + 1)
        stiff[q] = rigidity(low, high, valid)
        taken = z_up_take(taken, a, q + 1)
        low = high
    taken = gz_wide[3] + taken
    taken = merge(taken + y_up(taken))
    stiff[GZ] = rigidity(taken, plane_up(taken), gvalid)
    stiff[nx - 1] = blank
    element_pass(True)
    hist[nx - 1] = blank
    greet(hop_sem)

    def keep_lap(q, lap, carry):
        dbasis[0, q] = lap
        return carry

    laplace_pass(old_damage, keep_lap, zero, True)
    arrive(1)
    for f in range(DEEP, fields):
        gz_rows[f - DEEP + 1] = line_rows(*ghost_tiles(f))
    gather_back(stiff, inv_emit)

    def start_emit(q, got, dot):
        inv = inverse[q]
        for c in range(3):
            r = load_rows(DEEP + c, q) - got[c]
            v = inv * r
            basis[c, q] = v
            if q < nx:
                resid[c, q] = r[0:TILE]
                dot = dot + v[0:TILE] * r[0:TILE]
        return dot

    vector[0] = each_node(start_emit, zero)

    def hist_emit(q, total):
        react[q] = jnp.maximum(jnp.abs(load_rows(7, q)), 0.125 * total)

    gather_back(hist, hist_emit)

    for k in range(nd - 1):
        pass_one(lambda c, q, k=k: basis[3 * k + c, q], same, rows, True)
        element_pass(False)

        def apply_emit(q, got, carry, k=k):
            carry = list(carry)
            inv = inverse[q] * (2.0 / SPECTRUM)
            for c in range(3):
                w = got[c]
                here = basis[3 * k + c, q]
                v = inv * w - here
                if k:
                    v = 2.0 * v - basis[3 * (k - 1) + c, q]
                basis[3 * (k + 1) + c, q] = v
                if q < nx:
                    wi, vi = w[0:TILE], v[0:TILE]
                    if k + 2 < nd:
                        images[3 * k + c, q] = wi
                    carry[0] = carry[0] + here[0:TILE] * wi
                    carry[1] = carry[1] + vi * resid[c, q]
                    carry[2] = carry[2] + vi * wi
                    for j in range(k):
                        carry[3 + j] = carry[3 + j] + vi * images[3 * j + c, q]
            return tuple(carry)

        got = each_node(apply_emit, (zero,) * (3 + k))
        gram[k, k], vector[k + 1], gram[k + 1, k] = got[:3]
        for j in range(k):
            gram[k + 1, j] = got[3 + j]

    across = pl.ds((1 - gx) * lx, lx)
    x_basis = xcopy(basis.at[:, across, 0:TILE], basis_part, 2)
    x_basis.start()

    def last_energy():
        pass_one(lambda c, q: basis[3 * (nd - 1) + c, q], same, TILE, False)
        total = zero
        for r in (slice(0, TILE),):
            low = [modes[m, 0, r, :] for m in range(12)]
            for p in range(nx - 1):
                high = [modes[m, p + 1, r, :] for m in range(12)]
                S = [low[m] + high[m] if m % 4 else None for m in range(12)]
                D = [high[m] - low[m] for m in range(12)]
                xX, xXY, xXZ, xXYZ = D[0:4]
                yX, yXY, yXZ, yXYZ = D[4:8]
                zX, zXY, zXZ, zXYZ = D[8:12]
                _, xY, xZ, xYZ = S[0:4]
                _, yY, yZ, yYZ = S[4:8]
                _, zY, zZ, zYZ = S[8:12]
                div = xX + yY + zZ
                sxy, sxz, syz = xY + yX, xZ + zX, yZ + zY
                tw = xYZ + yXZ + zXY
                sum_two = xX * xX + yY * yY + zZ * zZ
                sum_shear = sxy * sxy + sxz * sxz + syz * syz
                sum_twist = xYZ * xYZ + yXZ * yXZ + zXY * zXY + tw * tw
                sum_bend = (yYZ * yYZ + xXZ * xXZ) + (zYZ * zYZ + xXY * xXY) + (yXY * yXY + zXZ * zXZ)
                sum_cross = yYZ * xXZ + zYZ * xXY + yXY * zXZ
                sum_last = xXYZ * xXYZ + yXYZ * yXYZ + zXYZ * zXYZ
                energy = (
                    (k_lame * (div * div) + k_two * sum_two)
                    + (k_shear * sum_shear + k_twist * sum_twist)
                    + (k_bend * sum_bend + (2.0 * k_cross) * sum_cross)
                    + k_last * sum_last
                ) * stiff[p, r, :]
                total = total + energy
                low = high
        return total

    gram[nd - 1, nd - 1] = last_energy()

    def dstart(q, lap, dot):
        reaction = reaction_of(q)
        if q == GZ:
            count, mask = cxg * cy * czg, gnode
        else:
            count, mask = (cy * cz if q in (0, nx - 1) else 2.0 * cy * cz), node
        inv = mask / (diag_scale * count + reaction)
        dinverse[q] = inv
        r = 2.0 * react[q] - (lap + reaction * old_damage(q))
        v = inv * r
        dbasis[0, q] = v
        if q < nx:
            dresid[q] = r[0:TILE]
            dot = dot + v[0:TILE] * r[0:TILE]
        return dot

    dvector, dgram = {}, {}
    dvector[0] = zero
    for q in range(nx + 1):
        dvector[0] = dstart(q, dbasis[0, q], dvector[0])
    for k in range(ng):
        more = k + 1 < ng

        def dstep(q, lap, carry, k=k, more=more):
            carry = list(carry)
            here = dbasis[k, q]
            w = lap + reaction_of(q) * here
            if q < nx:
                carry[0] = carry[0] + here[0:TILE] * w[0:TILE]
            if more:
                v = dinverse[q] * w - here
                if k:
                    v = 2.0 * v - dbasis[k - 1, q]
                dbasis[k + 1, q] = v
                if q < nx:
                    carry[1] = carry[1] + v[0:TILE] * dresid[q]
                    carry[2] = carry[2] + v[0:TILE] * w[0:TILE]
            return tuple(carry)

        got = laplace_pass(
            lambda q, k=k: dbasis[k, q], dstep, (zero,) * (3 if more else 1), more
        )
        dgram[k, k] = got[0]
        if more:
            dvector[k + 1], dgram[k + 1, k] = got[1:]

    parts = [vector[i] for i in range(nd)] + [dvector[i] for i in range(ng)]
    parts += [gram[i, j] for i in range(nd) for j in range(i + 1)]
    parts += [dgram[i, j] for i in range(ng) for j in range(i + 1)]
    at = lax.broadcasted_iota(jnp.int32, (1, 128), 1)
    packed = jnp.zeros((1, 128), f32)
    for i, piece in enumerate(parts):
        line = jnp.sum(piece, axis=0, keepdims=True)
        packed = jnp.where(at == i, jnp.sum(line, axis=1, keepdims=True), packed)
    slot_mine = gx * npeer + me
    sums[slot_mine] = packed
    pl.semaphore_wait(hop_sem, number_near)

    def peer(dy, dz):
        return lax.rem(gy + dy, ngy), lax.rem(gz + dz, ngz)

    def peer_copy(side, dy, dz, slot):
        return remote(
            sums.at[slot_mine], sums.at[slot], asend_sem.at[0], arecv_sem.at[0],
            (gx if side == 0 else 1 - gx, *peer(dy, dz)),
        )

    offsets = sorted(
        [(dy, dz) for dy in range(ngy) for dz in range(ngz)],
        key=lambda o: -(2 * (o[1] % 2) + (o[1] > 0) + o[0] % 2 + (o[0] > 0)),
    )
    peers = [(side, dy, dz) for dy, dz in offsets for side in (0, 1) if side or dy or dz]
    sends = [peer_copy(side, dy, dz, slot_mine) for side, dy, dz in peers]
    for s in sends:
        s.start()
    x_damage = xcopy(dbasis.at[:, across, 0:TILE], dbasis_part, 3)
    x_damage.start()
    x_react = xcopy(react.at[across, 0:TILE], react_part, 4)
    x_react.start()
    x_parts = [x_basis, x_damage, x_react]
    for passed in x_parts:
        passed.wait_recv()

    def both_tiles(near_tile, far_tile):
        return jnp.concatenate(order(near_tile, far_tile), axis=0)

    for p in range(lx):
        out_history[p] = both_tiles(react[gx * lx + p, 0:TILE], react_part[p])
    everyone = drain(sums.at[0 : 2 * npeer - 1], asend_sem.at[0], arecv_sem.at[0])
    everyone.wait_recv()
    layer = [sums[i] for i in range(2 * npeer)]
    while len(layer) > 1:
        layer = [a + b for a, b in zip(layer[::2], layer[1::2])] + layer[len(layer) & ~1 :]
    whole = layer[0]

    scalars = [
        jnp.sum(jnp.where(at == i, whole, 0.0), axis=1, keepdims=True) for i in range(len(parts))
    ]

    def solve(rhs, lower):
        n = len(rhs)
        A = [[lower[max(i, j)][min(i, j)] for j in range(n)] for i in range(n)]
        b = list(rhs)
        for i in range(n):
            pivot = 1.0 / A[i][i]
            for r in range(i + 1, n):
                ratio = A[r][i] * pivot
                for c in range(i + 1, n):
                    A[r][c] = A[r][c] - ratio * A[i][c]
                b[r] = b[r] - ratio * b[i]
        out = [None] * n
        for i in reversed(range(n)):
            s = b[i]
            for j in range(i + 1, n):
                s = s - A[i][j] * out[j]
            out[i] = s / A[i][i]
        return out

    def triangle(flat, n):
        return [[flat[k * (k + 1) // 2 + j] for j in range(k + 1)] for k in range(n)]

    rest = scalars[nd + ng :]
    cut = nd * (nd + 1) // 2
    weights = solve(scalars[:nd], triangle(rest[:cut], nd))
    dweights = solve(scalars[nd : nd + ng], triangle(rest[cut:], ng))
    for p in range(lx):
        at_x = gx * lx + p
        for c in range(3):
            near_x = far_x = zero
            for k in range(nd):
                near_x = near_x + weights[k] * basis[3 * k + c, at_x, 0:TILE]
                far_x = far_x + weights[k] * basis_part[3 * k + c, p]
            lower, upper = order(near_x, far_x)
            out_disp[c, p, 0:TILE] = full_deep[c, 0, at_x] + lower
            out_disp[c, p, TILE:ly] = full_deep[c, 1, at_x] + upper
        near_d = far_d = zero
        for k in range(ng):
            near_d = near_d + dweights[k] * dbasis[k, at_x, 0:TILE]
            far_d = far_d + dweights[k] * dbasis_part[k, p]
        lower, upper = order(near_d, far_d)
        out_damage[p, 0:TILE] = full_deep[3, 0, at_x] + lower
        out_damage[p, TILE:ly] = full_deep[3, 1, at_x] + upper

    for side, dz in ((0, -1), (1, 1)):
        pl.when(there(0, dz))(
            drain(full_deep.at[0, 0], zsend_sem.at[side], zrecv_sem.at[0]).wait_send
        )
        for dy in (-1, 1):
            pl.when(there(dy, dz))(
                drain(zsend_deep.at[side], csend_sem.at[2 * (dy > 0) + side], crecv_sem.at[0]).wait_send
            )
    for kind in range(3):
        for dy in (-1, 1):
            pl.when(there(dy, 0))(ycopy(0, dy, kind).wait_send)
    for passed in x_own + x_parts:
        passed.wait_send()
    everyone.wait_send()


def hand_on(*refs):
    sources, targets, sem = refs[:3], refs[3:6], refs[6]
    copies = [
        pltpu.make_async_copy(source, target, sem.at[i])
        for i, (source, target) in enumerate(zip(sources, targets))
    ]
    for copy in copies:
        copy.start()
    for copy in copies:
        copy.wait()


def body_fused(sizes, *arrays):
    ngy, ngz, lx, ly, lz = sizes
    nx, rows, wide, fields = 2 * lx, 2 * TILE, 3 * TILE, 8
    packs, pairs, extras = fields * lx // 16, DEEP * lx // 2, DEEP * lx // TILE
    npeer = ngy * ngz
    f32 = jnp.float32
    planes = (nx + 1, rows, lz)
    vmem = pl.BlockSpec(memory_space=pltpu.VMEM)
    hbm = pl.BlockSpec(memory_space=pltpu.HBM)
    dma = pltpu.SemaphoreType.DMA

    def room(*shape):
        return pltpu.VMEM(shape, f32)

    results = pl.pallas_call(
        functools.partial(kernel, sizes),
        out_shape=(
            pltpu.VMEM((3, lx, ly, lz), f32),
            pltpu.VMEM((lx, ly, lz), f32),
            pltpu.VMEM((lx, ly, lz), f32),
        ),
        in_specs=[hbm] * 6,
        out_specs=(vmem,) * 3,
        scratch_shapes=[
            room(3, lx, ly, lz),
            room(3, lx, ly, lz),
            room(lx, ly, lz),
            room(lx, ly, lz),
            pltpu.VMEM((lx, ly, lz), jnp.int32),
            pltpu.VMEM((lx, ly, lz), jnp.int32),
            room(DEEP, 2, nx, TILE, lz),
            room(DEEP, 2, nx, TILE, lz),
            room(pairs + extras, TILE, 128),
            room(pairs + extras, TILE, 128),
            room(pairs, TILE, 128),
            room(pairs, TILE, 128),
            room(2, pairs + extras, TILE, 128),
            room(2, pairs, TILE, 128),
            room(2, 2, TILE, 128),
            room(2, 2, TILE, 128),
            room(2, 2, 3, TILE, 128),
            room(2, 2, 3, TILE, 128),
            room(4, wide, 128),
            room(5, rows, 128),
            room(12, *planes),
            room(3 * DISP_ITERS, *planes),
            room(3 * (DISP_ITERS - 2), nx, TILE, lz),
            room(3, nx, TILE, lz),
            room(*planes),
            room(*planes),
            room(*planes),
            room(*planes),
            room(*planes),
            room(DMG_ITERS, *planes),
            room(nx, TILE, lz),
            room(3 * DISP_ITERS, lx, TILE, lz),
            room(DMG_ITERS, lx, TILE, lz),
            room(lx, TILE, lz),
            room(2 * npeer, 1, 128),
            dma((2,)),
            dma((6,)),
            dma((3,)),
            dma((2,)),
            dma((4,)),
            dma((4,)),
            dma((4,)),
            dma((5,)),
            dma((5,)),
            dma((1,)),
            dma((1,)),
            pltpu.SemaphoreType.REGULAR,
        ],
        compiler_params=pltpu.CompilerParams(
            collective_id=0, has_side_effects=True, vmem_limit_bytes=VMEM_LIMIT
        ),
    )(*[pltpu.with_memory_space_constraint(a, pltpu.HBM) for a in arrays])
    return pl.pallas_call(
        hand_on,
        out_shape=tuple(jax.ShapeDtypeStruct(r.shape, f32) for r in results),
        in_specs=[vmem] * 3,
        out_specs=(hbm,) * 3,
        scratch_shapes=[dma((3,))],
        compiler_params=pltpu.CompilerParams(vmem_limit_bytes=1024 * 1024),
    )(*[pltpu.with_memory_space_constraint(r, pltpu.VMEM) for r in results])


VMEM_LIMIT = 24 * 1024 * 1024


def solution(mesh):
    shape = dict(mesh.shape)

    def body(*arrays):
        lx, ly, lz = arrays[2].shape
        fits = shape["gx"] == 2 and shape["gy"] * shape["gz"] > 1
        fits = fits and max(shape["gy"], shape["gz"]) <= 4
        fits = fits and lx == 4 and ly == 2 * TILE and lz == 128
        if fits:
            return body_fused((shape["gy"], shape["gz"], lx, ly, lz), *arrays)
        return body_any_mesh(*arrays)

    return jax.shard_map(
        body,
        mesh=mesh,
        in_specs=(
            P(None, "gx", "gy", "gz"),
            P(None, "gx", "gy", "gz"),
            P("gx", "gy", "gz"),
            P("gx", "gy", "gz"),
            P("gx", "gy", "gz"),
            P("gx", "gy", "gz"),
        ),
        out_specs=(P(None, "gx", "gy", "gz"), P("gx", "gy", "gz"), P("gx", "gy", "gz")),
        check_vma=False,
    )
```
